512 devices in a mesh: depth: 256 (over z, y, x), chan: 2 (over core).
Axes of the slice: x: 4, y: 8, z: 8, core: 2. Of those that a mesh axis runs over, the one named last changes fastest.
Arguments:
- feats: bfloat16 [32, 512, 8, 128], P('chan', 'depth'), may hold values from -6 to 6
- weight_one: bfloat16 [32, 32, 27], replicated, may hold values from -0.21875 to 0.21875
- weight_two: bfloat16 [64, 32, 27], replicated, may hold values from -0.21875 to 0.21875
- cotangent: bfloat16 [64, 256, 4, 64], P('chan', 'depth'), may hold values from -6 to 6
Outputs:
- grad_feats: bfloat16 [32, 512, 8, 128], P('chan', 'depth')
- grad_weight_one: float32 [32, 32, 27], P(None, 'chan')
- grad_weight_two: float32 [64, 32, 27], P(None, 'chan')
The draws below stay inside these ranges and needn't reach their ends.
All inputs are finite; a program needn't handle non-finite values.
Results may differ from the reference program's by a relative error of at most 0.013.
Values may be sent and summed in bfloat16 or wider, within the bound.
No kernel may reach another device: no remote copies, remote signals or barrier semaphores. Data moves between devices by JAX's collectives and lax.ppermute only.
A program may use at most 128 MiB of HBM per device.

```python
import jax
import jax.numpy as jnp
from jax import lax

C0 = 32
C1 = 64
H = 8
W = 128
NZ = 512


def shard_levels(rng, dims, cuts, low, largest):
    factor_of, own = 1.0, jax.random.fold_in(rng, 6)
    for axis_at, blocks in cuts:
        draws = jnp.exp(jax.random.uniform(jax.random.fold_in(own, axis_at), (blocks,), jnp.float32, low / len(cuts), largest / len(cuts)))
        factor_of = factor_of * jnp.repeat(draws, dims[axis_at] // blocks).reshape([-1 if axis == axis_at else 1 for axis in range(len(dims))])
    return factor_of


def gaussian(rng, shape, scale, bound, cuts=(), held_as=jnp.bfloat16):
    entries = scale * jax.random.normal(rng, shape, jnp.float32)
    if cuts:
        entries = entries * shard_levels(rng, shape, cuts, -0.22, 0.18)
    return jnp.clip(entries, -bound, bound).astype(held_as)


def setup_inputs(seed: int = 0) -> dict:
    splits = jax.random.split(jax.random.key(seed), 5)
    feats = gaussian(splits[0], (C0, NZ, H, W), 1.0, 6.0, ((0, 2), (1, 256)))
    weight_one = gaussian(splits[1], (C0, C0, 27), (27 * C0) ** -0.5, 0.21875)
    weight_two = gaussian(splits[2], (C1, C0, 27), (27 * C0) ** -0.5, 0.21875)
    cotangent = gaussian(splits[3], (C1, NZ // 2, H // 2, W // 2), 1.0, 6.0, ((0, 2), (1, 256)))
    return dict(feats=feats, weight_one=weight_one, weight_two=weight_two, cotangent=cotangent)


OFFSETS = [(first, second, third) for first in range(3) for second in range(3) for third in range(3)]

def pad_all(field):
    return jnp.pad(field.astype(jnp.float32), ((0, 0), (1, 1), (1, 1), (1, 1)))

def convolve(field, weight):
    chans, planes, height, across = field.shape
    padded = pad_all(field)
    total = jnp.zeros((weight.shape[0], planes, height, across), jnp.float32)
    for index, (first, second, third) in enumerate(OFFSETS):
        window = padded[:, first:first + planes, second:second + height, third:third + across]
        total = total + jnp.einsum('oi,izhw->ozhw', weight[:, :, index].astype(jnp.float32), window, precision=lax.Precision.HIGHEST)
    return total

def transpose_conv(grads, weight):
    chans, planes, height, across = grads.shape
    padded = pad_all(grads)
    total = jnp.zeros((weight.shape[1], planes, height, across), jnp.float32)
    for index, (first, second, third) in enumerate(OFFSETS):
        window = padded[:, 2 - first:2 - first + planes, 2 - second:2 - second + height, 2 - third:2 - third + across]
        total = total + jnp.einsum('oi,ozhw->izhw', weight[:, :, index].astype(jnp.float32), window, precision=lax.Precision.HIGHEST)
    return total

def weight_grad(grads, field):
    chans, planes, height, across = field.shape
    padded = pad_all(field)
    grads_wide = grads.astype(jnp.float32)
    pieces = []
    for index, (first, second, third) in enumerate(OFFSETS):
        window = padded[:, first:first + planes, second:second + height, third:third + across]
        pieces.append(jnp.einsum('ozhw,izhw->oi', grads_wide, window, precision=lax.Precision.HIGHEST))
    return jnp.stack(pieces, axis=-1)

def slope(pre):
    sig = jax.nn.sigmoid(pre)
    return sig * (1.0 + pre * (1.0 - sig))

def one_volume(feats, weight_one, weight_two, cotangent):
    chans, planes, height, across = feats.shape
    pre_one = convolve(feats, weight_one)
    act_one = jax.nn.silu(pre_one).astype(jnp.bfloat16)
    pooled = act_one.astype(jnp.float32).reshape(chans, planes // 2, 2, height // 2, 2, across // 2, 2).mean(axis=(2, 4, 6)).astype(jnp.bfloat16)
    pre_two = convolve(pooled, weight_two)
    grad_two = (cotangent.astype(jnp.float32) * slope(pre_two)).astype(jnp.bfloat16)
    grad_weight_two = weight_grad(grad_two, pooled)
    back_pooled = transpose_conv(grad_two, weight_two)
    spread = jnp.repeat(jnp.repeat(jnp.repeat(back_pooled, 2, axis=1), 2, axis=2), 2, axis=3) * 0.125
    grad_one = (spread * slope(pre_one)).astype(jnp.bfloat16)
    grad_weight_one = weight_grad(grad_one, feats)
    grad_feats = transpose_conv(grad_one, weight_one).astype(jnp.bfloat16)
    return (grad_feats, grad_weight_one, grad_weight_two)

def reference(feats, weight_one, weight_two, cotangent):
    return one_volume(feats, weight_one, weight_two, cotangent)
```

```python
import functools

import jax
import jax.numpy as jnp
from jax import lax
from jax.experimental import pallas as pl
from jax.experimental.pallas import tpu as pltpu
from jax.sharding import Mesh
from jax.sharding import PartitionSpec as P

DEPTH = ("z", "y_high", "y_low", "x")
NEAR = ("y_low", "x")
FAR = ("z", "y_high")
SLABS = 256
ROW = 4
BF16 = jnp.bfloat16
F32 = jnp.float32


def depth_shift(block, steps):
    pairs = [(i, i + steps) for i in range(SLABS) if 0 <= i + steps < SLABS]
    return lax.ppermute(block, DEPTH, pairs)


def slope(pre):
    sig = jax.nn.sigmoid(pre)
    return sig * (1.0 + pre * (1.0 - sig))


def pick(rows, lanes, width, step):
    row = lax.broadcasted_iota(jnp.int32, (rows, lanes), 0)
    lane = lax.broadcasted_iota(jnp.int32, (rows, lanes), 1)
    target = step(row // width) * width + row % width
    return jnp.where(lane == target, 1.0, 0.0).astype(BF16)


def band_kernel(w1, w1t, w2, w2t, t1, t1t, t2, t2t):
    def fill(weights, out, height, rows, width, lanes, sign):
        for h in range(height):
            marks = pick(3 * width, lanes, width, lambda b: h + sign * (b - 1))
            bands = jnp.dot(weights[...], marks, preferred_element_type=F32).astype(BF16)
            for tap in range(9):
                out[h * rows : (h + 1) * rows, tap * lanes : (tap + 1) * lanes] = bands[
                    tap * rows : (tap + 1) * rows
                ]

    fill(w1, t1, 8, 32, 32, 256, 1)
    fill(w2, t2, 4, 64, 32, 128, 1)
    fill(w2t, t2t, 4, 32, 64, 256, -1)
    fill(w1t, t1t, 8, 16, 32, 256, -1)


def shifted(value, step):
    lanes = value.shape[-1]
    lane = lax.broadcasted_iota(jnp.int32, value.shape, 1)
    low = jnp.where(lane < step, 0.0, pltpu.roll(value, step, 1))
    high = jnp.where(lane >= lanes - step, 0.0, pltpu.roll(value, lanes - step, 1))
    return low.astype(BF16), value.astype(BF16), high.astype(BF16)


def main_kernel(
    scalars, own, oth, t1, t1t, t2, t2t, gf, wg, XP, PS, SL, QP, GP, HP, CT, FS, FP, G1, G2
):
    member = scalars[0]
    place = scalars[1]
    x = scalars[2]
    half = pl.multiple_of(member * 16, 16)

    def slot(delta):
        return lax.rem(x + delta + 4, 4)

    planes = [(slot(0), 0)]
    planes += [(slot(delta), 8 * p) for delta in (-3, -2, -1) for p in range(2)]
    planes += [(slot(0), 12), (slot(0), 20)]
    planes += [(slot(delta), 20 + 8 * p) for delta in (1, 2, 3) for p in range(2)]
    planes += [(slot(0), 32)]
    for j, (at, start) in enumerate(planes):
        plane = jnp.concatenate(
            [own[at, start : start + 8], oth[at, start : start + 8]], axis=1
        ).reshape(256, 128)
        for c, part in enumerate(shifted(plane.astype(F32), 1)):
            if j <= 8:
                XP[j, c, :, :128] = part
            if j >= 7:
                XP[j - 7, c, :, 128:] = part

    for k in range(7):
        pre = jnp.dot(t1[...], XP[k : k + 3].reshape(2304, 256), preferred_element_type=F32)
        act = (pre * jax.nn.sigmoid(pre)).astype(BF16).astype(F32).reshape(4, 2, 32, 256)
        rows = (act[:, 0] + act[:, 1]).reshape(128, 256)
        PS[k] = rows[:, :128]
        PS[k + 7] = rows[:, 128:]
        if k >= 5:
            SL[k - 5] = slope(pre[:, :128])
        if k <= 1:
            SL[k + 2] = slope(pre[:, 128:])

    lane = lax.broadcasted_iota(jnp.int32, (128, 128), 1)
    even = lane % 2 == 0
    for c in range(3):
        QP[4, c, :, 128:] = jnp.zeros((128, 128), BF16)
    for j in range(7):
        total = PS[2 * j] + PS[2 * j + 1]
        total = total + jnp.where(even, pltpu.roll(total, 127, 1), pltpu.roll(total, 1, 1))
        at = place + (j - 3)
        factor = jnp.where((at >= 0) & (at < SLABS), 0.125, 0.0)
        pooled = (total * factor).astype(BF16).astype(F32)
        for c, part in enumerate(shifted(pooled, 2)):
            if j <= 4:
                QP[j, c, :, :128] = part
            if j >= 3:
                QP[j - 3, c, :, 128:] = part

    cots = [(slot(-2), 16), (slot(-1), 16), (slot(0), 28), (slot(1), 36), (slot(2), 36)]
    own_o = pl.multiple_of(member * 32, 32)
    oth_o = pl.multiple_of(32 - member * 32, 32)
    for e, (at, start) in enumerate(cots):
        for high in range(2):
            here = start + 2 * high
            CT[e, high, pl.ds(own_o, 32), :] = own[at, here : here + 2].reshape(32, 128)
            CT[e, high, pl.ds(oth_o, 32), :] = oth[at, here : here + 2].reshape(32, 128)
    row = lax.broadcasted_iota(jnp.int32, (128, 256), 0)
    col = lax.broadcasted_iota(jnp.int32, (128, 256), 1)
    spread = jnp.where(row == (col // 128) * 64 + (col % 128) // 2, 1.0, 0.0).astype(BF16)
    cot = jnp.dot(CT[...].reshape(640, 128), spread, preferred_element_type=F32)

    for e in range(3):
        pre_two = jnp.dot(t2[...], QP[e : e + 3].reshape(1152, 256), preferred_element_type=F32)
        slopes = slope(pre_two)
        for plane in (e, e + 3):
            if plane > 4:
                continue
            side = slopes[:, :128] if plane == e else slopes[:, 128:]
            base = plane * 128
            cots_of = jnp.concatenate(
                [
                    cot[base : base + 64, :128],
                    cot[base : base + 64, 128:],
                    cot[base + 64 : base + 128, :128],
                    cot[base + 64 : base + 128, 128:],
                ],
                axis=0,
            )
            grad = (cots_of * side).astype(BF16).astype(F32)
            for c, part in enumerate(shifted(grad, 2)):
                for m in range(3):
                    n = plane - m
                    if 0 <= n <= 2:
                        GP[m, c, :, n * 128 : (n + 1) * 128] = part
            if plane == 2:
                lanes = lax.broadcasted_iota(jnp.int32, (256, 128), 1)
                kept = jnp.where(lanes % 2 == 0, grad, 0.0).astype(BF16)
                G2[...] = jnp.zeros(G2.shape, BF16)
                for h in range(4):
                    G2[32:96, h * 128 : (h + 1) * 128] = kept[h * 64 : (h + 1) * 64]

    back = jnp.dot(t2t[...], GP[...].reshape(2304, 384), preferred_element_type=F32)
    G1[...] = jnp.zeros(G1.shape, BF16)
    for q, f in enumerate((0, 1, 1, 2)):
        at = place + (f - 1)
        factor = jnp.where((at >= 0) & (at < SLABS), 0.125, 0.0)
        part = (back[:, f * 128 : (f + 1) * 128] * factor).reshape(4, 1, 32, 128)
        wide = jnp.concatenate([part, part], axis=1).reshape(256, 128)
        grad = (wide * SL[q]).astype(BF16).astype(F32)
        for c, piece in enumerate(shifted(grad, 1)):
            if q <= 2:
                HP[q, c, :, :128] = piece
            if q >= 1:
                HP[q - 1, c, :, 128:] = piece
            if c == 1 and q in (1, 2):
                for h in range(8):
                    to = ((q - 1) * 8 + h) * 128
                    G1[0:32, to : to + 128] = piece[h * 32 : (h + 1) * 32]

    nothing = jnp.zeros((16, 128), BF16)
    for a in range(3):
        for b in range(3):
            for c in range(3):
                tap = (a * 3 + b) * 3 + c
                to = slice(tap * 16, tap * 16 + 16)
                for q in range(2):
                    j = 6 + a + q
                    m, side = (j, 0) if j <= 8 else (j - 7, 128)
                    for h in range(8):
                        at = h + b - 1
                        lanes = slice((q * 8 + h) * 128, (q * 8 + h + 1) * 128)
                        if 0 <= at < 8:
                            FS[to, lanes] = XP[m, c, at * 32 : at * 32 + 16, side : side + 128]
                        else:
                            FS[to, lanes] = nothing
                for h in range(4):
                    at = h + b - 1
                    lanes = slice(h * 128, (h + 1) * 128)
                    if 0 <= at < 4:
                        FP[to, lanes] = QP[2 + a, c, pl.ds(at * 32 + half, 16), :128]
                    else:
                        FP[to, lanes] = nothing
    along = (((1,), (1,)), ((), ()))
    wg[0:432] = lax.dot_general(
        FS[...], G1[...], along, preferred_element_type=F32
    ) + lax.dot_general(FP[...], G2[...], along, preferred_element_type=F32)
    wg[432:] = jnp.zeros((80, 128), F32)

    out = jnp.dot(t1t[...], HP[...].reshape(2304, 256), preferred_element_type=F32)
    gf[0] = out[:, :128].astype(BF16)
    gf[1] = out[:, 128:].astype(BF16)


def band_weights(w1, w1t, w2, w2t):
    shapes = [(256, 2304), (128, 2304), (256, 1152), (128, 2304)]
    return pl.pallas_call(
        band_kernel,
        out_shape=[jax.ShapeDtypeStruct(shape, BF16) for shape in shapes],
        cost_estimate=pl.CostEstimate(flops=10**9, bytes_accessed=4 * 10**6, transcendentals=0),
        name="bands",
    )(w1, w1t, w2, w2t)


def levels(scalars, own, oth, bands):
    vmem = pl.BlockSpec(memory_space=pltpu.VMEM)
    scratch = [
        ((9, 3, 256, 256), BF16),
        ((14, 128, 128), F32),
        ((4, 256, 128), F32),
        ((5, 3, 128, 256), BF16),
        ((3, 3, 256, 384), BF16),
        ((3, 3, 256, 256), BF16),
        ((5, 2, 64, 128), BF16),
        ((432, 2048), BF16),
        ((432, 512), BF16),
        ((128, 2048), BF16),
        ((128, 512), BF16),
    ]
    return pl.pallas_call(
        main_kernel,
        in_specs=[pl.BlockSpec(memory_space=pltpu.SMEM)] + [vmem] * 6,
        out_specs=[vmem, vmem],
        out_shape=[
            jax.ShapeDtypeStruct((2, 128, 128), BF16),
            jax.ShapeDtypeStruct((512, 128), F32),
        ],
        scratch_shapes=[pltpu.VMEM(shape, dtype) for shape, dtype in scratch],
        cost_estimate=pl.CostEstimate(
            flops=10**10, bytes_accessed=8 * 10**6, transcendentals=10**6
        ),
        name="levels",
    )(scalars, own, oth, *bands)


def total_over_depth(part):
    pieces = lax.all_to_all(part.reshape(16, 32, 128), NEAR, 0, 0, tiled=True)
    near = jnp.sum(pieces, axis=0)
    copies = jnp.broadcast_to(near, (16, 32, 128))
    pieces = lax.all_to_all(copies, FAR, 0, 0, tiled=True)
    whole = jnp.sum(pieces, axis=0)
    copies = jnp.broadcast_to(whole, (16, 32, 128))
    return lax.all_to_all(copies, NEAR, 0, 0, tiled=True).reshape(512, 128)


def shards(feats, weight_one, weight_two, cotangent):
    member = lax.axis_index("chan")
    place = lax.axis_index(DEPTH)
    x = lax.axis_index("x")
    fields = jnp.transpose(feats, (1, 2, 0, 3)).reshape(16, 16, 128)
    cot = jnp.transpose(cotangent.reshape(32, 2, 2, 64), (1, 0, 2, 3)).reshape(4, 16, 128)
    block = jnp.concatenate([fields, cot], axis=0)
    up = depth_shift(block, ROW)
    down = depth_shift(block, -ROW)

    w1 = weight_one.reshape(32, 32, 3, 3, 3)
    w2 = weight_two.reshape(64, 32, 3, 3, 3)
    own_one = lax.dynamic_slice_in_dim(w1, member * 16, 16, 1)
    other_one = lax.dynamic_slice_in_dim(w1, 16 - member * 16, 16, 1)
    ordered = jnp.concatenate([own_one, other_one], axis=1)
    bands = band_weights(
        jnp.transpose(ordered, (2, 4, 0, 3, 1)).reshape(288, 96),
        jnp.transpose(own_one[:, :, ::-1, :, ::-1], (2, 4, 1, 3, 0)).reshape(144, 96),
        jnp.transpose(w2, (2, 4, 0, 3, 1)).reshape(576, 96),
        jnp.transpose(w2[:, :, ::-1, :, ::-1], (2, 4, 1, 3, 0)).reshape(288, 192),
    )

    three = jnp.concatenate([up, block, down], axis=0)
    slots = [
        lax.dynamic_slice_in_dim(
            three, jnp.where(x > t, 0, jnp.where(x == t, 8, 20)).astype(jnp.int32), 40, 0
        )
        for t in range(4)
    ]
    own = lax.all_to_all(jnp.stack(slots, 0), "x", 0, 0, tiled=True)
    oth = lax.ppermute(own, "chan", [(0, 1), (1, 0)])
    scalars = jnp.stack([member, place, x]).astype(jnp.int32)
    grad_feats, part = levels(scalars, own, oth, bands)
    total = total_over_depth(part)[:432]
    grad_weight_one = jnp.transpose(total[:, :32].reshape(27, 16, 32), (2, 1, 0))
    grad_weight_two = jnp.transpose(total[:, 32:96].reshape(27, 16, 64), (2, 1, 0))
    grad_feats = jnp.transpose(grad_feats.reshape(2, 8, 16, 128), (2, 0, 1, 3))
    return (grad_feats, grad_weight_one, grad_weight_two)


def solution(mesh):
    finer = Mesh(
        mesh.devices.reshape(8, 2, 4, 4, mesh.shape["chan"]), DEPTH + ("chan",)
    )
    in_specs = (P("chan", DEPTH, None, None), P(), P(), P("chan", DEPTH, None, None))
    out_specs = (P("chan", DEPTH, None, None), P(None, "chan", None), P(None, "chan", None))
    return jax.shard_map(
        shards, mesh=finer, in_specs=in_specs, out_specs=out_specs, check_vma=False
    )
```

```python
import jax
import jax.numpy as jnp
from jax import lax
from jax.experimental import pallas as pl
from jax.experimental.pallas import tpu as pltpu
from jax.sharding import Mesh
from jax.sharding import PartitionSpec as P


DEPTH = ("z", "y", "x")
SLABS = 256
ROW = 4
BF16 = jnp.bfloat16
F32 = jnp.float32


def depth_shift(block, steps):
    pairs = [(i, i + steps) for i in range(SLABS) if 0 <= i + steps < SLABS]
    return lax.ppermute(block, DEPTH, pairs)


def slope(pre):
    sig = jax.nn.sigmoid(pre)
    return sig * (1.0 + pre * (1.0 - sig))


def near_groups():
    far_class = [0, 1, 0, 1, 1, 0, 1, 0]
    groups = {}
    for place in range(SLABS):
        z, y, x = place // 32, place // 4 % 8, place % 4
        rank = (x * 2 + far_class[y]) * 2 + far_class[z]
        groups.setdefault((z // 2, y // 2), {})[rank] = place
    near = [[block[rank] for rank in range(16)] for block in groups.values()]
    far = [[block[rank] for block in groups.values()] for rank in range(16)]
    return near, far


NEAR, FAR = near_groups()


def band_kernel(scalars, w1, w1t, w2, w2t, t1, t1t, t2, t2t):
    turn = scalars[0] * 16
    half = pl.multiple_of(turn, 16)

    def fill(weights, out, height, rows, width, lanes, sign, turn):
        row = lax.broadcasted_iota(jnp.int32, (3 * width, lanes), 0)
        lane = lax.broadcasted_iota(jnp.int32, (3 * width, lanes), 1)
        base = lane - (sign * (row // width - 1) * width + (row + turn) % width)
        for h in range(height):
            marks = jnp.where(base == h * width, 1.0, 0.0).astype(BF16)
            bands = jnp.dot(weights, marks, preferred_element_type=F32).astype(BF16)
            for tap in range(9):
                out[h * rows : (h + 1) * rows, tap * lanes : (tap + 1) * lanes] = bands[
                    tap * rows : (tap + 1) * rows
                ]

    def forward(ref):
        parts = [
            jnp.concatenate([ref[9 * a + 3 * b + c] for a in range(3) for c in range(3)], axis=0)
            for b in range(3)
        ]
        return jnp.concatenate(parts, axis=1)

    def backward(load):
        taps = [(2 - a, 2 - c) for a in range(3) for c in range(3)]
        parts = [
            jnp.concatenate([load(9 * a + 3 * b + c) for a, c in taps], axis=0) for b in range(3)
        ]
        return jnp.concatenate(parts, axis=1)

    fill(forward(w1), t1, 8, 32, 32, 256, 1, turn)
    fill(forward(w2), t2, 4, 64, 32, 128, 1, 0)
    fill(backward(lambda t: w2t[t]), t2t, 4, 32, 64, 256, -1, 0)
    fill(backward(lambda t: w1t[t, pl.ds(half, 16), :]), t1t, 8, 16, 32, 256, -1, 0)


def shifted(value, step):
    lanes = value.shape[-1]
    lane = lax.broadcasted_iota(jnp.int32, value.shape, 1)
    low = jnp.where(lane < step, 0.0, pltpu.roll(value, step, 1))
    high = jnp.where(lane >= lanes - step, 0.0, pltpu.roll(value, lanes - step, 1))
    return low.astype(BF16), value.astype(BF16), high.astype(BF16)


def main_kernel(
    scalars, own, oth, t1, t1t, t2, t2t, gf, wg, XP, PS, SL, QP, GP, HP, CT, FS, FP, G1, G2
):
    member = scalars[0]
    place = scalars[1]
    x = scalars[2]
    half = pl.multiple_of(member * 16, 16)

    def slot(delta):
        return lax.rem(x + delta + 4, 4)

    planes = [(slot(0), 0)]
    planes += [(slot(delta), 8 * p) for delta in (-3, -2, -1) for p in range(2)]
    planes += [(slot(0), 12), (slot(0), 20)]
    planes += [(slot(delta), 20 + 8 * p) for delta in (1, 2, 3) for p in range(2)]
    planes += [(slot(0), 32)]
    for j, (at, start) in enumerate(planes):
        plane = jnp.concatenate(
            [own[at, start : start + 8], oth[at, start : start + 8]], axis=1
        ).reshape(256, 128)
        for c, part in enumerate(shifted(plane.astype(F32), 1)):
            if j <= 8:
                XP[j, c, :, :128] = part
            if j >= 7:
                XP[j - 7, c, :, 128:] = part

    for k in range(7):
        pre = jnp.dot(t1[...], XP[k : k + 3].reshape(2304, 256), preferred_element_type=F32)
        act = (pre * jax.nn.sigmoid(pre)).astype(BF16).astype(F32).reshape(4, 2, 32, 256)
        rows = (act[:, 0] + act[:, 1]).reshape(128, 256)
        PS[k] = rows[:, :128]
        PS[k + 7] = rows[:, 128:]
        if k >= 5:
            SL[k - 5] = slope(pre[:, :128])
        if k <= 1:
            SL[k + 2] = slope(pre[:, 128:])

    lane = lax.broadcasted_iota(jnp.int32, (128, 128), 1)
    even = lane % 2 == 0
    for c in range(3):
        QP[4, c, :, 128:] = jnp.zeros((128, 128), BF16)
    for j in range(7):
        total = PS[2 * j] + PS[2 * j + 1]
        total = total + jnp.where(even, pltpu.roll(total, 127, 1), pltpu.roll(total, 1, 1))
        at = place + (j - 3)
        factor = jnp.where((at >= 0) & (at < SLABS), 0.125, 0.0)
        pooled = (total * factor).astype(BF16).astype(F32)
        for c, part in enumerate(shifted(pooled, 2)):
            if j <= 4:
                QP[j, c, :, :128] = part
            if j >= 3:
                QP[j - 3, c, :, 128:] = part

    cots = [(slot(-2), 16), (slot(-1), 16), (slot(0), 28), (slot(1), 36), (slot(2), 36)]
    own_o = pl.multiple_of(member * 32, 32)
    oth_o = pl.multiple_of(32 - member * 32, 32)
    for e, (at, start) in enumerate(cots):
        for high in range(2):
            here = start + 2 * high
            CT[e, high, pl.ds(own_o, 32), :] = own[at, here : here + 2].reshape(32, 128)
            CT[e, high, pl.ds(oth_o, 32), :] = oth[at, here : here + 2].reshape(32, 128)
    row = lax.broadcasted_iota(jnp.int32, (128, 256), 0)
    col = lax.broadcasted_iota(jnp.int32, (128, 256), 1)
    spread = jnp.where(row == (col // 128) * 64 + (col % 128) // 2, 1.0, 0.0).astype(BF16)
    cot = jnp.dot(CT[...].reshape(640, 128), spread, preferred_element_type=F32)

    for e in range(3):
        pre_two = jnp.dot(t2[...], QP[e : e + 3].reshape(1152, 256), preferred_element_type=F32)
        slopes = slope(pre_two)
        for plane in (e, e + 3):
            if plane > 4:
                continue
            side = slopes[:, :128] if plane == e else slopes[:, 128:]
            base = plane * 128
            cots_of = jnp.concatenate(
                [
                    cot[base : base + 64, :128],
                    cot[base : base + 64, 128:],
                    cot[base + 64 : base + 128, :128],
                    cot[base + 64 : base + 128, 128:],
                ],
                axis=0,
            )
            grad = (cots_of * side).astype(BF16).astype(F32)
            for c, part in enumerate(shifted(grad, 2)):
                for m in range(3):
                    n = plane - m
                    if 0 <= n <= 2:
                        GP[m, c, :, n * 128 : (n + 1) * 128] = part
            if plane == 2:
                lanes = lax.broadcasted_iota(jnp.int32, (256, 128), 1)
                kept = jnp.where(lanes % 2 == 0, grad, 0.0).astype(BF16)
                G2[...] = jnp.zeros(G2.shape, BF16)
                for h in range(4):
                    G2[32:96, h * 128 : (h + 1) * 128] = kept[h * 64 : (h + 1) * 64]

    back = jnp.dot(t2t[...], GP[...].reshape(2304, 384), preferred_element_type=F32)
    G1[...] = jnp.zeros(G1.shape, BF16)
    for q, f in enumerate((0, 1, 1, 2)):
        at = place + (f - 1)
        factor = jnp.where((at >= 0) & (at < SLABS), 0.125, 0.0)
        part = (back[:, f * 128 : (f + 1) * 128] * factor).reshape(4, 1, 32, 128)
        wide = jnp.concatenate([part, part], axis=1).reshape(256, 128)
        grad = (wide * SL[q]).astype(BF16).astype(F32)
        for c, piece in enumerate(shifted(grad, 1)):
            if q <= 2:
                HP[q, c, :, :128] = piece
            if q >= 1:
                HP[q - 1, c, :, 128:] = piece
            if c == 1 and q in (1, 2):
                for h in range(8):
                    to = ((q - 1) * 8 + h) * 128
                    G1[0:32, to : to + 128] = piece[h * 32 : (h + 1) * 32]

    nothing = jnp.zeros((16, 128), BF16)
    for a in range(3):
        for b in range(3):
            for c in range(3):
                tap = (a * 3 + b) * 3 + c
                to = slice(tap * 16, tap * 16 + 16)
                for q in range(2):
                    j = 6 + a + q
                    m, side = (j, 0) if j <= 8 else (j - 7, 128)
                    for h in range(8):
                        at = h + b - 1
                        lanes = slice((q * 8 + h) * 128, (q * 8 + h + 1) * 128)
                        if 0 <= at < 8:
                            FS[to, lanes] = XP[m, c, at * 32 : at * 32 + 16, side : side + 128]
                        else:
                            FS[to, lanes] = nothing
                for h in range(4):
                    at = h + b - 1
                    lanes = slice(h * 128, (h + 1) * 128)
                    if 0 <= at < 4:
                        FP[to, lanes] = QP[2 + a, c, pl.ds(at * 32 + half, 16), :128]
                    else:
                        FP[to, lanes] = nothing
    along = (((1,), (1,)), ((), ()))
    wg[0:432] = lax.dot_general(
        FS[...], G1[...], along, preferred_element_type=F32
    ) + lax.dot_general(FP[...], G2[...], along, preferred_element_type=F32)
    wg[432:] = jnp.zeros((80, 128), F32)

    out = jnp.dot(t1t[...], HP[...].reshape(2304, 256), preferred_element_type=F32)
    gf[0] = out[:, :128].astype(BF16)
    gf[1] = out[:, 128:].astype(BF16)


def band_weights(scalars, w1, w1t, w2, w2t):
    vmem = pl.BlockSpec(memory_space=pltpu.VMEM)
    shapes = [(256, 2304), (128, 2304), (256, 1152), (128, 2304)]
    return pl.pallas_call(
        band_kernel,
        in_specs=[pl.BlockSpec(memory_space=pltpu.SMEM)] + [vmem] * 4,
        out_specs=[vmem] * 4,
        out_shape=[jax.ShapeDtypeStruct(shape, BF16) for shape in shapes],
        cost_estimate=pl.CostEstimate(flops=10**9, bytes_accessed=4 * 10**6, transcendentals=0),
        compiler_params=pltpu.CompilerParams(vmem_limit_bytes=16 * 2**20),
        name="bands",
    )(scalars, w1, w1t, w2, w2t)


def levels(scalars, own, oth, bands):
    vmem = pl.BlockSpec(memory_space=pltpu.VMEM)
    scratch = [
        ((9, 3, 256, 256), BF16),
        ((14, 128, 128), F32),
        ((4, 256, 128), F32),
        ((5, 3, 128, 256), BF16),
        ((3, 3, 256, 384), BF16),
        ((3, 3, 256, 256), BF16),
        ((5, 2, 64, 128), BF16),
        ((432, 2048), BF16),
        ((432, 512), BF16),
        ((128, 2048), BF16),
        ((128, 512), BF16),
    ]
    return pl.pallas_call(
        main_kernel,
        in_specs=[pl.BlockSpec(memory_space=pltpu.SMEM)] + [vmem] * 6,
        out_specs=[vmem, vmem],
        out_shape=[
            jax.ShapeDtypeStruct((2, 128, 128), BF16),
            jax.ShapeDtypeStruct((512, 128), F32),
        ],
        scratch_shapes=[pltpu.VMEM(shape, dtype) for shape, dtype in scratch],
        cost_estimate=pl.CostEstimate(
            flops=10**10, bytes_accessed=8 * 10**6, transcendentals=10**6
        ),
        compiler_params=pltpu.CompilerParams(vmem_limit_bytes=28 * 2**20),
        name="levels",
    )(scalars, own, oth, *bands)


def exchange(pieces, groups):
    return lax.all_to_all(pieces, DEPTH, 0, 0, axis_index_groups=groups, tiled=True)


def total_over_depth(part):
    near = jnp.sum(exchange(part.reshape(16, 32, 128), NEAR), axis=0)
    whole = jnp.sum(exchange(jnp.broadcast_to(near, (16, 32, 128)), FAR), axis=0)
    copies = jnp.broadcast_to(whole.astype(BF16), (16, 32, 128))
    return exchange(copies, NEAR).reshape(512, 128).astype(F32)


def shards(feats, weight_one, weight_two, cotangent):
    member = lax.axis_index("chan")
    place = lax.axis_index(DEPTH)
    x = lax.axis_index("x")
    fields = jnp.transpose(feats, (1, 2, 0, 3)).reshape(16, 16, 128)
    cot = jnp.transpose(cotangent.reshape(32, 2, 2, 64), (1, 0, 2, 3)).reshape(4, 16, 128)
    block = jnp.concatenate([fields, cot], axis=0)
    up = depth_shift(block, ROW)
    down = depth_shift(block, -ROW)

    scalars = jnp.stack([member, place, x]).astype(jnp.int32)
    bands = band_weights(
        scalars,
        jnp.transpose(weight_one, (2, 0, 1)),
        jnp.transpose(weight_one, (2, 1, 0)),
        jnp.transpose(weight_two, (2, 0, 1)),
        jnp.transpose(weight_two, (2, 1, 0)),
    )

    three = jnp.concatenate([up, block, down], axis=0)
    slots = [
        lax.dynamic_slice_in_dim(
            three, jnp.where(x > t, 0, jnp.where(x == t, 8, 20)).astype(jnp.int32), 40, 0
        )
        for t in range(4)
    ]
    own = lax.all_to_all(jnp.stack(slots, 0), "x", 0, 0, tiled=True)
    oth = lax.ppermute(own, "chan", [(0, 1), (1, 0)])
    grad_feats, part = levels(scalars, own, oth, bands)
    total = total_over_depth(part)[:432]
    grad_weight_one = jnp.transpose(total[:, :32].reshape(27, 16, 32), (2, 1, 0))
    grad_weight_two = jnp.transpose(total[:, 32:96].reshape(27, 16, 64), (2, 1, 0))
    grad_feats = jnp.transpose(grad_feats.reshape(2, 8, 16, 128), (2, 0, 1, 3))
    return (grad_feats, grad_weight_one, grad_weight_two)


def solution(mesh):
    finer = Mesh(
        mesh.devices.reshape(8, 8, 4, mesh.shape["chan"]), DEPTH + ("chan",)
    )
    in_specs = (P("chan", DEPTH, None, None), P(), P(), P("chan", DEPTH, None, None))
    out_specs = (P("chan", DEPTH, None, None), P(None, "chan", None), P(None, "chan", None))

    return jax.shard_map(
        shards, mesh=finer, in_specs=in_specs, out_specs=out_specs, check_vma=False
    )
```

```python
import jax
import jax.numpy as jnp
from jax import lax
from jax.experimental import pallas as pl
from jax.experimental.pallas import tpu as pltpu
from jax.sharding import Mesh
from jax.sharding import PartitionSpec as P


DEPTH = ("z", "y", "x")
SLABS = 256
ROW = 4
BF16 = jnp.bfloat16
F32 = jnp.float32


def depth_shift(block, steps):
    pairs = [(i, i + steps) for i in range(SLABS) if 0 <= i + steps < SLABS]
    return lax.ppermute(block, DEPTH, pairs)


def slope(pre):
    sig = jax.nn.sigmoid(pre)
    return sig * (1.0 + pre * (1.0 - sig))


def near_groups():
    far_class = [0, 1, 0, 1, 1, 0, 1, 0]
    groups = {}
    for place in range(SLABS):
        z, y, x = place // 32, place // 4 % 8, place % 4
        rank = (x * 2 + far_class[y]) * 2 + far_class[z]
        groups.setdefault((z // 2, y // 2), {})[rank] = place
    near = [[block[rank] for rank in range(16)] for block in groups.values()]
    far = [[block[rank] for block in groups.values()] for rank in range(16)]
    return near, far


NEAR, FAR = near_groups()


def band_kernel(scalars, w1, w2, t1, t1t, t2, t2t, rows_one):
    turn = scalars[0] * 16
    half = pl.multiple_of(turn, 16)

    def marks_of(width, lanes, sign, turn):
        row = lax.broadcasted_iota(jnp.int32, (3 * width, lanes), 0)
        lane = lax.broadcasted_iota(jnp.int32, (3 * width, lanes), 1)
        base = lane - (sign * (row // width - 1) * width + (row + turn) % width)
        return lambda h: jnp.where(base == h * width, 1.0, 0.0).astype(BF16)

    def taps_of(ref, flip):
        order = [(2 - a, 2 - c) if flip else (a, c) for a in range(3) for c in range(3)]
        return [[ref[9 * a + 3 * b + c] for b in range(3)] for a, c in order]

    def straight(ref, flip, marks, height, put):
        taps = taps_of(ref, flip)
        parts = [jnp.concatenate([tap[b] for tap in taps], axis=0) for b in range(3)]
        weights = jnp.concatenate(parts, axis=1)
        for h in range(height):
            put(h, jnp.dot(weights, marks(h), preferred_element_type=F32).astype(BF16))

    def crossed(ref, flip, marks, height, put):
        parts = [jnp.concatenate(tap, axis=0) for tap in taps_of(ref, flip)]
        weights = jnp.concatenate(parts, axis=1)
        for h in range(height):
            bands = lax.dot_general(
                weights, marks(h), (((0,), (0,)), ((), ())), preferred_element_type=F32
            )
            put(h, bands.astype(BF16))

    def into(out, rows, lanes):
        def put(h, bands):
            for tap in range(9):
                out[h * rows : (h + 1) * rows, tap * lanes : (tap + 1) * lanes] = bands[
                    tap * rows : (tap + 1) * rows
                ]

        return put

    def put_half(h, bands):
        rows_one[h] = bands
        for tap in range(9):
            t1t[h * 16 : (h + 1) * 16, tap * 256 : (tap + 1) * 256] = rows_one[
                h, pl.ds(tap * 32 + half, 16), :
            ]

    straight(w1, False, marks_of(32, 256, 1, turn), 8, into(t1, 32, 256))
    crossed(w1, True, marks_of(32, 256, -1, 0), 8, put_half)
    crossed(w2, False, marks_of(32, 128, 1, 0), 4, into(t2, 64, 128))
    straight(w2, True, marks_of(64, 256, -1, 0), 4, into(t2t, 32, 256))


def shifted(value, step):
    lanes = value.shape[-1]
    lane = lax.broadcasted_iota(jnp.int32, value.shape, 1)
    low = jnp.where(lane < step, 0.0, pltpu.roll(value, step, 1))
    high = jnp.where(lane >= lanes - step, 0.0, pltpu.roll(value, lanes - step, 1))
    return low.astype(BF16), value.astype(BF16), high.astype(BF16)


def main_kernel(
    scalars, own, oth, t1, t1t, t2, t2t, gf, wg, XP, PS, SL, QP, GP, HP, CT, FS, FP, G1, G2
):
    member = scalars[0]
    place = scalars[1]
    x = scalars[2]
    half = pl.multiple_of(member * 16, 16)

    def slot(delta):
        return lax.rem(x + delta + 4, 4)

    planes = [(slot(0), 0)]
    planes += [(slot(delta), 8 * p) for delta in (-3, -2, -1) for p in range(2)]
    planes += [(slot(0), 12), (slot(0), 20)]
    planes += [(slot(delta), 20 + 8 * p) for delta in (1, 2, 3) for p in range(2)]
    planes += [(slot(0), 32)]

    def load_plane(j):
        at, start = planes[j]
        plane = jnp.concatenate(
            [own[at, start : start + 8], oth[at, start : start + 8]], axis=1
        ).reshape(256, 128)
        for c, part in enumerate(shifted(plane.astype(F32), 1)):
            if j <= 8:
                XP[j, c, :, :128] = part
            if j >= 7:
                XP[j - 7, c, :, 128:] = part

    for j in (0, 1, 7, 8):
        load_plane(j)

    for k in range(7):
        for j in (k + 2, k + 9):
            if j not in (7, 8) and j < 16:
                load_plane(j)
        pre = jnp.dot(t1[...], XP[k : k + 3].reshape(2304, 256), preferred_element_type=F32)
        act = (pre * jax.nn.sigmoid(pre)).astype(BF16).astype(F32).reshape(4, 2, 32, 256)
        rows = (act[:, 0] + act[:, 1]).reshape(128, 256)
        PS[k] = rows[:, :128]
        PS[k + 7] = rows[:, 128:]
        if k >= 5:
            SL[k - 5] = slope(pre[:, :128])
        if k <= 1:
            SL[k + 2] = slope(pre[:, 128:])

    lane = lax.broadcasted_iota(jnp.int32, (128, 128), 1)
    even = lane % 2 == 0
    for c in range(3):
        QP[4, c, :, 128:] = jnp.zeros((128, 128), BF16)
    for j in range(7):
        total = PS[2 * j] + PS[2 * j + 1]
        total = total + jnp.where(even, pltpu.roll(total, 127, 1), pltpu.roll(total, 1, 1))
        at = place + (j - 3)
        factor = jnp.where((at >= 0) & (at < SLABS), 0.125, 0.0)
        pooled = (total * factor).astype(BF16).astype(F32)
        for c, part in enumerate(shifted(pooled, 2)):
            if j <= 4:
                QP[j, c, :, :128] = part
            if j >= 3:
                QP[j - 3, c, :, 128:] = part

    cots = [(slot(-2), 16), (slot(-1), 16), (slot(0), 28), (slot(1), 36), (slot(2), 36)]
    own_o = pl.multiple_of(member * 32, 32)
    oth_o = pl.multiple_of(32 - member * 32, 32)
    for e, (at, start) in enumerate(cots):
        for high in range(2):
            here = start + 2 * high
            CT[e, high, pl.ds(own_o, 32), :] = own[at, here : here + 2].reshape(32, 128)
            CT[e, high, pl.ds(oth_o, 32), :] = oth[at, here : here + 2].reshape(32, 128)
    row = lax.broadcasted_iota(jnp.int32, (128, 256), 0)
    col = lax.broadcasted_iota(jnp.int32, (128, 256), 1)
    spread = jnp.where(row == (col // 128) * 64 + (col % 128) // 2, 1.0, 0.0).astype(BF16)
    cot = jnp.dot(CT[...].reshape(640, 128), spread, preferred_element_type=F32)

    for e in range(3):
        pre_two = jnp.dot(t2[...], QP[e : e + 3].reshape(1152, 256), preferred_element_type=F32)
        slopes = slope(pre_two)
        for plane in (e, e + 3):
            if plane > 4:
                continue
            side = slopes[:, :128] if plane == e else slopes[:, 128:]
            base = plane * 128
            cots_of = jnp.concatenate(
                [
                    cot[base : base + 64, :128],
                    cot[base : base + 64, 128:],
                    cot[base + 64 : base + 128, :128],
                    cot[base + 64 : base + 128, 128:],
                ],
                axis=0,
            )
            grad = (cots_of * side).astype(BF16).astype(F32)
            for c, part in enumerate(shifted(grad, 2)):
                for m in range(3):
                    n = plane - m
                    if 0 <= n <= 2:
                        GP[m, c, :, n * 128 : (n + 1) * 128] = part
            if plane == 2:
                lanes = lax.broadcasted_iota(jnp.int32, (256, 128), 1)
                kept = jnp.where(lanes % 2 == 0, grad, 0.0).astype(BF16)
                G2[...] = jnp.zeros(G2.shape, BF16)
                for h in range(4):
                    G2[32:96, h * 128 : (h + 1) * 128] = kept[h * 64 : (h + 1) * 64]

    back = jnp.dot(t2t[...], GP[...].reshape(2304, 384), preferred_element_type=F32)
    G1[...] = jnp.zeros(G1.shape, BF16)
    for q, f in enumerate((0, 1, 1, 2)):
        at = place + (f - 1)
        factor = jnp.where((at >= 0) & (at < SLABS), 0.125, 0.0)
        part = (back[:, f * 128 : (f + 1) * 128] * factor).reshape(4, 1, 32, 128)
        wide = jnp.concatenate([part, part], axis=1).reshape(256, 128)
        grad = (wide * SL[q]).astype(BF16).astype(F32)
        for c, piece in enumerate(shifted(grad, 1)):
            if q <= 2:
                HP[q, c, :, :128] = piece
            if q >= 1:
                HP[q - 1, c, :, 128:] = piece
            if c == 1 and q in (1, 2):
                for h in range(8):
                    to = ((q - 1) * 8 + h) * 128
                    G1[0:32, to : to + 128] = piece[h * 32 : (h + 1) * 32]

    nothing = jnp.zeros((16, 128), BF16)
    for a in range(3):
        for b in range(3):
            for c in range(3):
                tap = (a * 3 + b) * 3 + c
                to = slice(tap * 16, tap * 16 + 16)
                for q in range(2):
                    j = 6 + a + q
                    m, side = (j, 0) if j <= 8 else (j - 7, 128)
                    for h in range(8):
                        at = h + b - 1
                        lanes = slice((q * 8 + h) * 128, (q * 8 + h + 1) * 128)
                        if 0 <= at < 8:
                            FS[to, lanes] = XP[m, c, at * 32 : at * 32 + 16, side : side + 128]
                        else:
                            FS[to, lanes] = nothing
                for h in range(4):
                    at = h + b - 1
                    lanes = slice(h * 128, (h + 1) * 128)
                    if 0 <= at < 4:
                        FP[to, lanes] = QP[2 + a, c, pl.ds(at * 32 + half, 16), :128]
                    else:
                        FP[to, lanes] = nothing
    along = (((1,), (1,)), ((), ()))
    wg[0:432] = lax.dot_general(
        FS[...], G1[...], along, preferred_element_type=F32
    ) + lax.dot_general(FP[...], G2[...], along, preferred_element_type=F32)
    wg[432:] = jnp.zeros((80, 128), F32)

    out = jnp.dot(t1t[...], HP[...].reshape(2304, 256), preferred_element_type=F32)
    for p in range(2):
        side = out[:, p * 128 : (p + 1) * 128].reshape(8, 16, 128)
        gf[:, p] = jnp.transpose(side, (1, 0, 2)).astype(BF16)


def band_weights(scalars, w1, w2):
    vmem = pl.BlockSpec(memory_space=pltpu.VMEM)
    shapes = [(256, 2304), (128, 2304), (256, 1152), (128, 2304)]
    return pl.pallas_call(
        band_kernel,
        in_specs=[pl.BlockSpec(memory_space=pltpu.SMEM)] + [vmem] * 2,
        out_specs=[vmem] * 4,
        scratch_shapes=[pltpu.VMEM((8, 288, 256), BF16)],
        out_shape=[jax.ShapeDtypeStruct(shape, BF16) for shape in shapes],
        cost_estimate=pl.CostEstimate(flops=10**9, bytes_accessed=4 * 10**6, transcendentals=0),
        compiler_params=pltpu.CompilerParams(vmem_limit_bytes=16 * 2**20),
        name="bands",
    )(scalars, w1, w2)


def levels(scalars, own, oth, bands):
    vmem = pl.BlockSpec(memory_space=pltpu.VMEM)
    scratch = [
        ((9, 3, 256, 256), BF16),
        ((14, 128, 128), F32),
        ((4, 256, 128), F32),
        ((5, 3, 128, 256), BF16),
        ((3, 3, 256, 384), BF16),
        ((3, 3, 256, 256), BF16),
        ((5, 2, 64, 128), BF16),
        ((432, 2048), BF16),
        ((432, 512), BF16),
        ((128, 2048), BF16),
        ((128, 512), BF16),
    ]
    return pl.pallas_call(
        main_kernel,
        in_specs=[pl.BlockSpec(memory_space=pltpu.SMEM)] + [vmem] * 6,
        out_specs=[vmem, vmem],
        out_shape=[
            jax.ShapeDtypeStruct((16, 2, 8, 128), BF16),
            jax.ShapeDtypeStruct((512, 128), F32),
        ],
        scratch_shapes=[pltpu.VMEM(shape, dtype) for shape, dtype in scratch],
        cost_estimate=pl.CostEstimate(
            flops=10**10, bytes_accessed=8 * 10**6, transcendentals=10**6
        ),
        compiler_params=pltpu.CompilerParams(vmem_limit_bytes=28 * 2**20),
        name="levels",
    )(scalars, own, oth, *bands)


def exchange(pieces, groups):
    return lax.all_to_all(pieces, DEPTH, 0, 0, axis_index_groups=groups, tiled=True)


def total_over_depth(part):
    near = jnp.sum(exchange(part.reshape(16, 32, 128), NEAR), axis=0)
    whole = jnp.sum(exchange(jnp.broadcast_to(near, (16, 32, 128)), FAR), axis=0)
    copies = jnp.broadcast_to(whole.astype(BF16), (16, 32, 128))
    return exchange(copies, NEAR)


def split_kernel(total, one, two):
    rows = total[...].reshape(512, 128)[:432].astype(F32)
    one[...] = rows[:, :32]
    two[...] = rows[:, 32:96]


def split_total(total):
    vmem = pl.BlockSpec(memory_space=pltpu.VMEM)
    return pl.pallas_call(
        split_kernel,
        in_specs=[vmem],
        out_specs=[vmem, vmem],
        out_shape=[
            jax.ShapeDtypeStruct((432, 32), F32),
            jax.ShapeDtypeStruct((432, 64), F32),
        ],
        compiler_params=pltpu.CompilerParams(vmem_limit_bytes=4 * 2**20),
        name="split",
    )(total)


def shards(feats, weight_one, weight_two, cotangent):
    member = lax.axis_index("chan")
    place = lax.axis_index(DEPTH)
    x = lax.axis_index("x")
    fields = jnp.transpose(feats, (1, 2, 0, 3)).reshape(16, 16, 128)
    cot = jnp.transpose(cotangent.reshape(32, 2, 2, 64), (1, 0, 2, 3)).reshape(4, 16, 128)
    block = jnp.concatenate([fields, cot], axis=0)
    up = depth_shift(block, ROW)
    down = depth_shift(block, -ROW)

    scalars = jnp.stack([member, place, x]).astype(jnp.int32)
    bands = band_weights(
        scalars,
        jnp.transpose(weight_one, (2, 0, 1)),
        jnp.transpose(weight_two, (2, 1, 0)),
    )

    three = jnp.concatenate([up, block, down], axis=0)
    slots = [
        lax.dynamic_slice_in_dim(
            three, jnp.where(x > t, 0, jnp.where(x == t, 8, 20)).astype(jnp.int32), 40, 0
        )
        for t in range(4)
    ]
    own = lax.all_to_all(jnp.stack(slots, 0), "x", 0, 0, tiled=True)
    oth = lax.ppermute(own, "chan", [(0, 1), (1, 0)])
    grad_feats, part = levels(scalars, own, oth, bands)
    one, two = split_total(total_over_depth(part))
    grad_weight_one = jnp.transpose(one.reshape(27, 16, 32), (2, 1, 0))
    grad_weight_two = jnp.transpose(two.reshape(27, 16, 64), (2, 1, 0))
    return (grad_feats, grad_weight_one, grad_weight_two)


def solution(mesh):
    finer = Mesh(
        mesh.devices.reshape(8, 8, 4, mesh.shape["chan"]), DEPTH + ("chan",)
    )
    in_specs = (P("chan", DEPTH, None, None), P(), P(), P("chan", DEPTH, None, None))
    out_specs = (P("chan", DEPTH, None, None), P(None, "chan", None), P(None, "chan", None))

    return jax.shard_map(
        shards, mesh=finer, in_specs=in_specs, out_specs=out_specs, check_vma=False
    )
```

```python
import jax
import jax.numpy as jnp
from jax import lax
from jax.experimental import pallas as pl
from jax.experimental.pallas import tpu as pltpu
from jax.sharding import Mesh
from jax.sharding import PartitionSpec as P


DEPTH = ("z", "y", "x")
SLABS = 256
ROW = 4
BF16 = jnp.bfloat16
F32 = jnp.float32


def depth_shift(block, steps):
    pairs = [(i, i + steps) for i in range(SLABS) if 0 <= i + steps < SLABS]
    return lax.ppermute(block, DEPTH, pairs)


def slope(pre):
    sig = jax.nn.sigmoid(pre)
    return sig * (1.0 + pre * (1.0 - sig))


def near_groups():
    far_class = [0, 1, 0, 1, 1, 0, 1, 0]
    groups = {}
    for place in range(SLABS):
        z, y, x = place // 32, place // 4 % 8, place % 4
        rank = (x * 2 + far_class[y]) * 2 + far_class[z]
        groups.setdefault((z // 2, y // 2), {})[rank] = place
    near = [[block[rank] for rank in range(16)] for block in groups.values()]
    far = [[block[rank] for block in groups.values()] for rank in range(16)]
    return near, far


NEAR, FAR = near_groups()


def position():
    place = (lax.axis_index("z") * 8 + lax.axis_index("y")) * 4 + lax.axis_index("x")
    return lax.axis_index("chan"), place


def gather_kernel(feats_far, cot_far, w1, w2, block, w1_near, w2_near, feats, cot, sems):
    pairs = ((feats_far, feats), (cot_far, cot), (w1, w1_near), (w2, w2_near))
    copies = [
        pltpu.make_async_copy(source, target, sems.at[index])
        for index, (source, target) in enumerate(pairs)
    ]
    for copy in copies:
        copy.start()
    copies[0].wait()
    for p in range(2):
        plane = jnp.transpose(feats[:, p].astype(F32), (1, 0, 2))
        block[p * 8 : (p + 1) * 8] = plane.astype(BF16)
    copies[1].wait()
    rows = jnp.transpose(cot[...].reshape(32, 4, 64).astype(F32), (1, 0, 2))
    for high in range(2):
        pair = jnp.concatenate([rows[2 * high], rows[2 * high + 1]], axis=1)
        block[16 + 2 * high : 18 + 2 * high] = pair.astype(BF16).reshape(2, 16, 128)
    for copy in copies[2:]:
        copy.wait()


def band_kernel(w1, w2, t1, t1t, t2, t2t, rows_one):
    turn = position()[0] * 16
    half = pl.multiple_of(turn, 16)

    def marks_of(width, lanes, sign, turn):
        row = lax.broadcasted_iota(jnp.int32, (3 * width, lanes), 0)
        lane = lax.broadcasted_iota(jnp.int32, (3 * width, lanes), 1)
        base = lane - (sign * (row // width - 1) * width + (row + turn) % width)
        return lambda h: jnp.where(base == h * width, 1.0, 0.0).astype(BF16)

    def taps_of(ref, flip):
        order = [(2 - a, 2 - c) if flip else (a, c) for a in range(3) for c in range(3)]
        return [[ref[9 * a + 3 * b + c] for b in range(3)] for a, c in order]

    def straight(ref, flip, marks, height, put):
        taps = taps_of(ref, flip)
        parts = [jnp.concatenate([tap[b] for tap in taps], axis=0) for b in range(3)]
        weights = jnp.concatenate(parts, axis=1)
        for h in range(height):
            put(h, jnp.dot(weights, marks(h), preferred_element_type=F32).astype(BF16))

    def crossed(ref, flip, marks, height, put):
        parts = [jnp.concatenate(tap, axis=0) for tap in taps_of(ref, flip)]
        weights = jnp.concatenate(parts, axis=1)
        for h in range(height):
            bands = lax.dot_general(
                weights, marks(h), (((0,), (0,)), ((), ())), preferred_element_type=F32
            )
            put(h, bands.astype(BF16))

    def into(out, rows, lanes):
        def put(h, bands):
            for tap in range(9):
                out[h * rows : (h + 1) * rows, tap * lanes : (tap + 1) * lanes] = bands[
                    tap * rows : (tap + 1) * rows
                ]

        return put

    def put_half(h, bands):
        rows_one[h] = bands
        for tap in range(9):
            t1t[h * 16 : (h + 1) * 16, tap * 256 : (tap + 1) * 256] = rows_one[
                h, pl.ds(tap * 32 + half, 16), :
            ]

    straight(w1, False, marks_of(32, 256, 1, turn), 8, into(t1, 32, 256))
    crossed(w1, True, marks_of(32, 256, -1, 0), 8, put_half)
    crossed(w2, False, marks_of(32, 128, 1, 0), 4, into(t2, 64, 128))
    straight(w2, True, marks_of(64, 256, -1, 0), 4, into(t2t, 32, 256))


def shifted(value, step):
    lanes = value.shape[-1]
    lane = lax.broadcasted_iota(jnp.int32, value.shape, 1)
    low = jnp.where(lane < step, 0.0, pltpu.roll(value, step, 1))
    high = jnp.where(lane >= lanes - step, 0.0, pltpu.roll(value, lanes - step, 1))
    return low.astype(BF16), value.astype(BF16), high.astype(BF16)


def main_kernel(
    own, oth, t1, t1t, t2, t2t, gf, wg, XP, PS, SL, QP, GP, HP, CT, FS, FP, G1, G2, GF, sem
):
    member, place = position()
    x = lax.rem(place, 4)
    half = pl.multiple_of(member * 16, 16)

    def slot(delta):
        return lax.rem(x + delta + 4, 4)

    planes = [(slot(0), 0)]
    planes += [(slot(delta), 8 * p) for delta in (-3, -2, -1) for p in range(2)]
    planes += [(slot(0), 12), (slot(0), 20)]
    planes += [(slot(delta), 20 + 8 * p) for delta in (1, 2, 3) for p in range(2)]
    planes += [(slot(0), 32)]

    def load_plane(j):
        at, start = planes[j]
        plane = jnp.concatenate(
            [own[at, start : start + 8], oth[at, start : start + 8]], axis=1
        ).reshape(256, 128)
        for c, part in enumerate(shifted(plane.astype(F32), 1)):
            if j <= 8:
                XP[j, c, :, :128] = part
            if j >= 7:
                XP[j - 7, c, :, 128:] = part

    for j in (0, 1, 7, 8):
        load_plane(j)

    for k in range(7):
        for j in (k + 2, k + 9):
            if j not in (7, 8) and j < 16:
                load_plane(j)
        pre = jnp.dot(t1[...], XP[k : k + 3].reshape(2304, 256), preferred_element_type=F32)
        act = (pre * jax.nn.sigmoid(pre)).astype(BF16).astype(F32).reshape(4, 2, 32, 256)
        rows = (act[:, 0] + act[:, 1]).reshape(128, 256)
        PS[k] = rows[:, :128]
        PS[k + 7] = rows[:, 128:]
        if k >= 5:
            SL[k - 5] = slope(pre[:, :128])
        if k <= 1:
            SL[k + 2] = slope(pre[:, 128:])

    lane = lax.broadcasted_iota(jnp.int32, (128, 128), 1)
    even = lane % 2 == 0
    for c in range(3):
        QP[4, c, :, 128:] = jnp.zeros((128, 128), BF16)
    for j in range(7):
        total = PS[2 * j] + PS[2 * j + 1]
        total = total + jnp.where(even, pltpu.roll(total, 127, 1), pltpu.roll(total, 1, 1))
        at = place + (j - 3)
        factor = jnp.where((at >= 0) & (at < SLABS), 0.125, 0.0)
        pooled = (total * factor).astype(BF16).astype(F32)
        for c, part in enumerate(shifted(pooled, 2)):
            if j <= 4:
                QP[j, c, :, :128] = part
            if j >= 3:
                QP[j - 3, c, :, 128:] = part

    cots = [(slot(-2), 16), (slot(-1), 16), (slot(0), 28), (slot(1), 36), (slot(2), 36)]
    own_o = pl.multiple_of(member * 32, 32)
    oth_o = pl.multiple_of(32 - member * 32, 32)
    for e, (at, start) in enumerate(cots):
        for high in range(2):
            here = start + 2 * high
            CT[e, high, pl.ds(own_o, 32), :] = own[at, here : here + 2].reshape(32, 128)
            CT[e, high, pl.ds(oth_o, 32), :] = oth[at, here : here + 2].reshape(32, 128)
    row = lax.broadcasted_iota(jnp.int32, (128, 256), 0)
    col = lax.broadcasted_iota(jnp.int32, (128, 256), 1)
    spread = jnp.where(row == (col // 128) * 64 + (col % 128) // 2, 1.0, 0.0).astype(BF16)
    cot = jnp.dot(CT[...].reshape(640, 128), spread, preferred_element_type=F32)

    for e in range(3):
        pre_two = jnp.dot(t2[...], QP[e : e + 3].reshape(1152, 256), preferred_element_type=F32)
        slopes = slope(pre_two)
        for plane in (e, e + 3):
            if plane > 4:
                continue
            side = slopes[:, :128] if plane == e else slopes[:, 128:]
            base = plane * 128
            cots_of = jnp.concatenate(
                [
                    cot[base : base + 64, :128],
                    cot[base : base + 64, 128:],
                    cot[base + 64 : base + 128, :128],
                    cot[base + 64 : base + 128, 128:],
                ],
                axis=0,
            )
            grad = (cots_of * side).astype(BF16).astype(F32)
            for c, part in enumerate(shifted(grad, 2)):
                for m in range(3):
                    n = plane - m
                    if 0 <= n <= 2:
                        GP[m, c, :, n * 128 : (n + 1) * 128] = part
            if plane == 2:
                lanes = lax.broadcasted_iota(jnp.int32, (256, 128), 1)
                kept = jnp.where(lanes % 2 == 0, grad, 0.0).astype(BF16)
                G2[...] = jnp.zeros(G2.shape, BF16)
                for h in range(4):
                    G2[32:96, h * 128 : (h + 1) * 128] = kept[h * 64 : (h + 1) * 64]

    back = jnp.dot(t2t[...], GP[...].reshape(2304, 384), preferred_element_type=F32)
    G1[...] = jnp.zeros(G1.shape, BF16)
    for q, f in enumerate((0, 1, 1, 2)):
        at = place + (f - 1)
        factor = jnp.where((at >= 0) & (at < SLABS), 0.125, 0.0)
        part = (back[:, f * 128 : (f + 1) * 128] * factor).reshape(4, 1, 32, 128)
        wide = jnp.concatenate([part, part], axis=1).reshape(256, 128)
        grad = (wide * SL[q]).astype(BF16).astype(F32)
        for c, piece in enumerate(shifted(grad, 1)):
            if q <= 2:
                HP[q, c, :, :128] = piece
            if q >= 1:
                HP[q - 1, c, :, 128:] = piece
            if c == 1 and q in (1, 2):
                for h in range(8):
                    to = ((q - 1) * 8 + h) * 128
                    G1[0:32, to : to + 128] = piece[h * 32 : (h + 1) * 32]

    out = jnp.dot(t1t[...], HP[...].reshape(2304, 256), preferred_element_type=F32)
    for p in range(2):
        side = out[:, p * 128 : (p + 1) * 128].reshape(8, 16, 128)
        GF[:, p] = jnp.transpose(side, (1, 0, 2)).astype(BF16)
    away = pltpu.make_async_copy(GF, gf, sem)
    away.start()

    nothing = jnp.zeros((16, 128), BF16)
    for a in range(3):
        for b in range(3):
            for c in range(3):
                tap = (a * 3 + b) * 3 + c
                to = slice(tap * 16, tap * 16 + 16)
                for q in range(2):
                    j = 6 + a + q
                    m, side = (j, 0) if j <= 8 else (j - 7, 128)
                    for h in range(8):
                        at = h + b - 1
                        lanes = slice((q * 8 + h) * 128, (q * 8 + h + 1) * 128)
                        if 0 <= at < 8:
                            FS[to, lanes] = XP[m, c, at * 32 : at * 32 + 16, side : side + 128]
                        else:
                            FS[to, lanes] = nothing
                for h in range(4):
                    at = h + b - 1
                    lanes = slice(h * 128, (h + 1) * 128)
                    if 0 <= at < 4:
                        FP[to, lanes] = QP[2 + a, c, pl.ds(at * 32 + half, 16), :128]
                    else:
                        FP[to, lanes] = nothing
    along = (((1,), (1,)), ((), ()))
    wg[0:432] = lax.dot_general(
        FS[...], G1[...], along, preferred_element_type=F32
    ) + lax.dot_general(FP[...], G2[...], along, preferred_element_type=F32)
    wg[432:] = jnp.zeros((80, 128), F32)
    away.wait()


def own_block(feats, cot, w1, w2):
    vmem = pl.BlockSpec(memory_space=pltpu.VMEM)
    hbm = pl.BlockSpec(memory_space=pltpu.MemorySpace.HBM)
    return pl.pallas_call(
        gather_kernel,
        in_specs=[hbm] * 4,
        out_specs=[vmem] * 3,
        out_shape=[
            jax.ShapeDtypeStruct((20, 16, 128), BF16),
            jax.ShapeDtypeStruct(w1.shape, BF16),
            jax.ShapeDtypeStruct(w2.shape, BF16),
        ],
        scratch_shapes=[
            pltpu.VMEM(feats.shape, BF16),
            pltpu.VMEM(cot.shape, BF16),
            pltpu.SemaphoreType.DMA((4,)),
        ],
        compiler_params=pltpu.CompilerParams(vmem_limit_bytes=4 * 2**20),
        name="gather",
    )(*[pltpu.with_memory_space_constraint(array, pltpu.HBM) for array in (feats, cot, w1, w2)])


def band_weights(w1, w2):
    vmem = pl.BlockSpec(memory_space=pltpu.VMEM)
    shapes = [(256, 2304), (128, 2304), (256, 1152), (128, 2304)]
    return pl.pallas_call(
        band_kernel,
        in_specs=[vmem] * 2,
        out_specs=[vmem] * 4,
        scratch_shapes=[pltpu.VMEM((8, 288, 256), BF16)],
        out_shape=[jax.ShapeDtypeStruct(shape, BF16) for shape in shapes],
        cost_estimate=pl.CostEstimate(flops=10**9, bytes_accessed=4 * 10**6, transcendentals=0),
        compiler_params=pltpu.CompilerParams(vmem_limit_bytes=16 * 2**20),
        name="bands",
    )(w1, w2)


def levels(own, oth, bands):
    vmem = pl.BlockSpec(memory_space=pltpu.VMEM)
    scratch = [
        ((9, 3, 256, 256), BF16),
        ((14, 128, 128), F32),
        ((4, 256, 128), F32),
        ((5, 3, 128, 256), BF16),
        ((3, 3, 256, 384), BF16),
        ((3, 3, 256, 256), BF16),
        ((5, 2, 64, 128), BF16),
        ((432, 2048), BF16),
        ((432, 512), BF16),
        ((128, 2048), BF16),
        ((128, 512), BF16),
        ((16, 2, 8, 128), BF16),
    ]
    return pl.pallas_call(
        main_kernel,
        in_specs=[vmem] * 6,
        out_specs=[pl.BlockSpec(memory_space=pl.ANY), vmem],
        out_shape=[
            jax.ShapeDtypeStruct((16, 2, 8, 128), BF16),
            jax.ShapeDtypeStruct((512, 128), F32),
        ],
        scratch_shapes=[pltpu.VMEM(shape, dtype) for shape, dtype in scratch]
        + [pltpu.SemaphoreType.DMA(())],
        cost_estimate=pl.CostEstimate(
            flops=10**10, bytes_accessed=8 * 10**6, transcendentals=10**6
        ),
        compiler_params=pltpu.CompilerParams(vmem_limit_bytes=28 * 2**20),
        name="levels",
    )(own, oth, *bands)


def exchange(pieces, groups):
    return lax.all_to_all(pieces, DEPTH, 0, 0, axis_index_groups=groups, tiled=True)


def total_over_depth(part):
    near = jnp.sum(exchange(part.reshape(16, 32, 128), NEAR), axis=0)
    whole = jnp.sum(exchange(jnp.broadcast_to(near, (16, 32, 128)), FAR), axis=0)
    copies = jnp.broadcast_to(whole.astype(BF16), (16, 32, 128))
    return exchange(copies, NEAR)


def split_kernel(total, one, two):
    rows = total[...].reshape(512, 128)[:432].astype(F32)
    one[...] = rows[:, :32]
    two[...] = rows[:, 32:96]


def split_total(total):
    vmem = pl.BlockSpec(memory_space=pltpu.VMEM)
    return pl.pallas_call(
        split_kernel,
        in_specs=[vmem],
        out_specs=[vmem, vmem],
        out_shape=[
            jax.ShapeDtypeStruct((432, 32), F32),
            jax.ShapeDtypeStruct((432, 64), F32),
        ],
        compiler_params=pltpu.CompilerParams(vmem_limit_bytes=4 * 2**20),
        name="split",
    )(total)


def shards(feats, weight_one, weight_two, cotangent):
    x = lax.axis_index("x")
    block, w1, w2 = own_block(
        feats,
        cotangent,
        jnp.transpose(weight_one, (2, 0, 1)),
        jnp.transpose(weight_two, (2, 1, 0)),
    )
    up = depth_shift(block, ROW)
    down = depth_shift(block, -ROW)

    bands = band_weights(w1, w2)

    three = jnp.concatenate([up, block, down], axis=0)
    slots = [
        lax.dynamic_slice_in_dim(
            three, jnp.where(x > t, 0, jnp.where(x == t, 8, 20)).astype(jnp.int32), 40, 0
        )
        for t in range(4)
    ]
    own = lax.all_to_all(jnp.stack(slots, 0), "x", 0, 0, tiled=True)
    oth = lax.ppermute(own, "chan", [(0, 1), (1, 0)])
    grad_feats, part = levels(own, oth, bands)
    one, two = split_total(total_over_depth(part))
    grad_weight_one = jnp.transpose(one.reshape(27, 16, 32), (2, 1, 0))
    grad_weight_two = jnp.transpose(two.reshape(27, 16, 64), (2, 1, 0))
    return (grad_feats, grad_weight_one, grad_weight_two)


def solution(mesh):
    finer = Mesh(
        mesh.devices.reshape(8, 8, 4, mesh.shape["chan"]), DEPTH + ("chan",)
    )
    in_specs = (P("chan", DEPTH, None, None), P(), P(), P("chan", DEPTH, None, None))
    out_specs = (P("chan", DEPTH, None, None), P(None, "chan", None), P(None, "chan", None))

    return jax.shard_map(
        shards, mesh=finer, in_specs=in_specs, out_specs=out_specs, check_vma=False
    )
```

```python
import jax
import jax.numpy as jnp
from jax import lax
from jax.experimental import pallas as pl
from jax.experimental.pallas import tpu as pltpu
from jax.sharding import Mesh
from jax.sharding import PartitionSpec as P


DEPTH = ("z", "y", "x")
SLABS = 256
ROW = 4
BF16 = jnp.bfloat16
F32 = jnp.float32


def depth_shift(block, steps):
    pairs = [(i, i + steps) for i in range(SLABS) if 0 <= i + steps < SLABS]
    return lax.ppermute(block, DEPTH, pairs)


def slope(pre):
    sig = jax.nn.sigmoid(pre)
    return sig * (1.0 + pre * (1.0 - sig))


def near_groups():
    far_class = [0, 1, 0, 1, 1, 0, 1, 0]
    groups = {}
    for place in range(SLABS):
        z, y, x = place // 32, place // 4 % 8, place % 4
        rank = (x * 2 + far_class[y]) * 2 + far_class[z]
        groups.setdefault((z // 2, y // 2), {})[rank] = place
    near = [[block[rank] for rank in range(16)] for block in groups.values()]
    far = [[block[rank] for block in groups.values()] for rank in range(16)]
    return near, far


NEAR, FAR = near_groups()


def position():
    place = (lax.axis_index("z") * 8 + lax.axis_index("y")) * 4 + lax.axis_index("x")
    return lax.axis_index("chan"), place


def gather_kernel(feats_far, cot_far, w1, w2, block, w1_near, w2_near, feats, cot, sems):
    pairs = ((feats_far, feats), (cot_far, cot), (w1, w1_near), (w2, w2_near))
    copies = [
        pltpu.make_async_copy(source, target, sems.at[index])
        for index, (source, target) in enumerate(pairs)
    ]
    for copy in copies:
        copy.start()
    copies[0].wait()
    for p in range(2):
        plane = jnp.transpose(feats[:, p].astype(F32), (1, 0, 2))
        block[p * 8 : (p + 1) * 8] = plane.astype(BF16)
    copies[1].wait()
    rows = jnp.transpose(cot[...].reshape(32, 4, 64).astype(F32), (1, 0, 2))
    for high in range(2):
        pair = jnp.concatenate([rows[2 * high], rows[2 * high + 1]], axis=1)
        block[16 + 2 * high : 18 + 2 * high] = pair.astype(BF16).reshape(2, 16, 128)
    for copy in copies[2:]:
        copy.wait()


def band_kernel(w1, w2, t1, t1t, t2, t2t, rows_one):
    turn = position()[0] * 16
    half = pl.multiple_of(turn, 16)

    def marks_of(width, lanes, sign, turn):
        row = lax.broadcasted_iota(jnp.int32, (3 * width, lanes), 0)
        lane = lax.broadcasted_iota(jnp.int32, (3 * width, lanes), 1)
        base = lane - (sign * (row // width - 1) * width + (row + turn) % width)
        return lambda h: jnp.where(base == h * width, 1.0, 0.0).astype(BF16)

    def taps_of(ref, flip):
        order = [(2 - a, 2 - c) if flip else (a, c) for a in range(3) for c in range(3)]
        return [[ref[9 * a + 3 * b + c] for b in range(3)] for a, c in order]

    def straight(ref, flip, marks, height, put):
        taps = taps_of(ref, flip)
        parts = [jnp.concatenate([tap[b] for tap in taps], axis=0) for b in range(3)]
        weights = jnp.concatenate(parts, axis=1)
        for h in range(height):
            put(h, jnp.dot(weights, marks(h), preferred_element_type=F32).astype(BF16))

    def crossed(ref, flip, marks, height, put):
        parts = [jnp.concatenate(tap, axis=0) for tap in taps_of(ref, flip)]
        weights = jnp.concatenate(parts, axis=1)
        for h in range(height):
            bands = lax.dot_general(
                weights, marks(h), (((0,), (0,)), ((), ())), preferred_element_type=F32
            )
            put(h, bands.astype(BF16))

    def into(out, rows, lanes):
        def put(h, bands):
            for tap in range(9):
                out[h * rows : (h + 1) * rows, tap * lanes : (tap + 1) * lanes] = bands[
                    tap * rows : (tap + 1) * rows
                ]

        return put

    def put_half(h, bands):
        rows_one[h] = bands
        for tap in range(9):
            t1t[h * 16 : (h + 1) * 16, tap * 256 : (tap + 1) * 256] = rows_one[
                h, pl.ds(tap * 32 + half, 16), :
            ]

    straight(w1, False, marks_of(32, 256, 1, turn), 8, into(t1, 32, 256))
    crossed(w1, True, marks_of(32, 256, -1, 0), 8, put_half)
    crossed(w2, False, marks_of(32, 128, 1, 0), 4, into(t2, 64, 128))
    straight(w2, True, marks_of(64, 256, -1, 0), 4, into(t2t, 32, 256))


def shifted(value, step):
    lanes = value.shape[-1]
    lane = lax.broadcasted_iota(jnp.int32, value.shape, 1)
    low = jnp.where(lane < step, 0.0, pltpu.roll(value, step, 1))
    high = jnp.where(lane >= lanes - step, 0.0, pltpu.roll(value, lanes - step, 1))
    return low.astype(BF16), value.astype(BF16), high.astype(BF16)


def main_kernel(
    own, oth, t1, t1t, t2, t2t, gf, wg, XP, PS, SL, QP, GP, HP, CT, FS, FP, G1, G2, GF, sem
):
    member, place = position()
    x = lax.rem(place, 4)
    half = pl.multiple_of(member * 16, 16)

    def slot(delta):
        return lax.rem(x + delta + 4, 4)

    planes = [(slot(0), 0)]
    planes += [(slot(delta), 8 * p) for delta in (-3, -2, -1) for p in range(2)]
    planes += [(slot(0), 12), (slot(0), 20)]
    planes += [(slot(delta), 20 + 8 * p) for delta in (1, 2, 3) for p in range(2)]
    planes += [(slot(0), 32)]

    def load_plane(j):
        at, start = planes[j]
        plane = jnp.concatenate(
            [own[at, start : start + 8], oth[at, start : start + 8]], axis=1
        ).reshape(256, 128)
        for c, part in enumerate(shifted(plane.astype(F32), 1)):
            if j <= 8:
                XP[j, c, :, :128] = part
            if j >= 7:
                XP[j - 7, c, :, 128:] = part

    for j in (0, 1, 7, 8):
        load_plane(j)

    for k in range(7):
        for j in (k + 2, k + 9):
            if j not in (7, 8) and j < 16:
                load_plane(j)
        pre = jnp.dot(t1[...], XP[k : k + 3].reshape(2304, 256), preferred_element_type=F32)
        act = (pre * jax.nn.sigmoid(pre)).astype(BF16).astype(F32).reshape(4, 2, 32, 256)
        rows = (act[:, 0] + act[:, 1]).reshape(128, 256)
        PS[k] = rows[:, :128]
        PS[k + 7] = rows[:, 128:]
        if k >= 5:
            SL[k - 5] = slope(pre[:, :128])
        if k <= 1:
            SL[k + 2] = slope(pre[:, 128:])

    lane = lax.broadcasted_iota(jnp.int32, (128, 128), 1)
    even = lane % 2 == 0
    for c in range(3):
        QP[4, c, :, 128:] = jnp.zeros((128, 128), BF16)
    for j in range(7):
        total = PS[2 * j] + PS[2 * j + 1]
        total = total + jnp.where(even, pltpu.roll(total, 127, 1), pltpu.roll(total, 1, 1))
        at = place + (j - 3)
        factor = jnp.where((at >= 0) & (at < SLABS), 0.125, 0.0)
        pooled = (total * factor).astype(BF16).astype(F32)
        for c, part in enumerate(shifted(pooled, 2)):
            if j <= 4:
                QP[j, c, :, :128] = part
            if j >= 3:
                QP[j - 3, c, :, 128:] = part

    cots = [(slot(-2), 16), (slot(-1), 16), (slot(0), 28), (slot(1), 36), (slot(2), 36)]
    own_o = pl.multiple_of(member * 32, 32)
    oth_o = pl.multiple_of(32 - member * 32, 32)
    for e, (at, start) in enumerate(cots):
        for high in range(2):
            here = start + 2 * high
            CT[e, high, pl.ds(own_o, 32), :] = own[at, here : here + 2].reshape(32, 128)
            CT[e, high, pl.ds(oth_o, 32), :] = oth[at, here : here + 2].reshape(32, 128)
    row = lax.broadcasted_iota(jnp.int32, (128, 256), 0)
    col = lax.broadcasted_iota(jnp.int32, (128, 256), 1)
    spread = jnp.where(row == (col // 128) * 64 + (col % 128) // 2, 1.0, 0.0).astype(BF16)
    cot = jnp.dot(CT[...].reshape(640, 128), spread, preferred_element_type=F32)

    for e in range(3):
        pre_two = jnp.dot(t2[...], QP[e : e + 3].reshape(1152, 256), preferred_element_type=F32)
        slopes = slope(pre_two)
        for plane in (e, e + 3):
            if plane > 4:
                continue
            side = slopes[:, :128] if plane == e else slopes[:, 128:]
            base = plane * 128
            cots_of = jnp.concatenate(
                [
                    cot[base : base + 64, :128],
                    cot[base : base + 64, 128:],
                    cot[base + 64 : base + 128, :128],
                    cot[base + 64 : base + 128, 128:],
                ],
                axis=0,
            )
            grad = (cots_of * side).astype(BF16).astype(F32)
            for c, part in enumerate(shifted(grad, 2)):
                for m in range(3):
                    n = plane - m
                    if 0 <= n <= 2:
                        GP[m, c, :, n * 128 : (n + 1) * 128] = part
            if plane == 2:
                lanes = lax.broadcasted_iota(jnp.int32, (256, 128), 1)
                kept = jnp.where(lanes % 2 == 0, grad, 0.0).astype(BF16)
                for b in range(3):
                    for at in range(4):
                        h = at + 1 - b
                        here = jnp.zeros((64, 128), BF16)
                        if 0 <= h < 4:
                            here = kept[h * 64 : (h + 1) * 64]
                        G2[b * 64 : (b + 1) * 64, at * 128 : (at + 1) * 128] = here

    back = jnp.dot(t2t[...], GP[...].reshape(2304, 384), preferred_element_type=F32)
    for q, f in enumerate((0, 1, 1, 2)):
        at = place + (f - 1)
        factor = jnp.where((at >= 0) & (at < SLABS), 0.125, 0.0)
        part = (back[:, f * 128 : (f + 1) * 128] * factor).reshape(4, 1, 32, 128)
        wide = jnp.concatenate([part, part], axis=1).reshape(256, 128)
        grad = (wide * SL[q]).astype(BF16).astype(F32)
        for c, piece in enumerate(shifted(grad, 1)):
            if q <= 2:
                HP[q, c, :, :128] = piece
            if q >= 1:
                HP[q - 1, c, :, 128:] = piece
            if c == 1 and q in (1, 2):
                for b in range(3):
                    for at in range(8):
                        h = at + 1 - b
                        here = jnp.zeros((32, 128), BF16)
                        if 0 <= h < 8:
                            here = piece[h * 32 : (h + 1) * 32]
                        to = (q - 1) * 128 + b * 32
                        G1[to : to + 32, at * 128 : (at + 1) * 128] = here
    for q in range(2):
        G1[q * 128 + 96 : q * 128 + 128] = jnp.zeros((32, 1024), BF16)

    out = jnp.dot(t1t[...], HP[...].reshape(2304, 256), preferred_element_type=F32)
    for p in range(2):
        side = out[:, p * 128 : (p + 1) * 128].reshape(8, 16, 128)
        GF[:, p] = jnp.transpose(side, (1, 0, 2)).astype(BF16)
    away = pltpu.make_async_copy(GF, gf, sem)
    away.start()

    for c in range(3):
        for j in range(4):
            m, side = (j + 6, 0) if j <= 2 else (2, 128)
            to = (j * 3 + c) * 16
            for h in range(8):
                FS[to : to + 16, h * 128 : (h + 1) * 128] = XP[
                    m, c, h * 32 : h * 32 + 16, side : side + 128
                ]
        for a in range(3):
            to = (a * 3 + c) * 16
            for h in range(4):
                FP[to : to + 16, h * 128 : (h + 1) * 128] = QP[
                    2 + a, c, pl.ds(h * 32 + half, 16), :128
                ]
    along = (((1,), (1,)), ((), ()))
    one = lax.dot_general(FS[...], G1[...], along, preferred_element_type=F32)
    two = lax.dot_general(FP[...], G2[...], along, preferred_element_type=F32)
    wg[0:144] = one[0:144, :128] + one[48:192, 128:]
    wg[144:288] = two[:, :128]
    wg[288:432, :64] = two[:, 128:]
    wg[288:432, 64:] = jnp.zeros((144, 64), F32)
    wg[432:] = jnp.zeros((80, 128), F32)
    away.wait()


def own_block(feats, cot, w1, w2):
    vmem = pl.BlockSpec(memory_space=pltpu.VMEM)
    hbm = pl.BlockSpec(memory_space=pltpu.MemorySpace.HBM)
    return pl.pallas_call(
        gather_kernel,
        in_specs=[hbm] * 4,
        out_specs=[vmem] * 3,
        out_shape=[
            jax.ShapeDtypeStruct((20, 16, 128), BF16),
            jax.ShapeDtypeStruct(w1.shape, BF16),
            jax.ShapeDtypeStruct(w2.shape, BF16),
        ],
        scratch_shapes=[
            pltpu.VMEM(feats.shape, BF16),
            pltpu.VMEM(cot.shape, BF16),
            pltpu.SemaphoreType.DMA((4,)),
        ],
        compiler_params=pltpu.CompilerParams(vmem_limit_bytes=4 * 2**20),
        name="gather",
    )(*[pltpu.with_memory_space_constraint(array, pltpu.HBM) for array in (feats, cot, w1, w2)])


def band_weights(w1, w2):
    vmem = pl.BlockSpec(memory_space=pltpu.VMEM)
    shapes = [(256, 2304), (128, 2304), (256, 1152), (128, 2304)]
    return pl.pallas_call(
        band_kernel,
        in_specs=[vmem] * 2,
        out_specs=[vmem] * 4,
        scratch_shapes=[pltpu.VMEM((8, 288, 256), BF16)],
        out_shape=[jax.ShapeDtypeStruct(shape, BF16) for shape in shapes],
        cost_estimate=pl.CostEstimate(flops=10**9, bytes_accessed=4 * 10**6, transcendentals=0),
        compiler_params=pltpu.CompilerParams(vmem_limit_bytes=16 * 2**20),
        name="bands",
    )(w1, w2)


def levels(own, oth, bands):
    vmem = pl.BlockSpec(memory_space=pltpu.VMEM)
    scratch = [
        ((9, 3, 256, 256), BF16),
        ((14, 128, 128), F32),
        ((4, 256, 128), F32),
        ((5, 3, 128, 256), BF16),
        ((3, 3, 256, 384), BF16),
        ((3, 3, 256, 256), BF16),
        ((5, 2, 64, 128), BF16),
        ((192, 1024), BF16),
        ((144, 512), BF16),
        ((256, 1024), BF16),
        ((192, 512), BF16),
        ((16, 2, 8, 128), BF16),
    ]
    return pl.pallas_call(
        main_kernel,
        in_specs=[vmem] * 6,
        out_specs=[pl.BlockSpec(memory_space=pl.ANY), vmem],
        out_shape=[
            jax.ShapeDtypeStruct((16, 2, 8, 128), BF16),
            jax.ShapeDtypeStruct((512, 128), F32),
        ],
        scratch_shapes=[pltpu.VMEM(shape, dtype) for shape, dtype in scratch]
        + [pltpu.SemaphoreType.DMA(())],
        cost_estimate=pl.CostEstimate(
            flops=10**10, bytes_accessed=8 * 10**6, transcendentals=10**6
        ),
        compiler_params=pltpu.CompilerParams(vmem_limit_bytes=28 * 2**20),
        name="levels",
    )(own, oth, *bands)


def exchange(pieces, groups):
    return lax.all_to_all(pieces, DEPTH, 0, 0, axis_index_groups=groups, tiled=True)


def total_over_depth(part):
    near = jnp.sum(exchange(part.reshape(16, 32, 128), NEAR), axis=0)
    whole = jnp.sum(exchange(jnp.broadcast_to(near, (16, 32, 128)), FAR), axis=0)
    copies = jnp.broadcast_to(whole.astype(BF16), (16, 32, 128))
    return exchange(copies, NEAR)


def split_kernel(total, one, two):
    rows = total[...].reshape(512, 128).astype(F32)
    for a in range(3):
        for c in range(3):
            at = (a * 3 + c) * 16
            first = rows[at : at + 16]
            second = jnp.concatenate(
                [rows[144 + at : 160 + at], rows[288 + at : 304 + at]], axis=1
            )
            for b in range(3):
                to = ((a * 3 + b) * 3 + c) * 16
                one[to : to + 16] = first[:, b * 32 : (b + 1) * 32]
                two[to : to + 16] = second[:, b * 64 : (b + 1) * 64]


def split_total(total):
    vmem = pl.BlockSpec(memory_space=pltpu.VMEM)
    return pl.pallas_call(
        split_kernel,
        in_specs=[vmem],
        out_specs=[vmem, vmem],
        out_shape=[
            jax.ShapeDtypeStruct((432, 32), F32),
            jax.ShapeDtypeStruct((432, 64), F32),
        ],
        compiler_params=pltpu.CompilerParams(vmem_limit_bytes=4 * 2**20),
        name="split",
    )(total)


def shards(feats, weight_one, weight_two, cotangent):
    x = lax.axis_index("x")
    block, w1, w2 = own_block(
        feats,
        cotangent,
        jnp.transpose(weight_one, (2, 0, 1)),
        jnp.transpose(weight_two, (2, 1, 0)),
    )
    up = depth_shift(block, ROW)
    down = depth_shift(block, -ROW)

    bands = band_weights(w1, w2)

    three = jnp.concatenate([up, block, down], axis=0)
    slots = [
        lax.dynamic_slice_in_dim(
            three, jnp.where(x > t, 0, jnp.where(x == t, 8, 20)).astype(jnp.int32), 40, 0
        )
        for t in range(4)
    ]
    own = lax.all_to_all(jnp.stack(slots, 0), "x", 0, 0, tiled=True)
    oth = lax.ppermute(own, "chan", [(0, 1), (1, 0)])
    grad_feats, part = levels(own, oth, bands)
    one, two = split_total(total_over_depth(part))
    grad_weight_one = jnp.transpose(one.reshape(27, 16, 32), (2, 1, 0))
    grad_weight_two = jnp.transpose(two.reshape(27, 16, 64), (2, 1, 0))
    return (grad_feats, grad_weight_one, grad_weight_two)


def solution(mesh):
    finer = Mesh(
        mesh.devices.reshape(8, 8, 4, mesh.shape["chan"]), DEPTH + ("chan",)
    )
    in_specs = (P("chan", DEPTH, None, None), P(), P(), P("chan", DEPTH, None, None))
    out_specs = (P("chan", DEPTH, None, None), P(None, "chan", None), P(None, "chan", None))

    return jax.shard_map(
        shards, mesh=finer, in_specs=in_specs, out_specs=out_specs, check_vma=False
    )
```

```python
import jax
import jax.numpy as jnp
from jax import lax
from jax.experimental import pallas as pl
from jax.experimental.pallas import tpu as pltpu
from jax.sharding import Mesh
from jax.sharding import PartitionSpec as P


DEPTH = ("z", "y", "x")
SLABS = 256
ROW = 4
BF16 = jnp.bfloat16
F32 = jnp.float32


def depth_shift(block, steps):
    pairs = [(i, i + steps) for i in range(SLABS) if 0 <= i + steps < SLABS]
    return lax.ppermute(block, DEPTH, pairs)


def slope(pre):
    sig = jax.nn.sigmoid(pre)
    return sig * (1.0 + pre * (1.0 - sig))


def near_groups():
    far_class = [0, 1, 0, 1, 1, 0, 1, 0]
    groups = {}
    for place in range(SLABS):
        z, y, x = place // 32, place // 4 % 8, place % 4
        rank = (x * 2 + far_class[y]) * 2 + far_class[z]
        groups.setdefault((z // 2, y // 2), {})[rank] = place
    near = [[block[rank] for rank in range(16)] for block in groups.values()]
    far = [[block[rank] for block in groups.values()] for rank in range(16)]
    return near, far


NEAR, FAR = near_groups()


def position():
    place = (lax.axis_index("z") * 8 + lax.axis_index("y")) * 4 + lax.axis_index("x")
    return lax.axis_index("chan"), place


def gather_kernel(feats_far, cot_far, w1, w2, block, w1_near, w2_near, feats, cot, sems):
    pairs = ((feats_far, feats), (cot_far, cot), (w1, w1_near), (w2, w2_near))
    copies = [
        pltpu.make_async_copy(source, target, sems.at[index])
        for index, (source, target) in enumerate(pairs)
    ]
    for copy in copies:
        copy.start()
    copies[0].wait()
    for p in range(2):
        plane = jnp.transpose(feats[:, p].astype(F32), (1, 0, 2))
        block[p * 8 : (p + 1) * 8] = plane.astype(BF16)
    copies[1].wait()
    rows = jnp.transpose(cot[...].reshape(32, 4, 64).astype(F32), (1, 0, 2))
    for high in range(2):
        pair = jnp.concatenate([rows[2 * high], rows[2 * high + 1]], axis=1)
        block[16 + 2 * high : 18 + 2 * high] = pair.astype(BF16).reshape(2, 16, 128)
    for copy in copies[2:]:
        copy.wait()


def band_kernel(w1, w2, t1, t1t, t2, t2t, rows_one):
    turn = position()[0] * 16
    half = pl.multiple_of(turn, 16)

    def marks_of(width, lanes, sign, turn):
        row = lax.broadcasted_iota(jnp.int32, (3 * width, lanes), 0)
        lane = lax.broadcasted_iota(jnp.int32, (3 * width, lanes), 1)
        base = lane - (sign * (row // width - 1) * width + (row + turn) % width)
        return lambda h: jnp.where(base == h * width, 1.0, 0.0).astype(BF16)

    def taps_of(ref, flip):
        order = [(2 - a, 2 - c) if flip else (a, c) for a in range(3) for c in range(3)]
        return [[ref[9 * a + 3 * b + c] for b in range(3)] for a, c in order]

    def straight(ref, flip, marks, height, put):
        taps = taps_of(ref, flip)
        parts = [jnp.concatenate([tap[b] for tap in taps], axis=0) for b in range(3)]
        weights = jnp.concatenate(parts, axis=1)
        for h in range(height):
            put(h, jnp.dot(weights, marks(h), preferred_element_type=F32).astype(BF16))

    def crossed(ref, flip, marks, height, put):
        parts = [jnp.concatenate(tap, axis=0) for tap in taps_of(ref, flip)]
        weights = jnp.concatenate(parts, axis=1)
        for h in range(height):
            bands = lax.dot_general(
                weights, marks(h), (((0,), (0,)), ((), ())), preferred_element_type=F32
            )
            put(h, bands.astype(BF16))

    def into(out, rows, lanes):
        def put(h, bands):
            for tap in range(9):
                out[h * rows : (h + 1) * rows, tap * lanes : (tap + 1) * lanes] = bands[
                    tap * rows : (tap + 1) * rows
                ]

        return put

    def put_half(h, bands):
        rows_one[h] = bands
        for tap in range(9):
            t1t[h * 16 : (h + 1) * 16, tap * 256 : (tap + 1) * 256] = rows_one[
                h, pl.ds(tap * 32 + half, 16), :
            ]

    straight(w1, False, marks_of(32, 256, 1, turn), 8, into(t1, 32, 256))
    crossed(w1, True, marks_of(32, 256, -1, 0), 8, put_half)
    crossed(w2, False, marks_of(32, 128, 1, 0), 4, into(t2, 64, 128))
    straight(w2, True, marks_of(64, 256, -1, 0), 4, into(t2t, 32, 256))


def shifted(value, step):
    lanes = value.shape[-1]
    lane = lax.broadcasted_iota(jnp.int32, value.shape, 1)
    low = jnp.where(lane < step, 0.0, pltpu.roll(value, step, 1))
    high = jnp.where(lane >= lanes - step, 0.0, pltpu.roll(value, lanes - step, 1))
    return low.astype(BF16), value.astype(BF16), high.astype(BF16)


def main_kernel(
    own, oth, t1, t1t, t2, t2t, gf, wg, XP, PS, SL, QP, GP, HP, CT, FS, FP, G1, G2
):
    member, place = position()
    x = lax.rem(place, 4)
    half = pl.multiple_of(member * 16, 16)

    def slot(delta):
        return lax.rem(x + delta + 4, 4)

    planes = [(slot(0), 0)]
    planes += [(slot(delta), 8 * p) for delta in (-3, -2, -1) for p in range(2)]
    planes += [(slot(0), 12), (slot(0), 20)]
    planes += [(slot(delta), 20 + 8 * p) for delta in (1, 2, 3) for p in range(2)]
    planes += [(slot(0), 32)]

    def load_plane(j):
        at, start = planes[j]
        plane = jnp.concatenate(
            [own[at, start : start + 8], oth[at, start : start + 8]], axis=1
        ).reshape(256, 128)
        for c, part in enumerate(shifted(plane.astype(F32), 1)):
            if j <= 8:
                XP[j, c, :, :128] = part
            if j >= 7:
                XP[j - 7, c, :, 128:] = part

    for j in (0, 1, 7, 8):
        load_plane(j)

    for k in range(7):
        for j in (k + 2, k + 9):
            if j not in (7, 8) and j < 16:
                load_plane(j)
        pre = jnp.dot(t1[...], XP[k : k + 3].reshape(2304, 256), preferred_element_type=F32)
        act = (pre * jax.nn.sigmoid(pre)).astype(BF16).astype(F32).reshape(4, 2, 32, 256)
        rows = (act[:, 0] + act[:, 1]).reshape(128, 256)
        PS[k] = rows[:, :128]
        PS[k + 7] = rows[:, 128:]
        if k >= 5:
            SL[k - 5] = slope(pre[:, :128])
        if k <= 1:
            SL[k + 2] = slope(pre[:, 128:])

    lane = lax.broadcasted_iota(jnp.int32, (128, 128), 1)
    even = lane % 2 == 0
    for c in range(3):
        QP[4, c, :, 128:] = jnp.zeros((128, 128), BF16)
    for j in range(7):
        total = PS[2 * j] + PS[2 * j + 1]
        total = total + jnp.where(even, pltpu.roll(total, 127, 1), pltpu.roll(total, 1, 1))
        at = place + (j - 3)
        factor = jnp.where((at >= 0) & (at < SLABS), 0.125, 0.0)
        pooled = (total * factor).astype(BF16).astype(F32)
        for c, part in enumerate(shifted(pooled, 2)):
            if j <= 4:
                QP[j, c, :, :128] = part
            if j >= 3:
                QP[j - 3, c, :, 128:] = part

    cots = [(slot(-2), 16), (slot(-1), 16), (slot(0), 28), (slot(1), 36), (slot(2), 36)]
    own_o = pl.multiple_of(member * 32, 32)
    oth_o = pl.multiple_of(32 - member * 32, 32)
    for e, (at, start) in enumerate(cots):
        for high in range(2):
            here = start + 2 * high
            CT[e, high, pl.ds(own_o, 32), :] = own[at, here : here + 2].reshape(32, 128)
            CT[e, high, pl.ds(oth_o, 32), :] = oth[at, here : here + 2].reshape(32, 128)
    row = lax.broadcasted_iota(jnp.int32, (128, 256), 0)
    col = lax.broadcasted_iota(jnp.int32, (128, 256), 1)
    spread = jnp.where(row == (col // 128) * 64 + (col % 128) // 2, 1.0, 0.0).astype(BF16)
    cot = jnp.dot(CT[...].reshape(640, 128), spread, preferred_element_type=F32)

    for e in range(3):
        pre_two = jnp.dot(t2[...], QP[e : e + 3].reshape(1152, 256), preferred_element_type=F32)
        slopes = slope(pre_two)
        for plane in (e, e + 3):
            if plane > 4:
                continue
            side = slopes[:, :128] if plane == e else slopes[:, 128:]
            base = plane * 128
            cots_of = jnp.concatenate(
                [
                    cot[base : base + 64, :128],
                    cot[base : base + 64, 128:],
                    cot[base + 64 : base + 128, :128],
                    cot[base + 64 : base + 128, 128:],
                ],
                axis=0,
            )
            grad = (cots_of * side).astype(BF16).astype(F32)
            for c, part in enumerate(shifted(grad, 2)):
                for m in range(3):
                    n = plane - m
                    if 0 <= n <= 2:
                        GP[m, c, :, n * 128 : (n + 1) * 128] = part
            if plane == 2:
                lanes = lax.broadcasted_iota(jnp.int32, (256, 128), 1)
                kept = jnp.where(lanes % 2 == 0, grad, 0.0).astype(BF16)
                for b in range(3):
                    for at in range(4):
                        h = at + 1 - b
                        here = jnp.zeros((64, 128), BF16)
                        if 0 <= h < 4:
                            here = kept[h * 64 : (h + 1) * 64]
                        G2[b * 64 : (b + 1) * 64, at * 128 : (at + 1) * 128] = here

    back = jnp.dot(t2t[...], GP[...].reshape(2304, 384), preferred_element_type=F32)
    for q, f in enumerate((0, 1, 1, 2)):
        at = place + (f - 1)
        factor = jnp.where((at >= 0) & (at < SLABS), 0.125, 0.0)
        part = (back[:, f * 128 : (f + 1) * 128] * factor).reshape(4, 1, 32, 128)
        wide = jnp.concatenate([part, part], axis=1).reshape(256, 128)
        grad = (wide * SL[q]).astype(BF16).astype(F32)
        for c, piece in enumerate(shifted(grad, 1)):
            if q <= 2:
                HP[q, c, :, :128] = piece
            if q >= 1:
                HP[q - 1, c, :, 128:] = piece
            if c == 1 and q in (1, 2):
                for b in range(3):
                    for at in range(8):
                        h = at + 1 - b
                        here = jnp.zeros((32, 128), BF16)
                        if 0 <= h < 8:
                            here = piece[h * 32 : (h + 1) * 32]
                        to = (q - 1) * 128 + (64, 96, 0)[b]
                        G1[to : to + 32, at * 128 : (at + 1) * 128] = here
    for q in range(2):
        G1[q * 128 + 32 : q * 128 + 64] = jnp.zeros((32, 1024), BF16)

    out = jnp.dot(t1t[...], HP[...].reshape(2304, 256), preferred_element_type=F32)
    for p in range(2):
        side = out[:, p * 128 : (p + 1) * 128].reshape(8, 16, 128)
        gf[:, p] = jnp.transpose(side, (1, 0, 2)).astype(BF16)

    for c in range(3):
        for j in range(4):
            m, side = (j + 6, 0) if j <= 2 else (2, 128)
            to = (j * 3 + c) * 16
            for h in range(8):
                FS[to : to + 16, h * 128 : (h + 1) * 128] = XP[
                    m, c, h * 32 : h * 32 + 16, side : side + 128
                ]
        for a in range(3):
            to = (a * 3 + c) * 16
            for h in range(4):
                FP[to : to + 16, h * 128 : (h + 1) * 128] = QP[
                    2 + a, c, pl.ds(h * 32 + half, 16), :128
                ]
    along = (((1,), (1,)), ((), ()))
    one = lax.dot_general(FS[...], G1[...], along, preferred_element_type=F32)
    two = lax.dot_general(FP[...], G2[...], along, preferred_element_type=F32)
    one = one[0:144, :128] + one[48:192, 128:]
    wg[0:144] = jnp.concatenate([two[:, 128:], one[:, 64:]], axis=1)
    wg[144:288] = two[:, :128]
    thirds = [one[at : at + 48, :32] for at in (0, 48, 96)]
    wg[288:336] = jnp.concatenate(thirds + [jnp.zeros((48, 32), F32)], axis=1)
    wg[336:] = jnp.zeros((48, 128), F32)


def own_block(feats, cot, w1, w2):
    vmem = pl.BlockSpec(memory_space=pltpu.VMEM)
    hbm = pl.BlockSpec(memory_space=pltpu.MemorySpace.HBM)
    return pl.pallas_call(
        gather_kernel,
        in_specs=[hbm] * 4,
        out_specs=[vmem] * 3,
        out_shape=[
            jax.ShapeDtypeStruct((20, 16, 128), BF16),
            jax.ShapeDtypeStruct(w1.shape, BF16),
            jax.ShapeDtypeStruct(w2.shape, BF16),
        ],
        scratch_shapes=[
            pltpu.VMEM(feats.shape, BF16),
            pltpu.VMEM(cot.shape, BF16),
            pltpu.SemaphoreType.DMA((4,)),
        ],
        compiler_params=pltpu.CompilerParams(vmem_limit_bytes=4 * 2**20),
        name="gather",
    )(*[pltpu.with_memory_space_constraint(array, pltpu.HBM) for array in (feats, cot, w1, w2)])


def band_weights(w1, w2):
    vmem = pl.BlockSpec(memory_space=pltpu.VMEM)
    shapes = [(256, 2304), (128, 2304), (256, 1152), (128, 2304)]
    return pl.pallas_call(
        band_kernel,
        in_specs=[vmem] * 2,
        out_specs=[vmem] * 4,
        scratch_shapes=[pltpu.VMEM((8, 288, 256), BF16)],
        out_shape=[jax.ShapeDtypeStruct(shape, BF16) for shape in shapes],
        cost_estimate=pl.CostEstimate(flops=10**9, bytes_accessed=4 * 10**6, transcendentals=0),
        compiler_params=pltpu.CompilerParams(vmem_limit_bytes=16 * 2**20),
        name="bands",
    )(w1, w2)


def levels(own, oth, bands):
    vmem = pl.BlockSpec(memory_space=pltpu.VMEM)
    scratch = [
        ((9, 3, 256, 256), BF16),
        ((14, 128, 128), F32),
        ((4, 256, 128), F32),
        ((5, 3, 128, 256), BF16),
        ((3, 3, 256, 384), BF16),
        ((3, 3, 256, 256), BF16),
        ((5, 2, 64, 128), BF16),
        ((192, 1024), BF16),
        ((144, 512), BF16),
        ((256, 1024), BF16),
        ((192, 512), BF16),
    ]
    return pl.pallas_call(
        main_kernel,
        in_specs=[vmem] * 6,
        out_specs=[vmem, vmem],
        out_shape=[
            jax.ShapeDtypeStruct((16, 2, 8, 128), BF16),
            jax.ShapeDtypeStruct((384, 128), F32),
        ],
        scratch_shapes=[pltpu.VMEM(shape, dtype) for shape, dtype in scratch],
        cost_estimate=pl.CostEstimate(
            flops=10**10, bytes_accessed=8 * 10**6, transcendentals=10**6
        ),
        compiler_params=pltpu.CompilerParams(vmem_limit_bytes=28 * 2**20),
        name="levels",
    )(own, oth, *bands)


def exchange(pieces, groups):
    return lax.all_to_all(pieces, DEPTH, 0, 0, axis_index_groups=groups, tiled=True)


def total_over_depth(part):
    near = jnp.sum(exchange(part.reshape(16, 24, 128), NEAR), axis=0)
    whole = jnp.sum(exchange(jnp.broadcast_to(near, (16, 24, 128)), FAR), axis=0)
    copies = jnp.broadcast_to(whole.astype(BF16), (16, 24, 128))
    return exchange(copies, NEAR)


def split_kernel(total, gf, one, two, gf_out, sem):
    away = pltpu.make_async_copy(gf, gf_out, sem)
    away.start()
    rows = total[...].reshape(384, 128).astype(F32)
    for a in range(3):
        for c in range(3):
            at = (a * 3 + c) * 16
            first, second = rows[at : at + 16], rows[144 + at : 160 + at]
            rest = rows[288 + at % 48 : 304 + at % 48]
            third = at // 48 * 32
            ones = (first[:, 64:96], first[:, 96:], rest[:, third : third + 32])
            twos = (second[:, :64], second[:, 64:], first[:, :64])
            for b in range(3):
                to = ((a * 3 + b) * 3 + c) * 16
                one[to : to + 16] = ones[b]
                two[to : to + 16] = twos[b]
    away.wait()


def split_total(total, gf):
    vmem = pl.BlockSpec(memory_space=pltpu.VMEM)
    return pl.pallas_call(
        split_kernel,
        in_specs=[vmem, vmem],
        out_specs=[vmem, vmem, pl.BlockSpec(memory_space=pl.ANY)],
        out_shape=[
            jax.ShapeDtypeStruct((432, 32), F32),
            jax.ShapeDtypeStruct((432, 64), F32),
            jax.ShapeDtypeStruct(gf.shape, BF16),
        ],
        scratch_shapes=[pltpu.SemaphoreType.DMA(())],
        compiler_params=pltpu.CompilerParams(vmem_limit_bytes=4 * 2**20),
        name="split",
    )(total, gf)


def shards(feats, weight_one, weight_two, cotangent):
    x = lax.axis_index("x")
    block, w1, w2 = own_block(
        feats,
        cotangent,
        jnp.transpose(weight_one, (2, 0, 1)),
        jnp.transpose(weight_two, (2, 1, 0)),
    )
    up = depth_shift(block, ROW)
    down = depth_shift(block, -ROW)

    bands = band_weights(w1, w2)

    three = jnp.concatenate([up, block, down], axis=0)
    slots = [
        lax.dynamic_slice_in_dim(
            three, jnp.where(x > t, 0, jnp.where(x == t, 8, 20)).astype(jnp.int32), 40, 0
        )
        for t in range(4)
    ]
    own = lax.all_to_all(jnp.stack(slots, 0), "x", 0, 0, tiled=True)
    oth = lax.ppermute(own, "chan", [(0, 1), (1, 0)])
    grad_feats, part = levels(own, oth, bands)
    one, two, grad_feats = split_total(total_over_depth(part), grad_feats)
    grad_weight_one = jnp.transpose(one.reshape(27, 16, 32), (2, 1, 0))
    grad_weight_two = jnp.transpose(two.reshape(27, 16, 64), (2, 1, 0))
    return (grad_feats, grad_weight_one, grad_weight_two)


def solution(mesh):
    finer = Mesh(
        mesh.devices.reshape(8, 8, 4, mesh.shape["chan"]), DEPTH + ("chan",)
    )
    in_specs = (P("chan", DEPTH, None, None), P(), P(), P("chan", DEPTH, None, None))
    out_specs = (P("chan", DEPTH, None, None), P(None, "chan", None), P(None, "chan", None))

    return jax.shard_map(
        shards, mesh=finer, in_specs=in_specs, out_specs=out_specs, check_vma=False
    )
```

```python
import jax
import jax.numpy as jnp
from jax import lax
from jax.experimental import pallas as pl
from jax.experimental.pallas import tpu as pltpu
from jax.sharding import Mesh
from jax.sharding import PartitionSpec as P


DEPTH = ("z", "y", "x")
SLABS = 256
ROW = 4
BF16 = jnp.bfloat16
F32 = jnp.float32


def depth_shift(block, steps):
    pairs = [(i, i + steps) for i in range(SLABS) if 0 <= i + steps < SLABS]
    return lax.ppermute(block, DEPTH, pairs)


def slope(pre):
    sig = jax.nn.sigmoid(pre)
    return sig * (1.0 + pre * (1.0 - sig))


def near_groups():
    far_class = [0, 1, 0, 1, 1, 0, 1, 0]
    groups = {}
    for place in range(SLABS):
        z, y, x = place // 32, place // 4 % 8, place % 4
        rank = (x * 2 + far_class[y]) * 2 + far_class[z]
        groups.setdefault((z // 2, y // 2), {})[rank] = place
    near = [[block[rank] for rank in range(16)] for block in groups.values()]
    far = [[block[rank] for block in groups.values()] for rank in range(16)]
    return near, far


NEAR, FAR = near_groups()


def position():
    place = (lax.axis_index("z") * 8 + lax.axis_index("y")) * 4 + lax.axis_index("x")
    return lax.axis_index("chan"), place


def gather_kernel(feats_far, cot_far, w1, w2, block, w1_near, w2_near, feats, cot, sems):
    pairs = ((feats_far, feats), (cot_far, cot), (w1, w1_near), (w2, w2_near))
    copies = [
        pltpu.make_async_copy(source, target, sems.at[index])
        for index, (source, target) in enumerate(pairs)
    ]
    for copy in copies:
        copy.start()
    copies[0].wait()
    for p in range(2):
        plane = jnp.transpose(feats[:, p].astype(F32), (1, 0, 2))
        block[p * 8 : (p + 1) * 8] = plane.astype(BF16)
    copies[1].wait()
    rows = jnp.transpose(cot[...].reshape(32, 4, 64).astype(F32), (1, 0, 2))
    for high in range(2):
        pair = jnp.concatenate([rows[2 * high], rows[2 * high + 1]], axis=1)
        block[16 + 2 * high : 18 + 2 * high] = pair.astype(BF16).reshape(2, 16, 128)
    for copy in copies[2:]:
        copy.wait()


def band_kernel(w1, w2, t1, t1t, t2, t2t, rows_one):
    turn = position()[0] * 16
    half = pl.multiple_of(turn, 16)

    def marks_of(width, lanes, sign, turn):
        row = lax.broadcasted_iota(jnp.int32, (3 * width, lanes), 0)
        lane = lax.broadcasted_iota(jnp.int32, (3 * width, lanes), 1)
        base = lane - (sign * (row // width - 1) * width + (row + turn) % width)
        return lambda h: jnp.where(base == h * width, 1.0, 0.0).astype(BF16)

    def taps_of(ref, flip):
        order = [(2 - a, 2 - c) if flip else (a, c) for a in range(3) for c in range(3)]
        return [[ref[9 * a + 3 * b + c] for b in range(3)] for a, c in order]

    def straight(ref, flip, marks, height, put):
        taps = taps_of(ref, flip)
        parts = [jnp.concatenate([tap[b] for tap in taps], axis=0) for b in range(3)]
        weights = jnp.concatenate(parts, axis=1)
        for h in range(height):
            put(h, jnp.dot(weights, marks(h), preferred_element_type=F32).astype(BF16))

    def crossed(ref, flip, marks, height, put):
        parts = [jnp.concatenate(tap, axis=0) for tap in taps_of(ref, flip)]
        weights = jnp.concatenate(parts, axis=1)
        for h in range(height):
            bands = lax.dot_general(
                weights, marks(h), (((0,), (0,)), ((), ())), preferred_element_type=F32
            )
            put(h, bands.astype(BF16))

    def into(out, rows, lanes):
        def put(h, bands):
            for tap in range(9):
                out[h * rows : (h + 1) * rows, tap * lanes : (tap + 1) * lanes] = bands[
                    tap * rows : (tap + 1) * rows
                ]

        return put

    def put_half(h, bands):
        rows_one[h] = bands
        for tap in range(9):
            t1t[h * 16 : (h + 1) * 16, tap * 256 : (tap + 1) * 256] = rows_one[
                h, pl.ds(tap * 32 + half, 16), :
            ]

    straight(w1, False, marks_of(32, 256, 1, turn), 8, into(t1, 32, 256))
    crossed(w1, True, marks_of(32, 256, -1, 0), 8, put_half)
    crossed(w2, False, marks_of(32, 128, 1, 0), 4, into(t2, 64, 128))
    straight(w2, True, marks_of(64, 256, -1, 0), 4, into(t2t, 32, 256))


def shifted(value, step):
    lanes = value.shape[-1]
    lane = lax.broadcasted_iota(jnp.int32, value.shape, 1)
    low = jnp.where(lane < step, 0.0, pltpu.roll(value, step, 1))
    high = jnp.where(lane >= lanes - step, 0.0, pltpu.roll(value, lanes - step, 1))
    return low.astype(BF16), value.astype(BF16), high.astype(BF16)


def main_kernel(
    own, oth, t1, t1t, t2, t2t, gf, wg, XP, PS, SL, QP, GP, HP, CT, FS, FP, G1, G2
):
    member, place = position()
    x = lax.rem(place, 4)
    half = pl.multiple_of(member * 16, 16)

    def slot(delta):
        return lax.rem(x + delta + 4, 4)

    planes = [(slot(0), 0)]
    planes += [(slot(delta), 8 * p) for delta in (-3, -2, -1) for p in range(2)]
    planes += [(slot(0), 12), (slot(0), 20)]
    planes += [(slot(delta), 20 + 8 * p) for delta in (1, 2, 3) for p in range(2)]
    planes += [(slot(0), 32)]

    def load_plane(j):
        at, start = planes[j]
        plane = jnp.concatenate(
            [own[at, start : start + 8], oth[at, start : start + 8]], axis=1
        ).reshape(256, 128)
        for c, part in enumerate(shifted(plane.astype(F32), 1)):
            if j <= 8:
                XP[j, c, :, :128] = part
            if j >= 7:
                XP[j - 7, c, :, 128:] = part

    for j in (0, 1, 7, 8):
        load_plane(j)

    for k in range(7):
        for j in (k + 2, k + 9):
            if j not in (7, 8) and j < 16:
                load_plane(j)
        pre = jnp.dot(t1[...], XP[k : k + 3].reshape(2304, 256), preferred_element_type=F32)
        act = (pre * jax.nn.sigmoid(pre)).astype(BF16).astype(F32).reshape(4, 2, 32, 256)
        rows = (act[:, 0] + act[:, 1]).reshape(128, 256)
        PS[k] = rows[:, :128]
        PS[k + 7] = rows[:, 128:]
        if k >= 5:
            SL[k - 5] = slope(pre[:, :128])
        if k <= 1:
            SL[k + 2] = slope(pre[:, 128:])

    lane = lax.broadcasted_iota(jnp.int32, (128, 128), 1)
    even = lane % 2 == 0
    for c in range(3):
        QP[4, c, :, 128:] = jnp.zeros((128, 128), BF16)
    for j in range(7):
        total = PS[2 * j] + PS[2 * j + 1]
        total = total + jnp.where(even, pltpu.roll(total, 127, 1), pltpu.roll(total, 1, 1))
        at = place + (j - 3)
        factor = jnp.where((at >= 0) & (at < SLABS), 0.125, 0.0)
        pooled = (total * factor).astype(BF16).astype(F32)
        for c, part in enumerate(shifted(pooled, 2)):
            if j <= 4:
                QP[j, c, :, :128] = part
            if j >= 3:
                QP[j - 3, c, :, 128:] = part

    cots = [(slot(-2), 16), (slot(-1), 16), (slot(0), 28), (slot(1), 36), (slot(2), 36)]
    own_o = pl.multiple_of(member * 32, 32)
    oth_o = pl.multiple_of(32 - member * 32, 32)
    for e, (at, start) in enumerate(cots):
        for high in range(2):
            here = start + 2 * high
            CT[e, high, pl.ds(own_o, 32), :] = own[at, here : here + 2].reshape(32, 128)
            CT[e, high, pl.ds(oth_o, 32), :] = oth[at, here : here + 2].reshape(32, 128)
    row = lax.broadcasted_iota(jnp.int32, (128, 256), 0)
    col = lax.broadcasted_iota(jnp.int32, (128, 256), 1)
    spread = jnp.where(row == (col // 128) * 64 + (col % 128) // 2, 1.0, 0.0).astype(BF16)
    cot = jnp.dot(CT[...].reshape(640, 128), spread, preferred_element_type=F32)

    for e in range(3):
        pre_two = jnp.dot(t2[...], QP[e : e + 3].reshape(1152, 256), preferred_element_type=F32)
        slopes = slope(pre_two)
        for plane in (e, e + 3):
            if plane > 4:
                continue
            side = slopes[:, :128] if plane == e else slopes[:, 128:]
            base = plane * 128
            cots_of = jnp.concatenate(
                [
                    cot[base : base + 64, :128],
                    cot[base : base + 64, 128:],
                    cot[base + 64 : base + 128, :128],
                    cot[base + 64 : base + 128, 128:],
                ],
                axis=0,
            )
            grad = (cots_of * side).astype(BF16).astype(F32)
            for c, part in enumerate(shifted(grad, 2)):
                for m in range(3):
                    n = plane - m
                    if 0 <= n <= 2:
                        GP[m, c, :, n * 128 : (n + 1) * 128] = part
            if plane == 2:
                lanes = lax.broadcasted_iota(jnp.int32, (256, 128), 1)
                kept = jnp.where(lanes % 2 == 0, grad, 0.0).astype(BF16)
                for b in range(3):
                    for at in range(4):
                        h = at + 1 - b
                        here = jnp.zeros((64, 128), BF16)
                        if 0 <= h < 4:
                            here = kept[h * 64 : (h + 1) * 64]
                        G2[b * 64 : (b + 1) * 64, at * 128 : (at + 1) * 128] = here

    back = jnp.dot(t2t[...], GP[...].reshape(2304, 384), preferred_element_type=F32)
    for q, f in enumerate((0, 1, 1, 2)):
        at = place + (f - 1)
        factor = jnp.where((at >= 0) & (at < SLABS), 0.125, 0.0)
        part = (back[:, f * 128 : (f + 1) * 128] * factor).reshape(4, 1, 32, 128)
        wide = jnp.concatenate([part, part], axis=1).reshape(256, 128)
        grad = (wide * SL[q]).astype(BF16).astype(F32)
        for c, piece in enumerate(shifted(grad, 1)):
            if q <= 2:
                HP[q, c, :, :128] = piece
            if q >= 1:
                HP[q - 1, c, :, 128:] = piece
            if c == 1 and q in (1, 2):
                for b in range(3):
                    for at in range(8):
                        h = at + 1 - b
                        here = jnp.zeros((32, 128), BF16)
                        if 0 <= h < 8:
                            here = piece[h * 32 : (h + 1) * 32]
                        to = (q - 1) * 128 + (64, 96, 0)[b]
                        G1[to : to + 32, at * 128 : (at + 1) * 128] = here
    for q in range(2):
        G1[q * 128 + 32 : q * 128 + 64] = jnp.zeros((32, 1024), BF16)

    out = jnp.dot(t1t[...], HP[...].reshape(2304, 256), preferred_element_type=F32)
    for p in range(2):
        side = out[:, p * 128 : (p + 1) * 128].reshape(8, 16, 128)
        gf[:, p] = jnp.transpose(side, (1, 0, 2)).astype(BF16)

    for c in range(3):
        for j in range(4):
            m, side = (j + 6, 0) if j <= 2 else (2, 128)
            to = (j * 3 + c) * 16
            for h in range(8):
                FS[to : to + 16, h * 128 : (h + 1) * 128] = XP[
                    m, c, h * 32 : h * 32 + 16, side : side + 128
                ]
        for a in range(3):
            to = (a * 3 + c) * 16
            for h in range(4):
                FP[to : to + 16, h * 128 : (h + 1) * 128] = QP[
                    2 + a, c, pl.ds(h * 32 + half, 16), :128
                ]
    along = (((1,), (1,)), ((), ()))
    one = lax.dot_general(FS[...], G1[...], along, preferred_element_type=F32)
    two = lax.dot_general(FP[...], G2[...], along, preferred_element_type=F32)
    one = one[0:144, :128] + one[48:192, 128:]
    wg[0:144] = jnp.concatenate([two[:, 128:], one[:, 64:]], axis=1)
    wg[144:288] = two[:, :128]
    thirds = [one[at : at + 48, :32] for at in (0, 48, 96)]
    wg[288:336] = jnp.concatenate(thirds + [jnp.zeros((48, 32), F32)], axis=1)
    wg[336:] = jnp.zeros((48, 128), F32)


def own_block(feats, cot, w1, w2):
    vmem = pl.BlockSpec(memory_space=pltpu.VMEM)
    hbm = pl.BlockSpec(memory_space=pltpu.MemorySpace.HBM)
    return pl.pallas_call(
        gather_kernel,
        in_specs=[hbm] * 4,
        out_specs=[vmem] * 3,
        out_shape=[
            jax.ShapeDtypeStruct((20, 16, 128), BF16),
            jax.ShapeDtypeStruct(w1.shape, BF16),
            jax.ShapeDtypeStruct(w2.shape, BF16),
        ],
        scratch_shapes=[
            pltpu.VMEM(feats.shape, BF16),
            pltpu.VMEM(cot.shape, BF16),
            pltpu.SemaphoreType.DMA((4,)),
        ],
        compiler_params=pltpu.CompilerParams(vmem_limit_bytes=4 * 2**20),
        name="gather",
    )(*[pltpu.with_memory_space_constraint(array, pltpu.HBM) for array in (feats, cot, w1, w2)])


def band_weights(w1, w2):
    vmem = pl.BlockSpec(memory_space=pltpu.VMEM)
    shapes = [(256, 2304), (128, 2304), (256, 1152), (128, 2304)]
    return pl.pallas_call(
        band_kernel,
        in_specs=[vmem] * 2,
        out_specs=[vmem] * 4,
        scratch_shapes=[pltpu.VMEM((8, 288, 256), BF16)],
        out_shape=[jax.ShapeDtypeStruct(shape, BF16) for shape in shapes],
        cost_estimate=pl.CostEstimate(flops=10**9, bytes_accessed=4 * 10**6, transcendentals=0),
        compiler_params=pltpu.CompilerParams(vmem_limit_bytes=16 * 2**20),
        name="bands",
    )(w1, w2)


def levels(own, oth, bands):
    vmem = pl.BlockSpec(memory_space=pltpu.VMEM)
    scratch = [
        ((9, 3, 256, 256), BF16),
        ((14, 128, 128), F32),
        ((4, 256, 128), F32),
        ((5, 3, 128, 256), BF16),
        ((3, 3, 256, 384), BF16),
        ((3, 3, 256, 256), BF16),
        ((5, 2, 64, 128), BF16),
        ((192, 1024), BF16),
        ((144, 512), BF16),
        ((256, 1024), BF16),
        ((192, 512), BF16),
    ]
    return pl.pallas_call(
        main_kernel,
        in_specs=[vmem] * 6,
        out_specs=[vmem, vmem],
        out_shape=[
            jax.ShapeDtypeStruct((16, 2, 8, 128), BF16),
            jax.ShapeDtypeStruct((384, 128), F32),
        ],
        scratch_shapes=[pltpu.VMEM(shape, dtype) for shape, dtype in scratch],
        cost_estimate=pl.CostEstimate(
            flops=10**10, bytes_accessed=8 * 10**6, transcendentals=10**6
        ),
        compiler_params=pltpu.CompilerParams(vmem_limit_bytes=28 * 2**20),
        name="levels",
    )(own, oth, *bands)


def exchange(pieces, groups):
    return lax.all_to_all(pieces, DEPTH, 0, 0, axis_index_groups=groups, tiled=True)


def total_over_depth(part):
    near = jnp.sum(exchange(part.reshape(16, 24, 128), NEAR), axis=0)
    whole = jnp.sum(exchange(jnp.broadcast_to(near, (16, 24, 128)), FAR), axis=0)
    copies = jnp.broadcast_to(whole.astype(BF16), (16, 24, 128))
    return exchange(copies, NEAR)


def split_kernel(total, gf, one_out, two_out, gf_out, one, two, sems):
    pairs = ((gf, gf_out), (one, one_out), (two, two_out))
    away = [
        pltpu.make_async_copy(source, target, sems.at[index])
        for index, (source, target) in enumerate(pairs)
    ]
    away[0].start()
    rows = total[...].reshape(384, 128).astype(F32)
    for a in range(3):
        for c in range(3):
            at = (a * 3 + c) * 16
            first = rows[at : at + 16]
            rest = rows[288 + at % 48 : 304 + at % 48]
            third = at // 48 * 32
            ones = (first[:, 64:96], first[:, 96:], rest[:, third : third + 32])
            for b in range(3):
                to = ((a * 3 + b) * 3 + c) * 16
                one[to : to + 16] = ones[b]
    away[1].start()
    for a in range(3):
        for c in range(3):
            at = (a * 3 + c) * 16
            first, second = rows[at : at + 16], rows[144 + at : 160 + at]
            twos = (second[:, :64], second[:, 64:], first[:, :64])
            for b in range(3):
                to = ((a * 3 + b) * 3 + c) * 16
                two[to : to + 16] = twos[b]
    away[2].start()
    for copy in away:
        copy.wait()


def split_total(total, gf):
    vmem = pl.BlockSpec(memory_space=pltpu.VMEM)
    shapes = [(432, 32), (432, 64)]
    return pl.pallas_call(
        split_kernel,
        in_specs=[vmem, vmem],
        out_specs=[pl.BlockSpec(memory_space=pl.ANY)] * 3,
        out_shape=[jax.ShapeDtypeStruct(shape, F32) for shape in shapes]
        + [jax.ShapeDtypeStruct(gf.shape, BF16)],
        scratch_shapes=[pltpu.VMEM(shape, F32) for shape in shapes]
        + [pltpu.SemaphoreType.DMA((3,))],
        compiler_params=pltpu.CompilerParams(vmem_limit_bytes=4 * 2**20),
        name="split",
    )(total, gf)


def shards(feats, weight_one, weight_two, cotangent):
    x = lax.axis_index("x")
    block, w1, w2 = own_block(
        feats,
        cotangent,
        jnp.transpose(weight_one, (2, 0, 1)),
        jnp.transpose(weight_two, (2, 1, 0)),
    )
    up = depth_shift(block, ROW)
    down = depth_shift(block, -ROW)

    bands = band_weights(w1, w2)

    three = jnp.concatenate([up, block, down], axis=0)
    slots = [
        lax.dynamic_slice_in_dim(
            three, jnp.where(x > t, 0, jnp.where(x == t, 8, 20)).astype(jnp.int32), 40, 0
        )
        for t in range(4)
    ]
    own = lax.all_to_all(jnp.stack(slots, 0), "x", 0, 0, tiled=True)
    oth = lax.ppermute(own, "chan", [(0, 1), (1, 0)])
    grad_feats, part = levels(own, oth, bands)
    one, two, grad_feats = split_total(total_over_depth(part), grad_feats)
    grad_weight_one = jnp.transpose(one.reshape(27, 16, 32), (2, 1, 0))
    grad_weight_two = jnp.transpose(two.reshape(27, 16, 64), (2, 1, 0))
    return (grad_feats, grad_weight_one, grad_weight_two)


def solution(mesh):
    finer = Mesh(
        mesh.devices.reshape(8, 8, 4, mesh.shape["chan"]), DEPTH + ("chan",)
    )
    in_specs = (P("chan", DEPTH, None, None), P(), P(), P("chan", DEPTH, None, None))
    out_specs = (P("chan", DEPTH, None, None), P(None, "chan", None), P(None, "chan", None))

    return jax.shard_map(
        shards, mesh=finer, in_specs=in_specs, out_specs=out_specs, check_vma=False
    )
```

```python
import jax
import jax.numpy as jnp
from jax import lax
from jax.experimental import pallas as pl
from jax.experimental.pallas import tpu as pltpu
from jax.sharding import Mesh
from jax.sharding import PartitionSpec as P


DEPTH = ("z", "y", "x")
SLABS = 256
ROW = 4
BF16 = jnp.bfloat16
F32 = jnp.float32


def depth_shift(block, steps):
    pairs = [(i, i + steps) for i in range(SLABS) if 0 <= i + steps < SLABS]
    return lax.ppermute(block, DEPTH, pairs)


def slope(pre):
    sig = jax.nn.sigmoid(pre)
    return sig * (1.0 + pre * (1.0 - sig))


def near_groups():
    far_class = [0, 1, 0, 1, 1, 0, 1, 0]
    groups = {}
    for place in range(SLABS):
        z, y, x = place // 32, place // 4 % 8, place % 4
        rank = (x * 2 + far_class[y]) * 2 + far_class[z]
        groups.setdefault((z // 2, y // 2), {})[rank] = place
    near = [[block[rank] for rank in range(16)] for block in groups.values()]
    far = [[block[rank] for block in groups.values()] for rank in range(16)]
    return near, far


NEAR, FAR = near_groups()


def position():
    place = (lax.axis_index("z") * 8 + lax.axis_index("y")) * 4 + lax.axis_index("x")
    return lax.axis_index("chan"), place


def gather_kernel(feats_far, cot_far, w1, w2, block, w1_near, w2_near, feats, cot, sems):
    pairs = ((feats_far, feats), (cot_far, cot), (w1, w1_near), (w2, w2_near))
    copies = [
        pltpu.make_async_copy(source, target, sems.at[index])
        for index, (source, target) in enumerate(pairs)
    ]
    for copy in copies:
        copy.start()
    copies[0].wait()
    for p in range(2):
        plane = jnp.transpose(feats[:, p].astype(F32), (1, 0, 2))
        block[p * 8 : (p + 1) * 8] = plane.astype(BF16)
    copies[1].wait()
    rows = jnp.transpose(cot[...].reshape(32, 4, 64).astype(F32), (1, 0, 2))
    for high in range(2):
        pair = jnp.concatenate([rows[2 * high], rows[2 * high + 1]], axis=1)
        block[16 + 2 * high : 18 + 2 * high] = pair.astype(BF16).reshape(2, 16, 128)
    for copy in copies[2:]:
        copy.wait()


def band_kernel(w1, w2, t1, t1t, t2, t2t, rows_one):
    turn = position()[0] * 16
    half = pl.multiple_of(turn, 16)

    def marks_of(width, lanes, sign, turn):
        row = lax.broadcasted_iota(jnp.int32, (3 * width, lanes), 0)
        lane = lax.broadcasted_iota(jnp.int32, (3 * width, lanes), 1)
        base = lane - (sign * (row // width - 1) * width + (row + turn) % width)
        return lambda h: jnp.where(base == h * width, 1.0, 0.0).astype(BF16)

    def taps_of(ref, flip):
        order = [(2 - a, 2 - c) if flip else (a, c) for a in range(3) for c in range(3)]
        return [[ref[9 * a + 3 * b + c] for b in range(3)] for a, c in order]

    def straight(ref, flip, marks, height, put):
        taps = taps_of(ref, flip)
        parts = [jnp.concatenate([tap[b] for tap in taps], axis=0) for b in range(3)]
        weights = jnp.concatenate(parts, axis=1)
        for h in range(height):
            put(h, jnp.dot(weights, marks(h), preferred_element_type=F32).astype(BF16))

    def crossed(ref, flip, marks, height, put):
        parts = [jnp.concatenate(tap, axis=0) for tap in taps_of(ref, flip)]
        weights = jnp.concatenate(parts, axis=1)
        for h in range(height):
            bands = lax.dot_general(
                weights, marks(h), (((0,), (0,)), ((), ())), preferred_element_type=F32
            )
            put(h, bands.astype(BF16))

    def into(out, rows, lanes):
        def put(h, bands):
            for tap in range(9):
                out[h * rows : (h + 1) * rows, tap * lanes : (tap + 1) * lanes] = bands[
                    tap * rows : (tap + 1) * rows
                ]

        return put

    def put_half(h, bands):
        rows_one[h] = bands
        for tap in range(9):
            t1t[h * 16 : (h + 1) * 16, tap * 256 : (tap + 1) * 256] = rows_one[
                h, pl.ds(tap * 32 + half, 16), :
            ]

    straight(w1, False, marks_of(32, 256, 1, turn), 8, into(t1, 32, 256))
    crossed(w1, True, marks_of(32, 256, -1, 0), 8, put_half)
    crossed(w2, False, marks_of(32, 128, 1, 0), 4, into(t2, 64, 128))
    straight(w2, True, marks_of(64, 256, -1, 0), 4, into(t2t, 32, 256))


def shifted(value, step):
    lanes = value.shape[-1]
    lane = lax.broadcasted_iota(jnp.int32, value.shape, 1)
    low = jnp.where(lane < step, 0.0, pltpu.roll(value, step, 1))
    high = jnp.where(lane >= lanes - step, 0.0, pltpu.roll(value, lanes - step, 1))
    return low.astype(BF16), value.astype(BF16), high.astype(BF16)


def main_kernel(
    own, oth, t1, t1t, t2, t2t, gf, wg, XP, PS, SL, QP, GP, HP, CT, FS, FP, G1, G2
):
    member, place = position()
    x = lax.rem(place, 4)
    half = pl.multiple_of(member * 16, 16)

    def slot(delta):
        return lax.rem(x + delta + 4, 4)

    planes = [(slot(0), 0)]
    planes += [(slot(delta), 8 * p) for delta in (-3, -2, -1) for p in range(2)]
    planes += [(slot(0), 12), (slot(0), 20)]
    planes += [(slot(delta), 20 + 8 * p) for delta in (1, 2, 3) for p in range(2)]
    planes += [(slot(0), 32)]

    def load_plane(j):
        at, start = planes[j]
        plane = jnp.concatenate(
            [own[at, start : start + 8], oth[at, start : start + 8]], axis=1
        ).reshape(256, 128)
        for c, part in enumerate(shifted(plane.astype(F32), 1)):
            if j <= 8:
                XP[j, c, :, :128] = part
            if j >= 7:
                XP[j - 7, c, :, 128:] = part

    for j in (0, 1, 7, 8):
        load_plane(j)

    for k in range(7):
        for j in (k + 2, k + 9):
            if j not in (7, 8) and j < 16:
                load_plane(j)
        pre = jnp.dot(t1[...], XP[k : k + 3].reshape(2304, 256), preferred_element_type=F32)
        act = (pre * jax.nn.sigmoid(pre)).astype(BF16).astype(F32).reshape(4, 2, 32, 256)
        rows = (act[:, 0] + act[:, 1]).reshape(128, 256)
        PS[k] = rows[:, :128]
        PS[k + 7] = rows[:, 128:]
        if k >= 5:
            SL[k - 5] = slope(pre[:, :128])
        if k <= 1:
            SL[k + 2] = slope(pre[:, 128:])

    lane = lax.broadcasted_iota(jnp.int32, (128, 128), 1)
    even = lane % 2 == 0
    for c in range(3):
        QP[4, c, :, 128:] = jnp.zeros((128, 128), BF16)
    for j in range(7):
        total = PS[2 * j] + PS[2 * j + 1]
        total = total + jnp.where(even, pltpu.roll(total, 127, 1), pltpu.roll(total, 1, 1))
        at = place + (j - 3)
        factor = jnp.where((at >= 0) & (at < SLABS), 0.125, 0.0)
        pooled = (total * factor).astype(BF16).astype(F32)
        for c, part in enumerate(shifted(pooled, 2)):
            if j <= 4:
                QP[j, c, :, :128] = part
            if j >= 3:
                QP[j - 3, c, :, 128:] = part

    cots = [(slot(-2), 16), (slot(-1), 16), (slot(0), 28), (slot(1), 36), (slot(2), 36)]
    own_o = pl.multiple_of(member * 32, 32)
    oth_o = pl.multiple_of(32 - member * 32, 32)
    for e, (at, start) in enumerate(cots):
        for high in range(2):
            here = start + 2 * high
            CT[e, high, pl.ds(own_o, 32), :] = own[at, here : here + 2].reshape(32, 128)
            CT[e, high, pl.ds(oth_o, 32), :] = oth[at, here : here + 2].reshape(32, 128)
    row = lax.broadcasted_iota(jnp.int32, (128, 256), 0)
    col = lax.broadcasted_iota(jnp.int32, (128, 256), 1)
    spread = jnp.where(row == (col // 128) * 64 + (col % 128) // 2, 1.0, 0.0).astype(BF16)
    cot = jnp.dot(CT[...].reshape(640, 128), spread, preferred_element_type=F32)

    for e in range(3):
        pre_two = jnp.dot(t2[...], QP[e : e + 3].reshape(1152, 256), preferred_element_type=F32)
        slopes = slope(pre_two)
        for plane in (e, e + 3):
            if plane > 4:
                continue
            side = slopes[:, :128] if plane == e else slopes[:, 128:]
            base = plane * 128
            cots_of = jnp.concatenate(
                [
                    cot[base : base + 64, :128],
                    cot[base : base + 64, 128:],
                    cot[base + 64 : base + 128, :128],
                    cot[base + 64 : base + 128, 128:],
                ],
                axis=0,
            )
            grad = (cots_of * side).astype(BF16).astype(F32)
            for c, part in enumerate(shifted(grad, 2)):
                for m in range(3):
                    n = plane - m
                    if 0 <= n <= 2:
                        GP[m, c, :, n * 128 : (n + 1) * 128] = part
            if plane == 2:
                lanes = lax.broadcasted_iota(jnp.int32, (256, 128), 1)
                kept = jnp.where(lanes % 2 == 0, grad, 0.0).astype(BF16)
                for b in range(3):
                    for at in range(4):
                        h = at + 1 - b
                        here = jnp.zeros((64, 128), BF16)
                        if 0 <= h < 4:
                            here = kept[h * 64 : (h + 1) * 64]
                        G2[b * 64 : (b + 1) * 64, at * 128 : (at + 1) * 128] = here

    back = jnp.dot(t2t[...], GP[...].reshape(2304, 384), preferred_element_type=F32)
    for q, f in enumerate((0, 1, 1, 2)):
        at = place + (f - 1)
        factor = jnp.where((at >= 0) & (at < SLABS), 0.125, 0.0)
        part = (back[:, f * 128 : (f + 1) * 128] * factor).reshape(4, 1, 32, 128)
        wide = jnp.concatenate([part, part], axis=1).reshape(256, 128)
        grad = (wide * SL[q]).astype(BF16).astype(F32)
        for c, piece in enumerate(shifted(grad, 1)):
            if q <= 2:
                HP[q, c, :, :128] = piece
            if q >= 1:
                HP[q - 1, c, :, 128:] = piece
            if c == 1 and q in (1, 2):
                for b in range(3):
                    for at in range(8):
                        h = at + 1 - b
                        here = jnp.zeros((32, 128), BF16)
                        if 0 <= h < 8:
                            here = piece[h * 32 : (h + 1) * 32]
                        to = (q - 1) * 128 + (64, 96, 0)[b]
                        G1[to : to + 32, at * 128 : (at + 1) * 128] = here
    for q in range(2):
        G1[q * 128 + 32 : q * 128 + 64] = jnp.zeros((32, 1024), BF16)

    out = jnp.dot(t1t[...], HP[...].reshape(2304, 256), preferred_element_type=F32)
    for p in range(2):
        side = out[:, p * 128 : (p + 1) * 128].reshape(8, 16, 128)
        gf[:, p] = jnp.transpose(side, (1, 0, 2)).astype(BF16)

    for c in range(3):
        for j in range(4):
            m, side = (j + 6, 0) if j <= 2 else (2, 128)
            to = (j * 3 + c) * 16
            for h in range(8):
                FS[to : to + 16, h * 128 : (h + 1) * 128] = XP[
                    m, c, h * 32 : h * 32 + 16, side : side + 128
                ]
        for a in range(3):
            to = (a * 3 + c) * 16
            for h in range(4):
                FP[to : to + 16, h * 128 : (h + 1) * 128] = QP[
                    2 + a, c, pl.ds(h * 32 + half, 16), :128
                ]
    along = (((1,), (1,)), ((), ()))
    one = lax.dot_general(FS[...], G1[...], along, preferred_element_type=F32)
    two = lax.dot_general(FP[...], G2[...], along, preferred_element_type=F32)
    one = one[0:144, :128] + one[48:192, 128:]
    wg[0:144] = jnp.concatenate([two[:, 128:], one[:, 64:]], axis=1).astype(BF16)
    wg[144:288] = two[:, :128].astype(BF16)
    thirds = [one[at : at + 48, :32] for at in (0, 48, 96)]
    rest = jnp.concatenate(thirds + [jnp.zeros((48, 32), F32)], axis=1)
    wg[288:336] = rest.astype(BF16)
    wg[336:] = jnp.zeros((48, 128), BF16)


def own_block(feats, cot, w1, w2):
    vmem = pl.BlockSpec(memory_space=pltpu.VMEM)
    hbm = pl.BlockSpec(memory_space=pltpu.MemorySpace.HBM)
    return pl.pallas_call(
        gather_kernel,
        in_specs=[hbm] * 4,
        out_specs=[vmem] * 3,
        out_shape=[
            jax.ShapeDtypeStruct((20, 16, 128), BF16),
            jax.ShapeDtypeStruct(w1.shape, BF16),
            jax.ShapeDtypeStruct(w2.shape, BF16),
        ],
        scratch_shapes=[
            pltpu.VMEM(feats.shape, BF16),
            pltpu.VMEM(cot.shape, BF16),
            pltpu.SemaphoreType.DMA((4,)),
        ],
        compiler_params=pltpu.CompilerParams(vmem_limit_bytes=4 * 2**20),
        name="gather",
    )(*[pltpu.with_memory_space_constraint(array, pltpu.HBM) for array in (feats, cot, w1, w2)])


def band_weights(w1, w2):
    vmem = pl.BlockSpec(memory_space=pltpu.VMEM)
    shapes = [(256, 2304), (128, 2304), (256, 1152), (128, 2304)]
    return pl.pallas_call(
        band_kernel,
        in_specs=[vmem] * 2,
        out_specs=[vmem] * 4,
        scratch_shapes=[pltpu.VMEM((8, 288, 256), BF16)],
        out_shape=[jax.ShapeDtypeStruct(shape, BF16) for shape in shapes],
        cost_estimate=pl.CostEstimate(flops=10**9, bytes_accessed=4 * 10**6, transcendentals=0),
        compiler_params=pltpu.CompilerParams(vmem_limit_bytes=16 * 2**20),
        name="bands",
    )(w1, w2)


def levels(own, oth, bands):
    vmem = pl.BlockSpec(memory_space=pltpu.VMEM)
    scratch = [
        ((9, 3, 256, 256), BF16),
        ((14, 128, 128), F32),
        ((4, 256, 128), F32),
        ((5, 3, 128, 256), BF16),
        ((3, 3, 256, 384), BF16),
        ((3, 3, 256, 256), BF16),
        ((5, 2, 64, 128), BF16),
        ((192, 1024), BF16),
        ((144, 512), BF16),
        ((256, 1024), BF16),
        ((192, 512), BF16),
    ]
    return pl.pallas_call(
        main_kernel,
        in_specs=[vmem] * 6,
        out_specs=[vmem, vmem],
        out_shape=[
            jax.ShapeDtypeStruct((16, 2, 8, 128), BF16),
            jax.ShapeDtypeStruct((384, 128), BF16),
        ],
        scratch_shapes=[pltpu.VMEM(shape, dtype) for shape, dtype in scratch],
        cost_estimate=pl.CostEstimate(
            flops=10**10, bytes_accessed=8 * 10**6, transcendentals=10**6
        ),
        compiler_params=pltpu.CompilerParams(vmem_limit_bytes=28 * 2**20),
        name="levels",
    )(own, oth, *bands)


def exchange(pieces, groups):
    return lax.all_to_all(pieces, DEPTH, 0, 0, axis_index_groups=groups, tiled=True)


def total_over_depth(part):
    pieces = exchange(part.reshape(16, 24, 128), NEAR)
    for groups in (FAR, NEAR):
        total = jnp.sum(pieces.astype(F32), axis=0).astype(BF16)
        pieces = exchange(jnp.broadcast_to(total, (16, 24, 128)), groups)
    return pieces


def split_kernel(total, gf, one_out, two_out, gf_out, one, two, sems):
    pairs = ((gf, gf_out), (one, one_out), (two, two_out))
    away = [
        pltpu.make_async_copy(source, target, sems.at[index])
        for index, (source, target) in enumerate(pairs)
    ]
    away[0].start()
    rows = total[...].reshape(384, 128).astype(F32)
    for a in range(3):
        for c in range(3):
            at = (a * 3 + c) * 16
            first = rows[at : at + 16]
            rest = rows[288 + at % 48 : 304 + at % 48]
            third = at // 48 * 32
            ones = (first[:, 64:96], first[:, 96:], rest[:, third : third + 32])
            for b in range(3):
                to = ((a * 3 + b) * 3 + c) * 16
                one[to : to + 16] = ones[b]
    away[1].start()
    for a in range(3):
        for c in range(3):
            at = (a * 3 + c) * 16
            first, second = rows[at : at + 16], rows[144 + at : 160 + at]
            twos = (second[:, :64], second[:, 64:], first[:, :64])
            for b in range(3):
                to = ((a * 3 + b) * 3 + c) * 16
                two[to : to + 16] = twos[b]
    away[2].start()
    for copy in away:
        copy.wait()


def split_total(total, gf):
    vmem = pl.BlockSpec(memory_space=pltpu.VMEM)
    shapes = [(432, 32), (432, 64)]
    return pl.pallas_call(
        split_kernel,
        in_specs=[vmem, vmem],
        out_specs=[pl.BlockSpec(memory_space=pl.ANY)] * 3,
        out_shape=[jax.ShapeDtypeStruct(shape, F32) for shape in shapes]
        + [jax.ShapeDtypeStruct(gf.shape, BF16)],
        scratch_shapes=[pltpu.VMEM(shape, F32) for shape in shapes]
        + [pltpu.SemaphoreType.DMA((3,))],
        compiler_params=pltpu.CompilerParams(vmem_limit_bytes=4 * 2**20),
        name="split",
    )(total, gf)


def shards(feats, weight_one, weight_two, cotangent):
    x = lax.axis_index("x")
    block, w1, w2 = own_block(
        feats,
        cotangent,
        jnp.transpose(weight_one, (2, 0, 1)),
        jnp.transpose(weight_two, (2, 1, 0)),
    )
    up = depth_shift(block, ROW)
    down = depth_shift(block, -ROW)

    bands = band_weights(w1, w2)

    three = jnp.concatenate([up, block, down], axis=0)
    slots = [
        lax.dynamic_slice_in_dim(
            three, jnp.where(x > t, 0, jnp.where(x == t, 8, 20)).astype(jnp.int32), 40, 0
        )
        for t in range(4)
    ]
    own = lax.all_to_all(jnp.stack(slots, 0), "x", 0, 0, tiled=True)
    oth = lax.ppermute(own, "chan", [(0, 1), (1, 0)])
    grad_feats, part = levels(own, oth, bands)
    one, two, grad_feats = split_total(total_over_depth(part), grad_feats)
    grad_weight_one = jnp.transpose(one.reshape(27, 16, 32), (2, 1, 0))
    grad_weight_two = jnp.transpose(two.reshape(27, 16, 64), (2, 1, 0))
    return (grad_feats, grad_weight_one, grad_weight_two)


def solution(mesh):
    finer = Mesh(
        mesh.devices.reshape(8, 8, 4, mesh.shape["chan"]), DEPTH + ("chan",)
    )
    in_specs = (P("chan", DEPTH, None, None), P(), P(), P("chan", DEPTH, None, None))
    out_specs = (P("chan", DEPTH, None, None), P(None, "chan", None), P(None, "chan", None))

    return jax.shard_map(
        shards, mesh=finer, in_specs=in_specs, out_specs=out_specs, check_vma=False
    )
```

```python
import jax
import jax.numpy as jnp
from jax import lax
from jax.experimental import pallas as pl
from jax.experimental.pallas import tpu as pltpu
from jax.sharding import Mesh
from jax.sharding import PartitionSpec as P


DEPTH = ("z", "y", "x")
SLABS = 256
ROW = 4
BF16 = jnp.bfloat16
F32 = jnp.float32


def depth_shift(block, steps):
    pairs = [(i, i + steps) for i in range(SLABS) if 0 <= i + steps < SLABS]
    return lax.ppermute(block, DEPTH, pairs)


def slope(pre):
    sig = jax.nn.sigmoid(pre)
    return sig * (1.0 + pre * (1.0 - sig))


def near_groups():
    far_class = [0, 1, 0, 1, 1, 0, 1, 0]
    groups = {}
    for place in range(SLABS):
        z, y, x = place // 32, place // 4 % 8, place % 4
        rank = (x * 2 + far_class[y]) * 2 + far_class[z]
        groups.setdefault((z // 2, y // 2), {})[rank] = place
    near = [[block[rank] for rank in range(16)] for block in groups.values()]
    far = [[block[rank] for block in groups.values()] for rank in range(16)]
    return near, far


NEAR, FAR = near_groups()


def position():
    place = (lax.axis_index("z") * 8 + lax.axis_index("y")) * 4 + lax.axis_index("x")
    return lax.axis_index("chan"), place


def gather_kernel(feats_far, cot_far, w1, w2, block, w1_near, w2_near, feats, cot, sems):
    pairs = ((feats_far, feats), (cot_far, cot), (w1, w1_near), (w2, w2_near))
    copies = [
        pltpu.make_async_copy(source, target, sems.at[index])
        for index, (source, target) in enumerate(pairs)
    ]
    for copy in copies:
        copy.start()
    copies[0].wait()
    for p in range(2):
        plane = jnp.transpose(feats[:, p].astype(F32), (1, 0, 2))
        block[p * 8 : (p + 1) * 8] = plane.astype(BF16)
    copies[1].wait()
    rows = jnp.transpose(cot[...].reshape(32, 4, 64).astype(F32), (1, 0, 2))
    for high in range(2):
        pair = jnp.concatenate([rows[2 * high], rows[2 * high + 1]], axis=1)
        block[16 + 2 * high : 18 + 2 * high] = pair.astype(BF16).reshape(2, 16, 128)
    for copy in copies[2:]:
        copy.wait()


def band_kernel(w1, w2, t1_own, t1_oth, t1t, t2, t2t, rows_one):
    turn = position()[0] * 16
    half = pl.multiple_of(turn, 16)

    def marks_of(width, lanes, sign):
        row = lax.broadcasted_iota(jnp.int32, (3 * width, lanes), 0)
        lane = lax.broadcasted_iota(jnp.int32, (3 * width, lanes), 1)
        base = lane - (sign * (row // width - 1) * width + row % width)
        return lambda h: jnp.where(base == h * width, 1.0, 0.0).astype(BF16)

    def marks_by_core():
        row = lax.broadcasted_iota(jnp.int32, (96, 256), 0)
        lane = lax.broadcasted_iota(jnp.int32, (96, 256), 1)
        chan = (row + turn) % 32
        fits = (lane // 128 == chan // 16) & (lane % 16 == chan % 16)
        base = jnp.where(fits, lane % 128 // 16 - (row // 32 - 1), -1)
        return lambda h: jnp.where(base == h, 1.0, 0.0).astype(BF16)

    def taps_of(ref, flip):
        order = [(2 - a, 2 - c) if flip else (a, c) for a in range(3) for c in range(3)]
        return [[ref[9 * a + 3 * b + c] for b in range(3)] for a, c in order]

    def straight(ref, flip, marks, height, put):
        taps = taps_of(ref, flip)
        parts = [jnp.concatenate([tap[b] for tap in taps], axis=0) for b in range(3)]
        weights = jnp.concatenate(parts, axis=1)
        for h in range(height):
            put(h, jnp.dot(weights, marks(h), preferred_element_type=F32).astype(BF16))

    def crossed(ref, flip, marks, height, put):
        parts = [jnp.concatenate(tap, axis=0) for tap in taps_of(ref, flip)]
        weights = jnp.concatenate(parts, axis=1)
        for h in range(height):
            bands = lax.dot_general(
                weights, marks(h), (((0,), (0,)), ((), ())), preferred_element_type=F32
            )
            put(h, bands.astype(BF16))

    def into(out, rows, lanes):
        def put(h, bands):
            for tap in range(9):
                out[h * rows : (h + 1) * rows, tap * lanes : (tap + 1) * lanes] = bands[
                    tap * rows : (tap + 1) * rows
                ]

        return put

    def put_half(h, bands):
        rows_one[h] = bands
        for tap in range(9):
            t1t[h * 16 : (h + 1) * 16, tap * 256 : (tap + 1) * 256] = rows_one[
                h, pl.ds(tap * 32 + half, 16), :
            ]

    def put_both(h, bands):
        for tap in range(9):
            for side, out in ((0, t1_own), (128, t1_oth)):
                out[h * 32 : (h + 1) * 32, tap * 128 : (tap + 1) * 128] = bands[
                    tap * 32 : (tap + 1) * 32, side : side + 128
                ]

    straight(w1, False, marks_by_core(), 8, put_both)
    crossed(w1, True, marks_of(32, 256, -1), 8, put_half)
    crossed(w2, False, marks_of(32, 128, 1), 4, into(t2, 64, 128))
    straight(w2, True, marks_of(64, 256, -1), 4, into(t2t, 32, 256))


def shifted(value, step):
    lanes = value.shape[-1]
    lane = lax.broadcasted_iota(jnp.int32, value.shape, 1)
    low = jnp.where(lane < step, 0.0, pltpu.roll(value, step, 1))
    high = jnp.where(lane >= lanes - step, 0.0, pltpu.roll(value, lanes - step, 1))
    return low.astype(BF16), value.astype(BF16), high.astype(BF16)


def plane_tiles(x):
    def slot(delta):
        return lax.rem(x + delta + 4, 4)

    planes = [(slot(0), 0)]
    planes += [(slot(delta), 8 * p) for delta in (-3, -2, -1) for p in range(2)]
    planes += [(slot(0), 12), (slot(0), 20)]
    planes += [(slot(delta), 20 + 8 * p) for delta in (1, 2, 3) for p in range(2)]
    return planes + [(slot(0), 32)]


def convolve_half(tiles, bands, fields, use):
    planes = plane_tiles(lax.rem(position()[1], 4))

    def load_plane(j):
        at, start = planes[j]
        plane = tiles[at, start : start + 8].reshape(128, 128)
        for c, part in enumerate(shifted(plane.astype(F32), 1)):
            if j <= 8:
                fields[j, c, :, :128] = part
            if j >= 7:
                fields[j - 7, c, :, 128:] = part

    for j in (0, 1, 7, 8):
        load_plane(j)
    for k in range(7):
        for j in (k + 2, k + 9):
            if j not in (7, 8) and j < 16:
                load_plane(j)
        field = fields[k : k + 3].reshape(1152, 256)
        use(k, jnp.dot(bands[...], field, preferred_element_type=F32))


def own_kernel(own, t1_own, fields, sums):
    def use(k, part):
        sums[k] = part

    convolve_half(own, t1_own, fields, use)


def main_kernel(
    own, oth, own_fields, own_sums, t1_oth, t1t, t2, t2t, gf, wg,
    XP, PS, SL, QP, GP, HP, CT, FS, FP, G1, G2,
):
    member, place = position()
    x = lax.rem(place, 4)
    half = pl.multiple_of(member * 16, 16)

    def slot(delta):
        return lax.rem(x + delta + 4, 4)

    def use(k, part):
        pre = part + own_sums[k]
        act = (pre * jax.nn.sigmoid(pre)).astype(BF16).astype(F32).reshape(4, 2, 32, 256)
        rows = (act[:, 0] + act[:, 1]).reshape(128, 256)
        PS[k] = rows[:, :128]
        PS[k + 7] = rows[:, 128:]
        if k >= 5:
            SL[k - 5] = slope(pre[:, :128])
        if k <= 1:
            SL[k + 2] = slope(pre[:, 128:])

    convolve_half(oth, t1_oth, XP, use)

    lane = lax.broadcasted_iota(jnp.int32, (128, 128), 1)
    even = lane % 2 == 0
    for c in range(3):
        QP[4, c, :, 128:] = jnp.zeros((128, 128), BF16)
    for j in range(7):
        total = PS[2 * j] + PS[2 * j + 1]
        total = total + jnp.where(even, pltpu.roll(total, 127, 1), pltpu.roll(total, 1, 1))
        at = place + (j - 3)
        factor = jnp.where((at >= 0) & (at < SLABS), 0.125, 0.0)
        pooled = (total * factor).astype(BF16).astype(F32)
        for c, part in enumerate(shifted(pooled, 2)):
            if j <= 4:
                QP[j, c, :, :128] = part
            if j >= 3:
                QP[j - 3, c, :, 128:] = part

    cots = [(slot(-2), 16), (slot(-1), 16), (slot(0), 28), (slot(1), 36), (slot(2), 36)]
    own_o = pl.multiple_of(member * 32, 32)
    oth_o = pl.multiple_of(32 - member * 32, 32)
    for e, (at, start) in enumerate(cots):
        for high in range(2):
            here = start + 2 * high
            CT[e, high, pl.ds(own_o, 32), :] = own[at, here : here + 2].reshape(32, 128)
            CT[e, high, pl.ds(oth_o, 32), :] = oth[at, here : here + 2].reshape(32, 128)
    row = lax.broadcasted_iota(jnp.int32, (128, 256), 0)
    col = lax.broadcasted_iota(jnp.int32, (128, 256), 1)
    spread = jnp.where(row == (col // 128) * 64 + (col % 128) // 2, 1.0, 0.0).astype(BF16)
    cot = jnp.dot(CT[...].reshape(640, 128), spread, preferred_element_type=F32)

    for e in range(3):
        pre_two = jnp.dot(t2[...], QP[e : e + 3].reshape(1152, 256), preferred_element_type=F32)
        slopes = slope(pre_two)
        for plane in (e, e + 3):
            if plane > 4:
                continue
            side = slopes[:, :128] if plane == e else slopes[:, 128:]
            base = plane * 128
            cots_of = jnp.concatenate(
                [
                    cot[base : base + 64, :128],
                    cot[base : base + 64, 128:],
                    cot[base + 64 : base + 128, :128],
                    cot[base + 64 : base + 128, 128:],
                ],
                axis=0,
            )
            grad = (cots_of * side).astype(BF16).astype(F32)
            for c, part in enumerate(shifted(grad, 2)):
                for m in range(3):
                    n = plane - m
                    if 0 <= n <= 2:
                        GP[m, c, :, n * 128 : (n + 1) * 128] = part
            if plane == 2:
                lanes = lax.broadcasted_iota(jnp.int32, (256, 128), 1)
                kept = jnp.where(lanes % 2 == 0, grad, 0.0).astype(BF16)
                for b in range(3):
                    for at in range(4):
                        h = at + 1 - b
                        here = jnp.zeros((64, 128), BF16)
                        if 0 <= h < 4:
                            here = kept[h * 64 : (h + 1) * 64]
                        G2[b * 64 : (b + 1) * 64, at * 128 : (at + 1) * 128] = here

    back = jnp.dot(t2t[...], GP[...].reshape(2304, 384), preferred_element_type=F32)
    for q, f in enumerate((0, 1, 1, 2)):
        at = place + (f - 1)
        factor = jnp.where((at >= 0) & (at < SLABS), 0.125, 0.0)
        part = (back[:, f * 128 : (f + 1) * 128] * factor).reshape(4, 1, 32, 128)
        wide = jnp.concatenate([part, part], axis=1).reshape(256, 128)
        grad = (wide * SL[q]).astype(BF16).astype(F32)
        for c, piece in enumerate(shifted(grad, 1)):
            if q <= 2:
                HP[q, c, :, :128] = piece
            if q >= 1:
                HP[q - 1, c, :, 128:] = piece
            if c == 1 and q in (1, 2):
                for b in range(3):
                    for at in range(8):
                        h = at + 1 - b
                        here = jnp.zeros((32, 128), BF16)
                        if 0 <= h < 8:
                            here = piece[h * 32 : (h + 1) * 32]
                        to = (q - 1) * 128 + (64, 96, 0)[b]
                        G1[to : to + 32, at * 128 : (at + 1) * 128] = here
    for q in range(2):
        G1[q * 128 + 32 : q * 128 + 64] = jnp.zeros((32, 1024), BF16)

    out = jnp.dot(t1t[...], HP[...].reshape(2304, 256), preferred_element_type=F32)
    for p in range(2):
        side = out[:, p * 128 : (p + 1) * 128].reshape(8, 16, 128)
        gf[:, p] = jnp.transpose(side, (1, 0, 2)).astype(BF16)

    for c in range(3):
        for j in range(4):
            m, side = (j + 6, 0) if j <= 2 else (2, 128)
            to = (j * 3 + c) * 16
            for h in range(8):
                FS[to : to + 16, h * 128 : (h + 1) * 128] = own_fields[
                    m, c, h * 16 : h * 16 + 16, side : side + 128
                ]
        for a in range(3):
            to = (a * 3 + c) * 16
            for h in range(4):
                FP[to : to + 16, h * 128 : (h + 1) * 128] = QP[
                    2 + a, c, pl.ds(h * 32 + half, 16), :128
                ]
    along = (((1,), (1,)), ((), ()))
    one = lax.dot_general(FS[...], G1[...], along, preferred_element_type=F32)
    two = lax.dot_general(FP[...], G2[...], along, preferred_element_type=F32)
    one = one[0:144, :128] + one[48:192, 128:]
    wg[0:144] = jnp.concatenate([two[:, 128:], one[:, 64:]], axis=1).astype(BF16)
    wg[144:288] = two[:, :128].astype(BF16)
    thirds = [one[at : at + 48, :32] for at in (0, 48, 96)]
    rest = jnp.concatenate(thirds + [jnp.zeros((48, 32), F32)], axis=1)
    wg[288:336] = rest.astype(BF16)
    wg[336:] = jnp.zeros((48, 128), BF16)


def own_block(feats, cot, w1, w2):
    vmem = pl.BlockSpec(memory_space=pltpu.VMEM)
    hbm = pl.BlockSpec(memory_space=pltpu.MemorySpace.HBM)
    return pl.pallas_call(
        gather_kernel,
        in_specs=[hbm] * 4,
        out_specs=[vmem] * 3,
        out_shape=[
            jax.ShapeDtypeStruct((20, 16, 128), BF16),
            jax.ShapeDtypeStruct(w1.shape, BF16),
            jax.ShapeDtypeStruct(w2.shape, BF16),
        ],
        scratch_shapes=[
            pltpu.VMEM(feats.shape, BF16),
            pltpu.VMEM(cot.shape, BF16),
            pltpu.SemaphoreType.DMA((4,)),
        ],
        compiler_params=pltpu.CompilerParams(vmem_limit_bytes=4 * 2**20),
        name="gather",
    )(*[pltpu.with_memory_space_constraint(array, pltpu.HBM) for array in (feats, cot, w1, w2)])


def band_weights(w1, w2):
    vmem = pl.BlockSpec(memory_space=pltpu.VMEM)
    shapes = [(256, 1152), (256, 1152), (128, 2304), (256, 1152), (128, 2304)]
    return pl.pallas_call(
        band_kernel,
        in_specs=[vmem] * 2,
        out_specs=[vmem] * 5,
        scratch_shapes=[pltpu.VMEM((8, 288, 256), BF16)],
        out_shape=[jax.ShapeDtypeStruct(shape, BF16) for shape in shapes],
        cost_estimate=pl.CostEstimate(flops=10**9, bytes_accessed=4 * 10**6, transcendentals=0),
        compiler_params=pltpu.CompilerParams(vmem_limit_bytes=16 * 2**20),
        name="bands",
    )(w1, w2)


def own_half(own, t1_own):
    vmem = pl.BlockSpec(memory_space=pltpu.VMEM)
    return pl.pallas_call(
        own_kernel,
        in_specs=[vmem, vmem],
        out_specs=[vmem, vmem],
        out_shape=[
            jax.ShapeDtypeStruct((9, 3, 128, 256), BF16),
            jax.ShapeDtypeStruct((7, 256, 256), F32),
        ],
        cost_estimate=pl.CostEstimate(flops=10**9, bytes_accessed=5 * 10**6, transcendentals=0),
        compiler_params=pltpu.CompilerParams(vmem_limit_bytes=12 * 2**20),
        name="half",
    )(own, t1_own)


def levels(fields, bands):
    vmem = pl.BlockSpec(memory_space=pltpu.VMEM)
    scratch = [
        ((9, 3, 128, 256), BF16),
        ((14, 128, 128), F32),
        ((4, 256, 128), F32),
        ((5, 3, 128, 256), BF16),
        ((3, 3, 256, 384), BF16),
        ((3, 3, 256, 256), BF16),
        ((5, 2, 64, 128), BF16),
        ((192, 1024), BF16),
        ((144, 512), BF16),
        ((256, 1024), BF16),
        ((192, 512), BF16),
    ]
    return pl.pallas_call(
        main_kernel,
        in_specs=[vmem] * 8,
        out_specs=[vmem, vmem],
        out_shape=[
            jax.ShapeDtypeStruct((16, 2, 8, 128), BF16),
            jax.ShapeDtypeStruct((384, 128), BF16),
        ],
        scratch_shapes=[pltpu.VMEM(shape, dtype) for shape, dtype in scratch],
        cost_estimate=pl.CostEstimate(
            flops=10**10, bytes_accessed=8 * 10**6, transcendentals=10**6
        ),
        compiler_params=pltpu.CompilerParams(vmem_limit_bytes=28 * 2**20),
        name="levels",
    )(*fields, *bands)


def exchange(pieces, groups):
    return lax.all_to_all(pieces, DEPTH, 0, 0, axis_index_groups=groups, tiled=True)


def total_over_depth(part):
    pieces = exchange(part.reshape(16, 24, 128), NEAR)
    for groups in (FAR, NEAR):
        total = jnp.sum(pieces.astype(F32), axis=0).astype(BF16)
        pieces = exchange(jnp.broadcast_to(total, (16, 24, 128)), groups)
    return pieces


def split_kernel(total, gf, one_out, two_out, gf_out, one, two, sems):
    pairs = ((gf, gf_out), (one, one_out), (two, two_out))
    away = [
        pltpu.make_async_copy(source, target, sems.at[index])
        for index, (source, target) in enumerate(pairs)
    ]
    away[0].start()
    rows = total[...].reshape(384, 128).astype(F32)
    for a in range(3):
        for c in range(3):
            at = (a * 3 + c) * 16
            first = rows[at : at + 16]
            rest = rows[288 + at % 48 : 304 + at % 48]
            third = at // 48 * 32
            ones = (first[:, 64:96], first[:, 96:], rest[:, third : third + 32])
            for b in range(3):
                to = ((a * 3 + b) * 3 + c) * 16
                one[to : to + 16] = ones[b]
    away[1].start()
    for a in range(3):
        for c in range(3):
            at = (a * 3 + c) * 16
            first, second = rows[at : at + 16], rows[144 + at : 160 + at]
            twos = (second[:, :64], second[:, 64:], first[:, :64])
            for b in range(3):
                to = ((a * 3 + b) * 3 + c) * 16
                two[to : to + 16] = twos[b]
    away[2].start()
    for copy in away:
        copy.wait()


def split_total(total, gf):
    vmem = pl.BlockSpec(memory_space=pltpu.VMEM)
    shapes = [(432, 32), (432, 64)]
    return pl.pallas_call(
        split_kernel,
        in_specs=[vmem, vmem],
        out_specs=[pl.BlockSpec(memory_space=pl.ANY)] * 3,
        out_shape=[jax.ShapeDtypeStruct(shape, F32) for shape in shapes]
        + [jax.ShapeDtypeStruct(gf.shape, BF16)],
        scratch_shapes=[pltpu.VMEM(shape, F32) for shape in shapes]
        + [pltpu.SemaphoreType.DMA((3,))],
        compiler_params=pltpu.CompilerParams(vmem_limit_bytes=4 * 2**20),
        name="split",
    )(total, gf)


def shards(feats, weight_one, weight_two, cotangent):
    x = lax.axis_index("x")
    block, w1, w2 = own_block(
        feats,
        cotangent,
        jnp.transpose(weight_one, (2, 0, 1)),
        jnp.transpose(weight_two, (2, 1, 0)),
    )
    up = depth_shift(block, ROW)
    down = depth_shift(block, -ROW)

    bands = band_weights(w1, w2)

    three = jnp.concatenate([up, block, down], axis=0)
    slots = [
        lax.dynamic_slice_in_dim(
            three, jnp.where(x > t, 0, jnp.where(x == t, 8, 20)).astype(jnp.int32), 40, 0
        )
        for t in range(4)
    ]
    own = lax.all_to_all(jnp.stack(slots, 0), "x", 0, 0, tiled=True)
    oth = lax.ppermute(own, "chan", [(0, 1), (1, 0)])
    own_fields, own_sums = own_half(own, bands[0])
    grad_feats, part = levels((own, oth, own_fields, own_sums), bands[1:])
    one, two, grad_feats = split_total(total_over_depth(part), grad_feats)
    grad_weight_one = jnp.transpose(one.reshape(27, 16, 32), (2, 1, 0))
    grad_weight_two = jnp.transpose(two.reshape(27, 16, 64), (2, 1, 0))
    return (grad_feats, grad_weight_one, grad_weight_two)


def solution(mesh):
    finer = Mesh(
        mesh.devices.reshape(8, 8, 4, mesh.shape["chan"]), DEPTH + ("chan",)
    )
    in_specs = (P("chan", DEPTH, None, None), P(), P(), P("chan", DEPTH, None, None))
    out_specs = (P("chan", DEPTH, None, None), P(None, "chan", None), P(None, "chan", None))

    return jax.shard_map(
        shards, mesh=finer, in_specs=in_specs, out_specs=out_specs, check_vma=False
    )
```

```python
import jax
import jax.numpy as jnp
from jax import lax
from jax.experimental import pallas as pl
from jax.experimental.pallas import tpu as pltpu
from jax.sharding import Mesh
from jax.sharding import PartitionSpec as P


DEPTH = ("z", "y", "x")
SLABS = 256
ROW = 4
BF16 = jnp.bfloat16
F32 = jnp.float32


def depth_shift(block, steps):
    pairs = [(i, i + steps) for i in range(SLABS) if 0 <= i + steps < SLABS]
    return lax.ppermute(block, DEPTH, pairs)


def slope(pre):
    sig = jax.nn.sigmoid(pre)
    return sig * (1.0 + pre * (1.0 - sig))


def near_groups():
    far_class = [0, 1, 0, 1, 1, 0, 1, 0]
    groups = {}
    for place in range(SLABS):
        z, y, x = place // 32, place // 4 % 8, place % 4
        rank = (x * 2 + far_class[y]) * 2 + far_class[z]
        groups.setdefault((z // 2, y // 2), {})[rank] = place
    near = [[block[rank] for rank in range(16)] for block in groups.values()]
    far = [[block[rank] for block in groups.values()] for rank in range(16)]
    return near, far


NEAR, FAR = near_groups()


def position():
    place = (lax.axis_index("z") * 8 + lax.axis_index("y")) * 4 + lax.axis_index("x")
    return lax.axis_index("chan"), place


def gather_kernel(feats_far, cot_far, block, feats, cot, sems):
    pairs = ((feats_far, feats), (cot_far, cot))
    copies = [
        pltpu.make_async_copy(source, target, sems.at[index])
        for index, (source, target) in enumerate(pairs)
    ]
    for copy in copies:
        copy.start()
    copies[0].wait()
    for p in range(2):
        plane = jnp.transpose(feats[:, p].astype(F32), (1, 0, 2))
        block[p * 8 : (p + 1) * 8] = plane.astype(BF16)
    copies[1].wait()
    rows = jnp.transpose(cot[...].reshape(32, 4, 64).astype(F32), (1, 0, 2))
    for high in range(2):
        pair = jnp.concatenate([rows[2 * high], rows[2 * high + 1]], axis=1)
        block[16 + 2 * high : 18 + 2 * high] = pair.astype(BF16).reshape(2, 16, 128)


def band_kernel(w1_far, w2_far, t1_own, t1_oth, t1t, t2, t2t, rows_one, w1, w2, sems):
    pairs = ((w1_far, w1), (w2_far, w2))
    copies = [
        pltpu.make_async_copy(source, target, sems.at[index])
        for index, (source, target) in enumerate(pairs)
    ]
    for copy in copies:
        copy.start()
    turn = position()[0] * 16
    half = pl.multiple_of(turn, 16)

    def marks_of(width, lanes, sign):
        row = lax.broadcasted_iota(jnp.int32, (3 * width, lanes), 0)
        lane = lax.broadcasted_iota(jnp.int32, (3 * width, lanes), 1)
        base = lane - (sign * (row // width - 1) * width + row % width)
        return lambda h: jnp.where(base == h * width, 1.0, 0.0).astype(BF16)

    def marks_by_core():
        row = lax.broadcasted_iota(jnp.int32, (96, 256), 0)
        lane = lax.broadcasted_iota(jnp.int32, (96, 256), 1)
        chan = (row + turn) % 32
        fits = (lane // 128 == chan // 16) & (lane % 16 == chan % 16)
        base = jnp.where(fits, lane % 128 // 16 - (row // 32 - 1), -1)
        return lambda h: jnp.where(base == h, 1.0, 0.0).astype(BF16)

    def taps_of(ref, flip):
        order = [(2 - a, 2 - c) if flip else (a, c) for a in range(3) for c in range(3)]
        return [[ref[9 * a + 3 * b + c] for b in range(3)] for a, c in order]

    def straight(ref, flip, marks, height, put):
        taps = taps_of(ref, flip)
        parts = [jnp.concatenate([tap[b] for tap in taps], axis=0) for b in range(3)]
        weights = jnp.concatenate(parts, axis=1)
        for h in range(height):
            put(h, jnp.dot(weights, marks(h), preferred_element_type=F32).astype(BF16))

    def crossed(ref, flip, marks, height, put):
        parts = [jnp.concatenate(tap, axis=0) for tap in taps_of(ref, flip)]
        weights = jnp.concatenate(parts, axis=1)
        for h in range(height):
            bands = lax.dot_general(
                weights, marks(h), (((0,), (0,)), ((), ())), preferred_element_type=F32
            )
            put(h, bands.astype(BF16))

    def into(out, rows, lanes):
        def put(h, bands):
            for tap in range(9):
                out[h * rows : (h + 1) * rows, tap * lanes : (tap + 1) * lanes] = bands[
                    tap * rows : (tap + 1) * rows
                ]

        return put

    def put_half(h, bands):
        rows_one[h] = bands
        for tap in range(9):
            t1t[h * 16 : (h + 1) * 16, tap * 256 : (tap + 1) * 256] = rows_one[
                h, pl.ds(tap * 32 + half, 16), :
            ]

    def put_both(h, bands):
        for tap in range(9):
            for side, out in ((0, t1_own), (128, t1_oth)):
                out[h * 32 : (h + 1) * 32, tap * 128 : (tap + 1) * 128] = bands[
                    tap * 32 : (tap + 1) * 32, side : side + 128
                ]

    copies[0].wait()
    straight(w1, False, marks_by_core(), 8, put_both)
    crossed(w1, True, marks_of(32, 256, -1), 8, put_half)
    copies[1].wait()
    crossed(w2, False, marks_of(32, 128, 1), 4, into(t2, 64, 128))
    straight(w2, True, marks_of(64, 256, -1), 4, into(t2t, 32, 256))


def shifted(value, step):
    value = value.astype(BF16)
    lanes = value.shape[-1]
    lane = lax.broadcasted_iota(jnp.int32, (1, lanes), 1)
    inner = jnp.where(lane < step, 0.0, 1.0).astype(BF16)
    outer = jnp.where(lane >= lanes - step, 0.0, 1.0).astype(BF16)
    low = pltpu.roll(value, step, 1) * inner
    high = pltpu.roll(value, lanes - step, 1) * outer
    return low, value, high


def plane_tiles(x):
    def slot(delta):
        return lax.rem(x + delta + 4, 4)

    planes = [(slot(0), 0)]
    planes += [(slot(delta), 8 * p) for delta in (-3, -2, -1) for p in range(2)]
    planes += [(slot(0), 12), (slot(0), 20)]
    planes += [(slot(delta), 20 + 8 * p) for delta in (1, 2, 3) for p in range(2)]
    return planes + [(slot(0), 32)]


def convolve_half(tiles, bands, fields, use):
    planes = plane_tiles(lax.rem(position()[1], ROW))

    def load_plane(j):
        at, start = planes[j]
        plane = tiles[at, start : start + 8].reshape(128, 128)
        for c, part in enumerate(shifted(plane, 1)):
            if j <= 8:
                fields[j, c, :, :128] = part
            if j >= 7:
                fields[j - 7, c, :, 128:] = part

    for j in (0, 1, 7, 8):
        load_plane(j)
    for k in range(7):
        for j in (k + 2, k + 9):
            if j not in (7, 8) and j < 16:
                load_plane(j)
        field = fields[k : k + 3].reshape(1152, 256)
        use(k, jnp.dot(bands[...], field, preferred_element_type=F32))


def own_kernel(own, t1_own, fields, sums):
    def use(k, part):
        sums[k] = part

    convolve_half(own, t1_own, fields, use)


def main_kernel(
    own, oth, own_fields, own_sums, t1_oth, t1t, t2, t2t, gf, wg,
    XP, PS, SL, QP, GP, HP, CT, FS, FP, G1, G2,
):
    member, place = position()
    x = lax.rem(place, 4)
    half = pl.multiple_of(member * 16, 16)

    def slot(delta):
        return lax.rem(x + delta + 4, 4)

    def use(k, part):
        pre = part + own_sums[k]
        act = (pre * jax.nn.sigmoid(pre)).astype(BF16).astype(F32).reshape(4, 2, 32, 256)
        rows = (act[:, 0] + act[:, 1]).reshape(128, 256)
        PS[k] = rows[:, :128]
        PS[k + 7] = rows[:, 128:]
        if k >= 5:
            SL[k - 5] = slope(pre[:, :128])
        if k <= 1:
            SL[k + 2] = slope(pre[:, 128:])

    convolve_half(oth, t1_oth, XP, use)

    lane = lax.broadcasted_iota(jnp.int32, (128, 128), 1)
    even = lane % 2 == 0
    for c in range(3):
        QP[4, c, :, 128:] = jnp.zeros((128, 128), BF16)
    for j in range(7):
        total = PS[2 * j] + PS[2 * j + 1]
        total = total + jnp.where(even, pltpu.roll(total, 127, 1), pltpu.roll(total, 1, 1))
        at = place + (j - 3)
        factor = jnp.where((at >= 0) & (at < SLABS), 0.125, 0.0)
        pooled = (total * factor).astype(BF16)
        for c, part in enumerate(shifted(pooled, 2)):
            if j <= 4:
                QP[j, c, :, :128] = part
            if j >= 3:
                QP[j - 3, c, :, 128:] = part

    cots = [(slot(-2), 16), (slot(-1), 16), (slot(0), 28), (slot(1), 36), (slot(2), 36)]
    own_o = pl.multiple_of(member * 32, 32)
    oth_o = pl.multiple_of(32 - member * 32, 32)
    for e, (at, start) in enumerate(cots):
        for high in range(2):
            here = start + 2 * high
            CT[e, high, pl.ds(own_o, 32), :] = own[at, here : here + 2].reshape(32, 128)
            CT[e, high, pl.ds(oth_o, 32), :] = oth[at, here : here + 2].reshape(32, 128)
    row = lax.broadcasted_iota(jnp.int32, (128, 256), 0)
    col = lax.broadcasted_iota(jnp.int32, (128, 256), 1)
    spread = jnp.where(row == (col // 128) * 64 + (col % 128) // 2, 1.0, 0.0).astype(BF16)
    cot = jnp.dot(CT[...].reshape(640, 128), spread, preferred_element_type=F32)

    for e in range(3):
        pre_two = jnp.dot(t2[...], QP[e : e + 3].reshape(1152, 256), preferred_element_type=F32)
        slopes = slope(pre_two)
        for plane in (e, e + 3):
            if plane > 4:
                continue
            side = slopes[:, :128] if plane == e else slopes[:, 128:]
            base = plane * 128
            cots_of = jnp.concatenate(
                [
                    cot[base : base + 64, :128],
                    cot[base : base + 64, 128:],
                    cot[base + 64 : base + 128, :128],
                    cot[base + 64 : base + 128, 128:],
                ],
                axis=0,
            )
            grad = (cots_of * side).astype(BF16)
            for c, part in enumerate(shifted(grad, 2)):
                for m in range(3):
                    n = plane - m
                    if 0 <= n <= 2:
                        GP[m, c, :, n * 128 : (n + 1) * 128] = part
            if plane == 2:
                lanes = lax.broadcasted_iota(jnp.int32, (1, 128), 1)
                kept = grad * jnp.where(lanes % 2 == 0, 1.0, 0.0).astype(BF16)
                for b in range(3):
                    for at in range(4):
                        h = at + 1 - b
                        here = jnp.zeros((64, 128), BF16)
                        if 0 <= h < 4:
                            here = kept[h * 64 : (h + 1) * 64]
                        G2[b * 64 : (b + 1) * 64, at * 128 : (at + 1) * 128] = here

    back = jnp.dot(t2t[...], GP[...].reshape(2304, 384), preferred_element_type=F32)
    for q, f in enumerate((0, 1, 1, 2)):
        at = place + (f - 1)
        factor = jnp.where((at >= 0) & (at < SLABS), 0.125, 0.0)
        part = (back[:, f * 128 : (f + 1) * 128] * factor).reshape(4, 1, 32, 128)
        wide = jnp.concatenate([part, part], axis=1).reshape(256, 128)
        grad = (wide * SL[q]).astype(BF16)
        for c, piece in enumerate(shifted(grad, 1)):
            if q <= 2:
                HP[q, c, :, :128] = piece
            if q >= 1:
                HP[q - 1, c, :, 128:] = piece
            if c == 1 and q in (1, 2):
                for b in range(3):
                    for at in range(8):
                        h = at + 1 - b
                        here = jnp.zeros((32, 128), BF16)
                        if 0 <= h < 8:
                            here = piece[h * 32 : (h + 1) * 32]
                        to = (q - 1) * 128 + (64, 96, 0)[b]
                        G1[to : to + 32, at * 128 : (at + 1) * 128] = here
    for q in range(2):
        G1[q * 128 + 32 : q * 128 + 64] = jnp.zeros((32, 1024), BF16)

    out = jnp.dot(t1t[...], HP[...].reshape(2304, 256), preferred_element_type=F32)
    for p in range(2):
        side = out[:, p * 128 : (p + 1) * 128].reshape(8, 16, 128)
        gf[:, p] = jnp.transpose(side, (1, 0, 2)).astype(BF16)

    for c in range(3):
        for j in range(4):
            m, side = (j + 6, 0) if j <= 2 else (2, 128)
            to = (j * 3 + c) * 16
            for h in range(8):
                FS[to : to + 16, h * 128 : (h + 1) * 128] = own_fields[
                    m, c, h * 16 : h * 16 + 16, side : side + 128
                ]
        for a in range(3):
            to = (a * 3 + c) * 16
            for h in range(4):
                FP[to : to + 16, h * 128 : (h + 1) * 128] = QP[
                    2 + a, c, pl.ds(h * 32 + half, 16), :128
                ]
    along = (((1,), (1,)), ((), ()))
    one = lax.dot_general(FS[...], G1[...], along, preferred_element_type=F32)
    two = lax.dot_general(FP[...], G2[...], along, preferred_element_type=F32)
    one = one[0:144, :128] + one[48:192, 128:]
    wg[0:144] = jnp.concatenate([two[:, 128:], one[:, 64:]], axis=1).astype(BF16)
    wg[144:288] = two[:, :128].astype(BF16)
    thirds = [one[at : at + 48, :32] for at in (0, 48, 96)]
    rest = jnp.concatenate(thirds + [jnp.zeros((48, 32), F32)], axis=1)
    wg[288:336] = rest.astype(BF16)
    wg[336:] = jnp.zeros((48, 128), BF16)


def far_operands(*arrays):
    return [pltpu.with_memory_space_constraint(array, pltpu.HBM) for array in arrays]


def own_block(feats, cot):
    hbm = pl.BlockSpec(memory_space=pltpu.MemorySpace.HBM)
    return pl.pallas_call(
        gather_kernel,
        in_specs=[hbm] * 2,
        out_specs=pl.BlockSpec(memory_space=pltpu.VMEM),
        out_shape=jax.ShapeDtypeStruct((20, 16, 128), BF16),
        scratch_shapes=[
            pltpu.VMEM(feats.shape, BF16),
            pltpu.VMEM(cot.shape, BF16),
            pltpu.SemaphoreType.DMA((2,)),
        ],
        compiler_params=pltpu.CompilerParams(vmem_limit_bytes=4 * 2**20),
        name="gather",
    )(*far_operands(feats, cot))


def band_weights(w1, w2):
    hbm = pl.BlockSpec(memory_space=pltpu.MemorySpace.HBM)
    shapes = [(256, 1152), (256, 1152), (128, 2304), (256, 1152), (128, 2304)]
    return pl.pallas_call(
        band_kernel,
        in_specs=[hbm] * 2,
        out_specs=[pl.BlockSpec(memory_space=pltpu.VMEM)] * 5,
        out_shape=[jax.ShapeDtypeStruct(shape, BF16) for shape in shapes],
        scratch_shapes=[
            pltpu.VMEM((8, 288, 256), BF16),
            pltpu.VMEM(w1.shape, BF16),
            pltpu.VMEM(w2.shape, BF16),
            pltpu.SemaphoreType.DMA((2,)),
        ],
        cost_estimate=pl.CostEstimate(flops=10**9, bytes_accessed=4 * 10**6, transcendentals=0),
        compiler_params=pltpu.CompilerParams(vmem_limit_bytes=16 * 2**20),
        name="bands",
    )(*far_operands(w1, w2))


def own_half(own, t1_own):
    vmem = pl.BlockSpec(memory_space=pltpu.VMEM)
    return pl.pallas_call(
        own_kernel,
        in_specs=[vmem, vmem],
        out_specs=[vmem, vmem],
        out_shape=[
            jax.ShapeDtypeStruct((9, 3, 128, 256), BF16),
            jax.ShapeDtypeStruct((7, 256, 256), F32),
        ],
        cost_estimate=pl.CostEstimate(flops=10**9, bytes_accessed=5 * 10**6, transcendentals=0),
        compiler_params=pltpu.CompilerParams(vmem_limit_bytes=12 * 2**20),
        name="half",
    )(own, t1_own)


def levels(fields, bands):
    vmem = pl.BlockSpec(memory_space=pltpu.VMEM)
    scratch = [
        ((9, 3, 128, 256), BF16),
        ((14, 128, 128), F32),
        ((4, 256, 128), F32),
        ((5, 3, 128, 256), BF16),
        ((3, 3, 256, 384), BF16),
        ((3, 3, 256, 256), BF16),
        ((5, 2, 64, 128), BF16),
        ((192, 1024), BF16),
        ((144, 512), BF16),
        ((256, 1024), BF16),
        ((192, 512), BF16),
    ]
    return pl.pallas_call(
        main_kernel,
        in_specs=[vmem] * 8,
        out_specs=[vmem, vmem],
        out_shape=[
            jax.ShapeDtypeStruct((16, 2, 8, 128), BF16),
            jax.ShapeDtypeStruct((384, 128), BF16),
        ],
        scratch_shapes=[pltpu.VMEM(shape, dtype) for shape, dtype in scratch],
        cost_estimate=pl.CostEstimate(
            flops=10**10, bytes_accessed=8 * 10**6, transcendentals=10**6
        ),
        compiler_params=pltpu.CompilerParams(vmem_limit_bytes=28 * 2**20),
        name="levels",
    )(*fields, *bands)


def exchange(pieces, groups):
    return lax.all_to_all(pieces, DEPTH, 0, 0, axis_index_groups=groups, tiled=True)


def total_over_depth(part):
    pieces = exchange(part.reshape(16, 24, 128), NEAR)
    for groups in (FAR, NEAR):
        total = jnp.sum(pieces.astype(F32), axis=0).astype(BF16)
        pieces = exchange(jnp.broadcast_to(total, (16, 24, 128)), groups)
    return pieces


def split_kernel(total, gf, one_out, two_out, gf_out, one, two, sems):
    pairs = ((gf, gf_out), (one, one_out), (two, two_out))
    away = [
        pltpu.make_async_copy(source, target, sems.at[index])
        for index, (source, target) in enumerate(pairs)
    ]
    away[0].start()
    rows = total[...].reshape(384, 128).astype(F32)
    for a in range(3):
        for c in range(3):
            at = (a * 3 + c) * 16
            first = rows[at : at + 16]
            rest = rows[288 + at % 48 : 304 + at % 48]
            third = at // 48 * 32
            ones = (first[:, 64:96], first[:, 96:], rest[:, third : third + 32])
            for b in range(3):
                to = ((a * 3 + b) * 3 + c) * 16
                one[to : to + 16] = ones[b]
    away[1].start()
    for a in range(3):
        for c in range(3):
            at = (a * 3 + c) * 16
            first, second = rows[at : at + 16], rows[144 + at : 160 + at]
            twos = (second[:, :64], second[:, 64:], first[:, :64])
            for b in range(3):
                to = ((a * 3 + b) * 3 + c) * 16
                two[to : to + 16] = twos[b]
    away[2].start()
    for copy in away:
        copy.wait()


def split_total(total, gf):
    vmem = pl.BlockSpec(memory_space=pltpu.VMEM)
    shapes = [(432, 32), (432, 64)]
    return pl.pallas_call(
        split_kernel,
        in_specs=[vmem, vmem],
        out_specs=[pl.BlockSpec(memory_space=pl.ANY)] * 3,
        out_shape=[jax.ShapeDtypeStruct(shape, F32) for shape in shapes]
        + [jax.ShapeDtypeStruct(gf.shape, BF16)],
        scratch_shapes=[pltpu.VMEM(shape, F32) for shape in shapes]
        + [pltpu.SemaphoreType.DMA((3,))],
        compiler_params=pltpu.CompilerParams(vmem_limit_bytes=4 * 2**20),
        name="split",
    )(total, gf)


def shards(feats, weight_one, weight_two, cotangent):
    x = lax.axis_index("x")
    block = own_block(feats, cotangent)
    up = depth_shift(block, ROW)
    down = depth_shift(block, -ROW)

    bands = band_weights(
        jnp.transpose(weight_one, (2, 0, 1)), jnp.transpose(weight_two, (2, 1, 0))
    )

    three = jnp.concatenate([up, block, down], axis=0)
    slots = [
        lax.dynamic_slice_in_dim(
            three, jnp.where(x > t, 0, jnp.where(x == t, 8, 20)).astype(jnp.int32), 40, 0
        )
        for t in range(4)
    ]
    own = lax.all_to_all(jnp.stack(slots, 0), "x", 0, 0, tiled=True)
    oth = lax.ppermute(own, "chan", [(0, 1), (1, 0)])
    own_fields, own_sums = own_half(own, bands[0])
    grad_feats, part = levels((own, oth, own_fields, own_sums), bands[1:])
    one, two, grad_feats = split_total(total_over_depth(part), grad_feats)
    grad_weight_one = jnp.transpose(one.reshape(27, 16, 32), (2, 1, 0))
    grad_weight_two = jnp.transpose(two.reshape(27, 16, 64), (2, 1, 0))
    return (grad_feats, grad_weight_one, grad_weight_two)


def solution(mesh):
    finer = Mesh(
        mesh.devices.reshape(8, 8, 4, mesh.shape["chan"]), DEPTH + ("chan",)
    )
    in_specs = (P("chan", DEPTH, None, None), P(), P(), P("chan", DEPTH, None, None))
    out_specs = (P("chan", DEPTH, None, None), P(None, "chan", None), P(None, "chan", None))

    return jax.shard_map(
        shards, mesh=finer, in_specs=in_specs, out_specs=out_specs, check_vma=False
    )
```

```python
import jax
import jax.numpy as jnp
from jax import lax
from jax.experimental import pallas as pl
from jax.experimental.pallas import tpu as pltpu
from jax.sharding import Mesh
from jax.sharding import PartitionSpec as P


DEPTH = ("z", "y", "x")
SLABS = 256
ROW = 4
BF16 = jnp.bfloat16
F32 = jnp.float32


def row_swap(block, first):
    pairs = []
    for low in range(first, SLABS // ROW - 1, 2):
        for x in range(ROW):
            here, there = low * ROW + x, (low + 1) * ROW + x
            pairs += [(here, there), (there, here)]
    return lax.ppermute(block, DEPTH, pairs)


def slope(pre):
    sig = jax.nn.sigmoid(pre)
    return sig * (1.0 + pre * (1.0 - sig))


def near_groups():
    far_class = [0, 1, 0, 1, 1, 0, 1, 0]
    groups = {}
    for place in range(SLABS):
        z, y, x = place // 32, place // 4 % 8, place % 4
        rank = (x * 2 + far_class[y]) * 2 + far_class[z]
        groups.setdefault((z // 2, y // 2), {})[rank] = place
    near = [[block[rank] for rank in range(16)] for block in groups.values()]
    far = [[block[rank] for block in groups.values()] for rank in range(16)]
    return near, far


NEAR, FAR = near_groups()


def position():
    place = (lax.axis_index("z") * 8 + lax.axis_index("y")) * 4 + lax.axis_index("x")
    return lax.axis_index("chan"), place


def gather_kernel(feats_far, cot_far, w1, w2, block, w1_near, w2_near, feats, cot, sems):
    pairs = ((feats_far, feats), (cot_far, cot), (w1, w1_near), (w2, w2_near))
    copies = [
        pltpu.make_async_copy(source, target, sems.at[index])
        for index, (source, target) in enumerate(pairs)
    ]
    for copy in copies:
        copy.start()
    copies[0].wait()
    for p in range(2):
        plane = jnp.transpose(feats[:, p].astype(F32), (1, 0, 2))
        block[p * 8 : (p + 1) * 8] = plane.astype(BF16)
    copies[1].wait()
    rows = jnp.transpose(cot[...].reshape(32, 4, 64).astype(F32), (1, 0, 2))
    for high in range(2):
        pair = jnp.concatenate([rows[2 * high], rows[2 * high + 1]], axis=1)
        block[16 + 2 * high : 18 + 2 * high] = pair.astype(BF16).reshape(2, 16, 128)
    for copy in copies[2:]:
        copy.wait()


def band_kernel(w1, w2, t1_own, t1_oth, t1t, t2, t2t, rows_one):
    turn = position()[0] * 16
    half = pl.multiple_of(turn, 16)

    def marks_of(width, lanes, sign):
        row = lax.broadcasted_iota(jnp.int32, (3 * width, lanes), 0)
        lane = lax.broadcasted_iota(jnp.int32, (3 * width, lanes), 1)
        base = lane - (sign * (row // width - 1) * width + row % width)
        return lambda h: jnp.where(base == h * width, 1.0, 0.0).astype(BF16)

    def marks_by_core():
        row = lax.broadcasted_iota(jnp.int32, (96, 256), 0)
        lane = lax.broadcasted_iota(jnp.int32, (96, 256), 1)
        chan = (row + turn) % 32
        fits = (lane // 128 == chan // 16) & (lane % 16 == chan % 16)
        base = jnp.where(fits, lane % 128 // 16 - (row // 32 - 1), -1)
        return lambda h: jnp.where(base == h, 1.0, 0.0).astype(BF16)

    def taps_of(ref, flip):
        order = [(2 - a, 2 - c) if flip else (a, c) for a in range(3) for c in range(3)]
        return [[ref[9 * a + 3 * b + c] for b in range(3)] for a, c in order]

    def straight(ref, flip, marks, height, put):
        taps = taps_of(ref, flip)
        parts = [jnp.concatenate([tap[b] for tap in taps], axis=0) for b in range(3)]
        weights = jnp.concatenate(parts, axis=1)
        for h in range(height):
            put(h, jnp.dot(weights, marks(h), preferred_element_type=F32).astype(BF16))

    def crossed(ref, flip, marks, height, put):
        parts = [jnp.concatenate(tap, axis=0) for tap in taps_of(ref, flip)]
        weights = jnp.concatenate(parts, axis=1)
        for h in range(height):
            bands = lax.dot_general(
                weights, marks(h), (((0,), (0,)), ((), ())), preferred_element_type=F32
            )
            put(h, bands.astype(BF16))

    def into(out, rows, lanes):
        def put(h, bands):
            for tap in range(9):
                out[h * rows : (h + 1) * rows, tap * lanes : (tap + 1) * lanes] = bands[
                    tap * rows : (tap + 1) * rows
                ]

        return put

    def put_half(h, bands):
        rows_one[h] = bands
        for tap in range(9):
            t1t[h * 16 : (h + 1) * 16, tap * 256 : (tap + 1) * 256] = rows_one[
                h, pl.ds(tap * 32 + half, 16), :
            ]

    def put_both(h, bands):
        for tap in range(9):
            for side, out in ((0, t1_own), (128, t1_oth)):
                out[h * 32 : (h + 1) * 32, tap * 128 : (tap + 1) * 128] = bands[
                    tap * 32 : (tap + 1) * 32, side : side + 128
                ]

    straight(w1, False, marks_by_core(), 8, put_both)
    crossed(w1, True, marks_of(32, 256, -1), 8, put_half)
    crossed(w2, False, marks_of(32, 128, 1), 4, into(t2, 64, 128))
    straight(w2, True, marks_of(64, 256, -1), 4, into(t2t, 32, 256))


def shifted(value, step):
    lanes = value.shape[-1]
    lane = lax.broadcasted_iota(jnp.int32, value.shape, 1)
    low = jnp.where(lane < step, 0.0, pltpu.roll(value, step, 1))
    high = jnp.where(lane >= lanes - step, 0.0, pltpu.roll(value, lanes - step, 1))
    return low.astype(BF16), value.astype(BF16), high.astype(BF16)


def plane_tiles(x):
    def slot(delta):
        return lax.rem(x + delta + 4, 4)

    planes = [(slot(0), 0)]
    planes += [(slot(delta), 8 * p) for delta in (-3, -2, -1) for p in range(2)]
    planes += [(slot(0), 12), (slot(0), 20)]
    planes += [(slot(delta), 20 + 8 * p) for delta in (1, 2, 3) for p in range(2)]
    return planes + [(slot(0), 32)]


def convolve_half(tiles, bands, fields, use):
    planes = plane_tiles(lax.rem(position()[1], 4))

    def load_plane(j):
        at, start = planes[j]
        plane = tiles[at, start : start + 8].reshape(128, 128)
        for c, part in enumerate(shifted(plane.astype(F32), 1)):
            if j <= 8:
                fields[j, c, :, :128] = part
            if j >= 7:
                fields[j - 7, c, :, 128:] = part

    for j in (0, 1, 7, 8):
        load_plane(j)
    for k in range(7):
        for j in (k + 2, k + 9):
            if j not in (7, 8) and j < 16:
                load_plane(j)
        field = fields[k : k + 3].reshape(1152, 256)
        use(k, jnp.dot(bands[...], field, preferred_element_type=F32))


def own_kernel(own, t1_own, fields, sums):
    def use(k, part):
        sums[k] = part

    convolve_half(own, t1_own, fields, use)


def main_kernel(
    own, oth, own_fields, own_sums, t1_oth, t1t, t2, t2t, gf, wg,
    XP, PS, SL, QP, GP, HP, CT, FS, FP, G1, G2,
):
    member, place = position()
    x = lax.rem(place, 4)
    half = pl.multiple_of(member * 16, 16)

    def slot(delta):
        return lax.rem(x + delta + 4, 4)

    def use(k, part):
        pre = part + own_sums[k]
        act = (pre * jax.nn.sigmoid(pre)).astype(BF16).astype(F32).reshape(4, 2, 32, 256)
        rows = (act[:, 0] + act[:, 1]).reshape(128, 256)
        PS[k] = rows[:, :128]
        PS[k + 7] = rows[:, 128:]
        if k >= 5:
            SL[k - 5] = slope(pre[:, :128])
        if k <= 1:
            SL[k + 2] = slope(pre[:, 128:])

    convolve_half(oth, t1_oth, XP, use)

    lane = lax.broadcasted_iota(jnp.int32, (128, 128), 1)
    even = lane % 2 == 0
    for c in range(3):
        QP[4, c, :, 128:] = jnp.zeros((128, 128), BF16)
    for j in range(7):
        total = PS[2 * j] + PS[2 * j + 1]
        total = total + jnp.where(even, pltpu.roll(total, 127, 1), pltpu.roll(total, 1, 1))
        at = place + (j - 3)
        factor = jnp.where((at >= 0) & (at < SLABS), 0.125, 0.0)
        pooled = (total * factor).astype(BF16).astype(F32)
        for c, part in enumerate(shifted(pooled, 2)):
            if j <= 4:
                QP[j, c, :, :128] = part
            if j >= 3:
                QP[j - 3, c, :, 128:] = part

    cots = [(slot(-2), 16), (slot(-1), 16), (slot(0), 28), (slot(1), 36), (slot(2), 36)]
    own_o = pl.multiple_of(member * 32, 32)
    oth_o = pl.multiple_of(32 - member * 32, 32)
    for e, (at, start) in enumerate(cots):
        for high in range(2):
            here = start + 2 * high
            CT[e, high, pl.ds(own_o, 32), :] = own[at, here : here + 2].reshape(32, 128)
            CT[e, high, pl.ds(oth_o, 32), :] = oth[at, here : here + 2].reshape(32, 128)
    row = lax.broadcasted_iota(jnp.int32, (128, 256), 0)
    col = lax.broadcasted_iota(jnp.int32, (128, 256), 1)
    spread = jnp.where(row == (col // 128) * 64 + (col % 128) // 2, 1.0, 0.0).astype(BF16)
    cot = jnp.dot(CT[...].reshape(640, 128), spread, preferred_element_type=F32)

    for e in range(3):
        pre_two = jnp.dot(t2[...], QP[e : e + 3].reshape(1152, 256), preferred_element_type=F32)
        slopes = slope(pre_two)
        for plane in (e, e + 3):
            if plane > 4:
                continue
            side = slopes[:, :128] if plane == e else slopes[:, 128:]
            base = plane * 128
            cots_of = jnp.concatenate(
                [
                    cot[base : base + 64, :128],
                    cot[base : base + 64, 128:],
                    cot[base + 64 : base + 128, :128],
                    cot[base + 64 : base + 128, 128:],
                ],
                axis=0,
            )
            grad = (cots_of * side).astype(BF16).astype(F32)
            for c, part in enumerate(shifted(grad, 2)):
                for m in range(3):
                    n = plane - m
                    if 0 <= n <= 2:
                        GP[m, c, :, n * 128 : (n + 1) * 128] = part
            if plane == 2:
                lanes = lax.broadcasted_iota(jnp.int32, (256, 128), 1)
                kept = jnp.where(lanes % 2 == 0, grad, 0.0).astype(BF16)
                for b in range(3):
                    for at in range(4):
                        h = at + 1 - b
                        here = jnp.zeros((64, 128), BF16)
                        if 0 <= h < 4:
                            here = kept[h * 64 : (h + 1) * 64]
                        G2[b * 64 : (b + 1) * 64, at * 128 : (at + 1) * 128] = here

    back = jnp.dot(t2t[...], GP[...].reshape(2304, 384), preferred_element_type=F32)
    for q, f in enumerate((0, 1, 1, 2)):
        at = place + (f - 1)
        factor = jnp.where((at >= 0) & (at < SLABS), 0.125, 0.0)
        part = (back[:, f * 128 : (f + 1) * 128] * factor).reshape(4, 1, 32, 128)
        wide = jnp.concatenate([part, part], axis=1).reshape(256, 128)
        grad = (wide * SL[q]).astype(BF16).astype(F32)
        for c, piece in enumerate(shifted(grad, 1)):
            if q <= 2:
                HP[q, c, :, :128] = piece
            if q >= 1:
                HP[q - 1, c, :, 128:] = piece
            if c == 1 and q in (1, 2):
                for b in range(3):
                    for at in range(8):
                        h = at + 1 - b
                        here = jnp.zeros((32, 128), BF16)
                        if 0 <= h < 8:
                            here = piece[h * 32 : (h + 1) * 32]
                        to = (q - 1) * 128 + (64, 96, 0)[b]
                        G1[to : to + 32, at * 128 : (at + 1) * 128] = here
    for q in range(2):
        G1[q * 128 + 32 : q * 128 + 64] = jnp.zeros((32, 1024), BF16)

    out = jnp.dot(t1t[...], HP[...].reshape(2304, 256), preferred_element_type=F32)
    for p in range(2):
        side = out[:, p * 128 : (p + 1) * 128].reshape(8, 16, 128)
        gf[:, p] = jnp.transpose(side, (1, 0, 2)).astype(BF16)

    for c in range(3):
        for j in range(4):
            m, side = (j + 6, 0) if j <= 2 else (2, 128)
            to = (j * 3 + c) * 16
            for h in range(8):
                FS[to : to + 16, h * 128 : (h + 1) * 128] = own_fields[
                    m, c, h * 16 : h * 16 + 16, side : side + 128
                ]
        for a in range(3):
            to = (a * 3 + c) * 16
            for h in range(4):
                FP[to : to + 16, h * 128 : (h + 1) * 128] = QP[
                    2 + a, c, pl.ds(h * 32 + half, 16), :128
                ]
    along = (((1,), (1,)), ((), ()))
    one = lax.dot_general(FS[...], G1[...], along, preferred_element_type=F32)
    two = lax.dot_general(FP[...], G2[...], along, preferred_element_type=F32)
    one = one[0:144, :128] + one[48:192, 128:]
    wg[0:144] = jnp.concatenate([two[:, 128:], one[:, 64:]], axis=1).astype(BF16)
    wg[144:288] = two[:, :128].astype(BF16)
    thirds = [one[at : at + 48, :32] for at in (0, 48, 96)]
    rest = jnp.concatenate(thirds + [jnp.zeros((48, 32), F32)], axis=1)
    wg[288:336] = rest.astype(BF16)
    wg[336:] = jnp.zeros((48, 128), BF16)


def own_block(feats, cot, w1, w2):
    vmem = pl.BlockSpec(memory_space=pltpu.VMEM)
    hbm = pl.BlockSpec(memory_space=pltpu.MemorySpace.HBM)
    return pl.pallas_call(
        gather_kernel,
        in_specs=[hbm] * 4,
        out_specs=[vmem] * 3,
        out_shape=[
            jax.ShapeDtypeStruct((20, 16, 128), BF16),
            jax.ShapeDtypeStruct(w1.shape, BF16),
            jax.ShapeDtypeStruct(w2.shape, BF16),
        ],
        scratch_shapes=[
            pltpu.VMEM(feats.shape, BF16),
            pltpu.VMEM(cot.shape, BF16),
            pltpu.SemaphoreType.DMA((4,)),
        ],
        compiler_params=pltpu.CompilerParams(vmem_limit_bytes=4 * 2**20),
        name="gather",
    )(*[pltpu.with_memory_space_constraint(array, pltpu.HBM) for array in (feats, cot, w1, w2)])


def band_weights(w1, w2):
    vmem = pl.BlockSpec(memory_space=pltpu.VMEM)
    shapes = [(256, 1152), (256, 1152), (128, 2304), (256, 1152), (128, 2304)]
    return pl.pallas_call(
        band_kernel,
        in_specs=[vmem] * 2,
        out_specs=[vmem] * 5,
        scratch_shapes=[pltpu.VMEM((8, 288, 256), BF16)],
        out_shape=[jax.ShapeDtypeStruct(shape, BF16) for shape in shapes],
        cost_estimate=pl.CostEstimate(flops=10**9, bytes_accessed=4 * 10**6, transcendentals=0),
        compiler_params=pltpu.CompilerParams(vmem_limit_bytes=16 * 2**20),
        name="bands",
    )(w1, w2)


def own_half(own, t1_own):
    vmem = pl.BlockSpec(memory_space=pltpu.VMEM)
    return pl.pallas_call(
        own_kernel,
        in_specs=[vmem, vmem],
        out_specs=[vmem, vmem],
        out_shape=[
            jax.ShapeDtypeStruct((9, 3, 128, 256), BF16),
            jax.ShapeDtypeStruct((7, 256, 256), F32),
        ],
        cost_estimate=pl.CostEstimate(flops=10**9, bytes_accessed=5 * 10**6, transcendentals=0),
        compiler_params=pltpu.CompilerParams(vmem_limit_bytes=12 * 2**20),
        name="half",
    )(own, t1_own)


def levels(fields, bands):
    vmem = pl.BlockSpec(memory_space=pltpu.VMEM)
    scratch = [
        ((9, 3, 128, 256), BF16),
        ((14, 128, 128), F32),
        ((4, 256, 128), F32),
        ((5, 3, 128, 256), BF16),
        ((3, 3, 256, 384), BF16),
        ((3, 3, 256, 256), BF16),
        ((5, 2, 64, 128), BF16),
        ((192, 1024), BF16),
        ((144, 512), BF16),
        ((256, 1024), BF16),
        ((192, 512), BF16),
    ]
    return pl.pallas_call(
        main_kernel,
        in_specs=[vmem] * 8,
        out_specs=[vmem, vmem],
        out_shape=[
            jax.ShapeDtypeStruct((16, 2, 8, 128), BF16),
            jax.ShapeDtypeStruct((384, 128), BF16),
        ],
        scratch_shapes=[pltpu.VMEM(shape, dtype) for shape, dtype in scratch],
        cost_estimate=pl.CostEstimate(
            flops=10**10, bytes_accessed=8 * 10**6, transcendentals=10**6
        ),
        compiler_params=pltpu.CompilerParams(vmem_limit_bytes=28 * 2**20),
        name="levels",
    )(*fields, *bands)


def exchange(pieces, groups):
    return lax.all_to_all(pieces, DEPTH, 0, 0, axis_index_groups=groups, tiled=True)


def total_over_depth(part):
    pieces = exchange(part.reshape(16, 24, 128), NEAR)
    for groups in (FAR, NEAR):
        total = jnp.sum(pieces.astype(F32), axis=0).astype(BF16)
        pieces = exchange(jnp.broadcast_to(total, (16, 24, 128)), groups)
    return pieces


def split_kernel(total, gf, one_out, two_out, gf_out, one, two, sems):
    pairs = ((gf, gf_out), (one, one_out), (two, two_out))
    away = [
        pltpu.make_async_copy(source, target, sems.at[index])
        for index, (source, target) in enumerate(pairs)
    ]
    away[0].start()
    rows = total[...].reshape(384, 128).astype(F32)
    for a in range(3):
        for c in range(3):
            at = (a * 3 + c) * 16
            first = rows[at : at + 16]
            rest = rows[288 + at % 48 : 304 + at % 48]
            third = at // 48 * 32
            ones = (first[:, 64:96], first[:, 96:], rest[:, third : third + 32])
            for b in range(3):
                to = ((a * 3 + b) * 3 + c) * 16
                one[to : to + 16] = ones[b]
    away[1].start()
    for a in range(3):
        for c in range(3):
            at = (a * 3 + c) * 16
            first, second = rows[at : at + 16], rows[144 + at : 160 + at]
            twos = (second[:, :64], second[:, 64:], first[:, :64])
            for b in range(3):
                to = ((a * 3 + b) * 3 + c) * 16
                two[to : to + 16] = twos[b]
    away[2].start()
    for copy in away:
        copy.wait()


def split_total(total, gf):
    vmem = pl.BlockSpec(memory_space=pltpu.VMEM)
    shapes = [(432, 32), (432, 64)]
    return pl.pallas_call(
        split_kernel,
        in_specs=[vmem, vmem],
        out_specs=[pl.BlockSpec(memory_space=pl.ANY)] * 3,
        out_shape=[jax.ShapeDtypeStruct(shape, F32) for shape in shapes]
        + [jax.ShapeDtypeStruct(gf.shape, BF16)],
        scratch_shapes=[pltpu.VMEM(shape, F32) for shape in shapes]
        + [pltpu.SemaphoreType.DMA((3,))],
        compiler_params=pltpu.CompilerParams(vmem_limit_bytes=4 * 2**20),
        name="split",
    )(total, gf)


def shards(feats, weight_one, weight_two, cotangent):
    x = lax.axis_index("x")
    block, w1, w2 = own_block(
        feats,
        cotangent,
        jnp.transpose(weight_one, (2, 0, 1)),
        jnp.transpose(weight_two, (2, 1, 0)),
    )
    even = row_swap(block, 0)
    odd = row_swap(block, 1)
    upper = lax.axis_index("y") % 2 == 1
    up, down = jnp.where(upper, even, odd), jnp.where(upper, odd, even)

    bands = band_weights(w1, w2)

    three = jnp.concatenate([up, block, down], axis=0)
    slots = [
        lax.dynamic_slice_in_dim(
            three, jnp.where(x > t, 0, jnp.where(x == t, 8, 20)).astype(jnp.int32), 40, 0
        )
        for t in range(4)
    ]
    own = lax.all_to_all(jnp.stack(slots, 0), "x", 0, 0, tiled=True)
    oth = lax.ppermute(own, "chan", [(0, 1), (1, 0)])
    own_fields, own_sums = own_half(own, bands[0])
    grad_feats, part = levels((own, oth, own_fields, own_sums), bands[1:])
    one, two, grad_feats = split_total(total_over_depth(part), grad_feats)
    grad_weight_one = jnp.transpose(one.reshape(27, 16, 32), (2, 1, 0))
    grad_weight_two = jnp.transpose(two.reshape(27, 16, 64), (2, 1, 0))
    return (grad_feats, grad_weight_one, grad_weight_two)


def solution(mesh):
    finer = Mesh(
        mesh.devices.reshape(8, 8, 4, mesh.shape["chan"]), DEPTH + ("chan",)
    )
    in_specs = (P("chan", DEPTH, None, None), P(), P(), P("chan", DEPTH, None, None))
    out_specs = (P("chan", DEPTH, None, None), P(None, "chan", None), P(None, "chan", None))

    return jax.shard_map(
        shards, mesh=finer, in_specs=in_specs, out_specs=out_specs, check_vma=False
    )
```

```python
import jax
import jax.numpy as jnp
from jax import lax
from jax.experimental import pallas as pl
from jax.experimental.pallas import tpu as pltpu
from jax.sharding import Mesh
from jax.sharding import PartitionSpec as P


DEPTH = ("z", "y", "x")
SLABS = 256
ROW = 4
BF16 = jnp.bfloat16
F32 = jnp.float32


def row_swap(block, first):
    pairs = []
    for low in range(first, SLABS // ROW - 1, 2):
        for x in range(ROW):
            here, there = low * ROW + x, (low + 1) * ROW + x
            pairs += [(here, there), (there, here)]
    return lax.ppermute(block, DEPTH, pairs)


def slope(pre):
    sig = jax.nn.sigmoid(pre)
    return sig * (1.0 + pre * (1.0 - sig))


def near_groups():
    far_class = [0, 1, 0, 1, 1, 0, 1, 0]
    groups = {}
    for place in range(SLABS):
        z, y, x = place // 32, place // 4 % 8, place % 4
        rank = (x * 2 + far_class[y]) * 2 + far_class[z]
        groups.setdefault((z // 2, y // 2), {})[rank] = place
    near = [[block[rank] for rank in range(16)] for block in groups.values()]
    far = [[block[rank] for block in groups.values()] for rank in range(16)]
    return near, far


NEAR, FAR = near_groups()


def position():
    place = (lax.axis_index("z") * 8 + lax.axis_index("y")) * 4 + lax.axis_index("x")
    return lax.axis_index("chan"), place


def gather_kernel(feats_far, cot_far, w1, w2, block, w1_near, w2_near, feats, cot, sems):
    pairs = ((feats_far, feats), (cot_far, cot), (w1, w1_near), (w2, w2_near))
    copies = [
        pltpu.make_async_copy(source, target, sems.at[index])
        for index, (source, target) in enumerate(pairs)
    ]
    for copy in copies:
        copy.start()
    copies[0].wait()
    for p in range(2):
        plane = jnp.transpose(feats[:, p].astype(F32), (1, 0, 2))
        block[p * 8 : (p + 1) * 8] = plane.astype(BF16)
    copies[1].wait()
    rows = jnp.transpose(cot[...].reshape(32, 4, 64).astype(F32), (1, 0, 2))
    for high in range(2):
        pair = jnp.concatenate([rows[2 * high], rows[2 * high + 1]], axis=1)
        block[16 + 2 * high : 18 + 2 * high] = pair.astype(BF16).reshape(2, 16, 128)
    for copy in copies[2:]:
        copy.wait()


def band_kernel(w1, w2, t1_own, t1_oth, t1t, t2, t2t, rows_one):
    turn = position()[0] * 16
    half = pl.multiple_of(turn, 16)

    def marks_of(width, lanes, sign):
        row = lax.broadcasted_iota(jnp.int32, (3 * width, lanes), 0)
        lane = lax.broadcasted_iota(jnp.int32, (3 * width, lanes), 1)
        base = lane - (sign * (row // width - 1) * width + row % width)
        return lambda h: jnp.where(base == h * width, 1.0, 0.0).astype(BF16)

    def marks_by_core():
        row = lax.broadcasted_iota(jnp.int32, (96, 256), 0)
        lane = lax.broadcasted_iota(jnp.int32, (96, 256), 1)
        chan = (row + turn) % 32
        fits = (lane // 128 == chan // 16) & (lane % 16 == chan % 16)
        base = jnp.where(fits, lane % 128 // 16 - (row // 32 - 1), -1)
        return lambda h: jnp.where(base == h, 1.0, 0.0).astype(BF16)

    def taps_of(ref, flip):
        order = [(2 - a, 2 - c) if flip else (a, c) for a in range(3) for c in range(3)]
        return [[ref[9 * a + 3 * b + c] for b in range(3)] for a, c in order]

    def straight(ref, flip, marks, height, put):
        taps = taps_of(ref, flip)
        parts = [jnp.concatenate([tap[b] for tap in taps], axis=0) for b in range(3)]
        weights = jnp.concatenate(parts, axis=1)
        for h in range(height):
            put(h, jnp.dot(weights, marks(h), preferred_element_type=F32).astype(BF16))

    def crossed(ref, flip, marks, height, put):
        parts = [jnp.concatenate(tap, axis=0) for tap in taps_of(ref, flip)]
        weights = jnp.concatenate(parts, axis=1)
        for h in range(height):
            bands = lax.dot_general(
                weights, marks(h), (((0,), (0,)), ((), ())), preferred_element_type=F32
            )
            put(h, bands.astype(BF16))

    def into(out, rows, lanes):
        def put(h, bands):
            for tap in range(9):
                out[h * rows : (h + 1) * rows, tap * lanes : (tap + 1) * lanes] = bands[
                    tap * rows : (tap + 1) * rows
                ]

        return put

    def put_half(h, bands):
        rows_one[h] = bands
        for tap in range(9):
            t1t[h * 16 : (h + 1) * 16, tap * 256 : (tap + 1) * 256] = rows_one[
                h, pl.ds(tap * 32 + half, 16), :
            ]

    def put_both(h, bands):
        for tap in range(9):
            for side, out in ((0, t1_own), (128, t1_oth)):
                out[h * 32 : (h + 1) * 32, tap * 128 : (tap + 1) * 128] = bands[
                    tap * 32 : (tap + 1) * 32, side : side + 128
                ]

    straight(w1, False, marks_by_core(), 8, put_both)
    crossed(w1, True, marks_of(32, 256, -1), 8, put_half)
    crossed(w2, False, marks_of(32, 128, 1), 4, into(t2, 64, 128))
    straight(w2, True, marks_of(64, 256, -1), 4, into(t2t, 32, 256))


def shifted(value, step):
    lanes = value.shape[-1]
    lane = lax.broadcasted_iota(jnp.int32, value.shape, 1)
    low = jnp.where(lane < step, 0.0, pltpu.roll(value, step, 1))
    high = jnp.where(lane >= lanes - step, 0.0, pltpu.roll(value, lanes - step, 1))
    return low.astype(BF16), value.astype(BF16), high.astype(BF16)


def plane_tiles(x):
    def slot(delta):
        return lax.rem(x + delta + 4, 4)

    planes = [(slot(0), 0)]
    planes += [(slot(delta), 8 * p) for delta in (-3, -2, -1) for p in range(2)]
    planes += [(slot(0), 12), (slot(0), 20)]
    planes += [(slot(delta), 20 + 8 * p) for delta in (1, 2, 3) for p in range(2)]
    return planes + [(slot(0), 32)]


def convolve_half(tiles, bands, fields, use):
    planes = plane_tiles(lax.rem(position()[1], 4))

    def load_plane(j):
        at, start = planes[j]
        plane = tiles[at, start : start + 8].reshape(128, 128)
        for c, part in enumerate(shifted(plane.astype(F32), 1)):
            if j <= 8:
                fields[j, c, :, :128] = part
            if j >= 7:
                fields[j - 7, c, :, 128:] = part

    for j in (0, 1, 7, 8):
        load_plane(j)
    for k in range(7):
        for j in (k + 2, k + 9):
            if j not in (7, 8) and j < 16:
                load_plane(j)
        field = fields[k : k + 3].reshape(1152, 256)
        use(k, jnp.dot(bands[...], field, preferred_element_type=F32))


def own_kernel(own, t1_own, fields, sums):
    def use(k, part):
        sums[k] = part

    convolve_half(own, t1_own, fields, use)


def main_kernel(
    own, oth, own_fields, own_sums, t1_oth, t1t, t2, t2t, gf, wg,
    XP, PS, SL, QP, GP, HP, CT, FS, FP, G1, G2,
):
    member, place = position()
    x = lax.rem(place, 4)
    half = pl.multiple_of(member * 16, 16)

    def slot(delta):
        return lax.rem(x + delta + 4, 4)

    def use(k, part):
        pre = part + own_sums[k]
        act = (pre * jax.nn.sigmoid(pre)).astype(BF16).astype(F32).reshape(4, 2, 32, 256)
        rows = (act[:, 0] + act[:, 1]).reshape(128, 256)
        PS[k] = rows[:, :128]
        PS[k + 7] = rows[:, 128:]
        if k >= 5:
            SL[k - 5] = slope(pre[:, :128])
        if k <= 1:
            SL[k + 2] = slope(pre[:, 128:])

    convolve_half(oth, t1_oth, XP, use)

    lane = lax.broadcasted_iota(jnp.int32, (128, 128), 1)
    even = lane % 2 == 0
    for c in range(3):
        QP[4, c, :, 128:] = jnp.zeros((128, 128), BF16)
    for j in range(7):
        total = PS[2 * j] + PS[2 * j + 1]
        total = total + jnp.where(even, pltpu.roll(total, 127, 1), pltpu.roll(total, 1, 1))
        at = place + (j - 3)
        factor = jnp.where((at >= 0) & (at < SLABS), 0.125, 0.0)
        pooled = (total * factor).astype(BF16).astype(F32)
        for c, part in enumerate(shifted(pooled, 2)):
            if j <= 4:
                QP[j, c, :, :128] = part
            if j >= 3:
                QP[j - 3, c, :, 128:] = part

    cots = [(slot(-2), 16), (slot(-1), 16), (slot(0), 28), (slot(1), 36), (slot(2), 36)]
    own_o = pl.multiple_of(member * 32, 32)
    oth_o = pl.multiple_of(32 - member * 32, 32)
    for e, (at, start) in enumerate(cots):
        for high in range(2):
            here = start + 2 * high
            CT[e, high, pl.ds(own_o, 32), :] = own[at, here : here + 2].reshape(32, 128)
            CT[e, high, pl.ds(oth_o, 32), :] = oth[at, here : here + 2].reshape(32, 128)
    row = lax.broadcasted_iota(jnp.int32, (128, 256), 0)
    col = lax.broadcasted_iota(jnp.int32, (128, 256), 1)
    spread = jnp.where(row == (col // 128) * 64 + (col % 128) // 2, 1.0, 0.0).astype(BF16)
    cot = jnp.dot(CT[...].reshape(640, 128), spread, preferred_element_type=F32)

    for e in range(3):
        pre_two = jnp.dot(t2[...], QP[e : e + 3].reshape(1152, 256), preferred_element_type=F32)
        slopes = slope(pre_two)
        for plane in (e, e + 3):
            if plane > 4:
                continue
            side = slopes[:, :128] if plane == e else slopes[:, 128:]
            base = plane * 128
            cots_of = jnp.concatenate(
                [
                    cot[base : base + 64, :128],
                    cot[base : base + 64, 128:],
                    cot[base + 64 : base + 128, :128],
                    cot[base + 64 : base + 128, 128:],
                ],
                axis=0,
            )
            grad = (cots_of * side).astype(BF16).astype(F32)
            for c, part in enumerate(shifted(grad, 2)):
                for m in range(3):
                    n = plane - m
                    if 0 <= n <= 2:
                        GP[m, c, :, n * 128 : (n + 1) * 128] = part
            if plane == 2:
                lanes = lax.broadcasted_iota(jnp.int32, (256, 128), 1)
                kept = jnp.where(lanes % 2 == 0, grad, 0.0).astype(BF16)
                for b in range(3):
                    for at in range(4):
                        h = at + 1 - b
                        here = jnp.zeros((64, 128), BF16)
                        if 0 <= h < 4:
                            here = kept[h * 64 : (h + 1) * 64]
                        G2[b * 64 : (b + 1) * 64, at * 128 : (at + 1) * 128] = here

    back = jnp.dot(t2t[...], GP[...].reshape(2304, 384), preferred_element_type=F32)
    for q, f in enumerate((0, 1, 1, 2)):
        at = place + (f - 1)
        factor = jnp.where((at >= 0) & (at < SLABS), 0.125, 0.0)
        part = (back[:, f * 128 : (f + 1) * 128] * factor).reshape(4, 1, 32, 128)
        wide = jnp.concatenate([part, part], axis=1).reshape(256, 128)
        grad = (wide * SL[q]).astype(BF16).astype(F32)
        for c, piece in enumerate(shifted(grad, 1)):
            if q <= 2:
                HP[q, c, :, :128] = piece
            if q >= 1:
                HP[q - 1, c, :, 128:] = piece
            if c == 1 and q in (1, 2):
                for b in range(3):
                    for at in range(8):
                        h = at + 1 - b
                        here = jnp.zeros((32, 128), BF16)
                        if 0 <= h < 8:
                            here = piece[h * 32 : (h + 1) * 32]
                        to = (q - 1) * 128 + (64, 96, 0)[b]
                        G1[to : to + 32, at * 128 : (at + 1) * 128] = here
    for q in range(2):
        G1[q * 128 + 32 : q * 128 + 64] = jnp.zeros((32, 1024), BF16)

    out = jnp.dot(t1t[...], HP[...].reshape(2304, 256), preferred_element_type=F32)
    for p in range(2):
        side = out[:, p * 128 : (p + 1) * 128].reshape(8, 16, 128)
        gf[:, p] = jnp.transpose(side, (1, 0, 2)).astype(BF16)

    for c in range(3):
        for j in range(4):
            m, side = (j + 6, 0) if j <= 2 else (2, 128)
            to = (j * 3 + c) * 16
            for h in range(8):
                FS[to : to + 16, h * 128 : (h + 1) * 128] = own_fields[
                    m, c, h * 16 : h * 16 + 16, side : side + 128
                ]
        for a in range(3):
            to = (a * 3 + c) * 16
            for h in range(4):
                FP[to : to + 16, h * 128 : (h + 1) * 128] = QP[
                    2 + a, c, pl.ds(h * 32 + half, 16), :128
                ]
    along = (((1,), (1,)), ((), ()))
    one = lax.dot_general(FS[...], G1[...], along, preferred_element_type=F32)
    two = lax.dot_general(FP[...], G2[...], along, preferred_element_type=F32)
    one = one[0:144, :128] + one[48:192, 128:]
    wg[0:144] = jnp.concatenate([two[:, 128:], one[:, 64:]], axis=1).astype(BF16)
    wg[144:288] = two[:, :128].astype(BF16)
    thirds = [one[at : at + 48, :32] for at in (0, 48, 96)]
    rest = jnp.concatenate(thirds + [jnp.zeros((48, 32), F32)], axis=1)
    wg[288:336] = rest.astype(BF16)
    wg[336:] = jnp.zeros((48, 128), BF16)


def own_block(feats, cot, w1, w2):
    vmem = pl.BlockSpec(memory_space=pltpu.VMEM)
    hbm = pl.BlockSpec(memory_space=pltpu.MemorySpace.HBM)
    return pl.pallas_call(
        gather_kernel,
        in_specs=[hbm] * 4,
        out_specs=[vmem] * 3,
        out_shape=[
            jax.ShapeDtypeStruct((20, 16, 128), BF16),
            jax.ShapeDtypeStruct(w1.shape, BF16),
            jax.ShapeDtypeStruct(w2.shape, BF16),
        ],
        scratch_shapes=[
            pltpu.VMEM(feats.shape, BF16),
            pltpu.VMEM(cot.shape, BF16),
            pltpu.SemaphoreType.DMA((4,)),
        ],
        compiler_params=pltpu.CompilerParams(vmem_limit_bytes=4 * 2**20),
        name="gather",
    )(*[pltpu.with_memory_space_constraint(array, pltpu.HBM) for array in (feats, cot, w1, w2)])


def band_weights(w1, w2):
    vmem = pl.BlockSpec(memory_space=pltpu.VMEM)
    shapes = [(256, 1152), (256, 1152), (128, 2304), (256, 1152), (128, 2304)]
    return pl.pallas_call(
        band_kernel,
        in_specs=[vmem] * 2,
        out_specs=[vmem] * 5,
        scratch_shapes=[pltpu.VMEM((8, 288, 256), BF16)],
        out_shape=[jax.ShapeDtypeStruct(shape, BF16) for shape in shapes],
        cost_estimate=pl.CostEstimate(flops=10**9, bytes_accessed=4 * 10**6, transcendentals=0),
        compiler_params=pltpu.CompilerParams(vmem_limit_bytes=16 * 2**20),
        name="bands",
    )(w1, w2)


def slot_kernel(even, block, odd, slots, rows):
    for at, part in enumerate((even, block, odd, block, even)):
        rows[at * 20 : (at + 1) * 20] = part[...]
    place = position()[1]
    x = lax.rem(place, ROW)
    first = jnp.where(lax.rem(place // ROW, 2) == 1, 0, 40)
    for t in range(4):
        at = first + jnp.where(x > t, 0, jnp.where(x == t, 8, 20))
        slots[t] = rows[pl.ds(at, 40)]


def row_slots(even, block, odd):
    vmem = pl.BlockSpec(memory_space=pltpu.VMEM)
    return pl.pallas_call(
        slot_kernel,
        in_specs=[vmem] * 3,
        out_specs=vmem,
        out_shape=jax.ShapeDtypeStruct((4, 40, 16, 128), BF16),
        scratch_shapes=[pltpu.VMEM((100, 16, 128), BF16)],
        compiler_params=pltpu.CompilerParams(vmem_limit_bytes=4 * 2**20),
        name="slots",
    )(even, block, odd)


def own_half(own, t1_own):
    vmem = pl.BlockSpec(memory_space=pltpu.VMEM)
    return pl.pallas_call(
        own_kernel,
        in_specs=[vmem, vmem],
        out_specs=[vmem, vmem],
        out_shape=[
            jax.ShapeDtypeStruct((9, 3, 128, 256), BF16),
            jax.ShapeDtypeStruct((7, 256, 256), F32),
        ],
        cost_estimate=pl.CostEstimate(flops=10**9, bytes_accessed=5 * 10**6, transcendentals=0),
        compiler_params=pltpu.CompilerParams(vmem_limit_bytes=12 * 2**20),
        name="half",
    )(own, t1_own)


def levels(fields, bands):
    vmem = pl.BlockSpec(memory_space=pltpu.VMEM)
    scratch = [
        ((9, 3, 128, 256), BF16),
        ((14, 128, 128), F32),
        ((4, 256, 128), F32),
        ((5, 3, 128, 256), BF16),
        ((3, 3, 256, 384), BF16),
        ((3, 3, 256, 256), BF16),
        ((5, 2, 64, 128), BF16),
        ((192, 1024), BF16),
        ((144, 512), BF16),
        ((256, 1024), BF16),
        ((192, 512), BF16),
    ]
    return pl.pallas_call(
        main_kernel,
        in_specs=[vmem] * 8,
        out_specs=[vmem, vmem],
        out_shape=[
            jax.ShapeDtypeStruct((16, 2, 8, 128), BF16),
            jax.ShapeDtypeStruct((384, 128), BF16),
        ],
        scratch_shapes=[pltpu.VMEM(shape, dtype) for shape, dtype in scratch],
        cost_estimate=pl.CostEstimate(
            flops=10**10, bytes_accessed=8 * 10**6, transcendentals=10**6
        ),
        compiler_params=pltpu.CompilerParams(vmem_limit_bytes=28 * 2**20),
        name="levels",
    )(*fields, *bands)


def exchange(pieces, groups):
    return lax.all_to_all(pieces, DEPTH, 0, 0, axis_index_groups=groups, tiled=True)


def total_over_depth(part):
    pieces = exchange(part.reshape(16, 24, 128), NEAR)
    for groups in (FAR, NEAR):
        total = jnp.sum(pieces.astype(F32), axis=0).astype(BF16)
        pieces = exchange(jnp.broadcast_to(total, (16, 24, 128)), groups)
    return pieces


def split_kernel(total, gf, one_out, two_out, gf_out, one, two, sems):
    pairs = ((gf, gf_out), (one, one_out), (two, two_out))
    away = [
        pltpu.make_async_copy(source, target, sems.at[index])
        for index, (source, target) in enumerate(pairs)
    ]
    away[0].start()
    rows = total[...].reshape(384, 128).astype(F32)
    for a in range(3):
        for c in range(3):
            at = (a * 3 + c) * 16
            first = rows[at : at + 16]
            rest = rows[288 + at % 48 : 304 + at % 48]
            third = at // 48 * 32
            ones = (first[:, 64:96], first[:, 96:], rest[:, third : third + 32])
            for b in range(3):
                to = ((a * 3 + b) * 3 + c) * 16
                one[to : to + 16] = ones[b]
    away[1].start()
    for a in range(3):
        for c in range(3):
            at = (a * 3 + c) * 16
            first, second = rows[at : at + 16], rows[144 + at : 160 + at]
            twos = (second[:, :64], second[:, 64:], first[:, :64])
            for b in range(3):
                to = ((a * 3 + b) * 3 + c) * 16
                two[to : to + 16] = twos[b]
    away[2].start()
    for copy in away:
        copy.wait()


def split_total(total, gf):
    vmem = pl.BlockSpec(memory_space=pltpu.VMEM)
    shapes = [(432, 32), (432, 64)]
    return pl.pallas_call(
        split_kernel,
        in_specs=[vmem, vmem],
        out_specs=[pl.BlockSpec(memory_space=pl.ANY)] * 3,
        out_shape=[jax.ShapeDtypeStruct(shape, F32) for shape in shapes]
        + [jax.ShapeDtypeStruct(gf.shape, BF16)],
        scratch_shapes=[pltpu.VMEM(shape, F32) for shape in shapes]
        + [pltpu.SemaphoreType.DMA((3,))],
        compiler_params=pltpu.CompilerParams(vmem_limit_bytes=4 * 2**20),
        name="split",
    )(total, gf)


def shards(feats, weight_one, weight_two, cotangent):
    block, w1, w2 = own_block(
        feats,
        cotangent,
        jnp.transpose(weight_one, (2, 0, 1)),
        jnp.transpose(weight_two, (2, 1, 0)),
    )
    even = row_swap(block, 0)
    odd = row_swap(block, 1)

    bands = band_weights(w1, w2)

    own = lax.all_to_all(row_slots(even, block, odd), "x", 0, 0, tiled=True)
    oth = lax.ppermute(own, "chan", [(0, 1), (1, 0)])
    own_fields, own_sums = own_half(own, bands[0])
    grad_feats, part = levels((own, oth, own_fields, own_sums), bands[1:])
    one, two, grad_feats = split_total(total_over_depth(part), grad_feats)
    grad_weight_one = jnp.transpose(one.reshape(27, 16, 32), (2, 1, 0))
    grad_weight_two = jnp.transpose(two.reshape(27, 16, 64), (2, 1, 0))
    return (grad_feats, grad_weight_one, grad_weight_two)


def solution(mesh):
    finer = Mesh(
        mesh.devices.reshape(8, 8, 4, mesh.shape["chan"]), DEPTH + ("chan",)
    )
    in_specs = (P("chan", DEPTH, None, None), P(), P(), P("chan", DEPTH, None, None))
    out_specs = (P("chan", DEPTH, None, None), P(None, "chan", None), P(None, "chan", None))

    return jax.shard_map(
        shards, mesh=finer, in_specs=in_specs, out_specs=out_specs, check_vma=False
    )
```

```python
import jax
import jax.numpy as jnp
from jax import lax
from jax.experimental import pallas as pl
from jax.experimental.pallas import tpu as pltpu
from jax.sharding import Mesh
from jax.sharding import PartitionSpec as P


DEPTH = ("z", "y", "x")
SLABS = 256
ROW = 4
BF16 = jnp.bfloat16
F32 = jnp.float32


def row_swap(block, first):
    pairs = []
    for low in range(first, SLABS // ROW - 1, 2):
        for x in range(ROW):
            here, there = low * ROW + x, (low + 1) * ROW + x
            pairs += [(here, there), (there, here)]
    return lax.ppermute(block, DEPTH, pairs)


def slope(pre):
    sig = jax.nn.sigmoid(pre)
    return sig * (1.0 + pre * (1.0 - sig))


def near_groups():
    far_class = [0, 1, 0, 1, 1, 0, 1, 0]
    groups = {}
    for place in range(SLABS):
        z, y, x = place // 32, place // 4 % 8, place % 4
        rank = (x * 2 + far_class[y]) * 2 + far_class[z]
        groups.setdefault((z // 2, y // 2), {})[rank] = place
    near = [[block[rank] for rank in range(16)] for block in groups.values()]
    far = [[block[rank] for block in groups.values()] for rank in range(16)]
    return near, far


NEAR, FAR = near_groups()


def position():
    place = (lax.axis_index("z") * 8 + lax.axis_index("y")) * 4 + lax.axis_index("x")
    return lax.axis_index("chan"), place


def gather_kernel(feats_far, cot_far, w1, w2, block, w1_near, w2_near, feats, cot, sems):
    pairs = ((feats_far, feats), (cot_far, cot), (w1, w1_near), (w2, w2_near))
    copies = [
        pltpu.make_async_copy(source, target, sems.at[index])
        for index, (source, target) in enumerate(pairs)
    ]
    for copy in copies:
        copy.start()
    copies[0].wait()
    for p in range(2):
        plane = jnp.transpose(feats[:, p].astype(F32), (1, 0, 2))
        block[p * 8 : (p + 1) * 8] = plane.astype(BF16)
    copies[1].wait()
    rows = jnp.transpose(cot[...].reshape(32, 4, 64).astype(F32), (1, 0, 2))
    for high in range(2):
        pair = jnp.concatenate([rows[2 * high], rows[2 * high + 1]], axis=1)
        block[16 + 2 * high : 18 + 2 * high] = pair.astype(BF16).reshape(2, 16, 128)
    for copy in copies[2:]:
        copy.wait()


def band_kernel(w1, w2, t1_own, t1_oth, t1t, t2, t2t, rows_one):
    turn = position()[0] * 16
    half = pl.multiple_of(turn, 16)

    def marks_of(width, lanes, sign):
        row = lax.broadcasted_iota(jnp.int32, (3 * width, lanes), 0)
        lane = lax.broadcasted_iota(jnp.int32, (3 * width, lanes), 1)
        base = lane - (sign * (row // width - 1) * width + row % width)
        return lambda h: jnp.where(base == h * width, 1.0, 0.0).astype(BF16)

    def marks_by_core():
        row = lax.broadcasted_iota(jnp.int32, (96, 256), 0)
        lane = lax.broadcasted_iota(jnp.int32, (96, 256), 1)
        chan = (row + turn) % 32
        fits = (lane // 128 == chan // 16) & (lane % 16 == chan % 16)
        base = jnp.where(fits, lane % 128 // 16 - (row // 32 - 1), -1)
        return lambda h: jnp.where(base == h, 1.0, 0.0).astype(BF16)

    def taps_of(ref, flip):
        order = [(2 - a, 2 - c) if flip else (a, c) for a in range(3) for c in range(3)]
        return [[ref[9 * a + 3 * b + c] for b in range(3)] for a, c in order]

    def straight(ref, flip, marks, height, put):
        taps = taps_of(ref, flip)
        parts = [jnp.concatenate([tap[b] for tap in taps], axis=0) for b in range(3)]
        weights = jnp.concatenate(parts, axis=1)
        for h in range(height):
            put(h, jnp.dot(weights, marks(h), preferred_element_type=F32).astype(BF16))

    def crossed(ref, flip, marks, height, put):
        parts = [jnp.concatenate(tap, axis=0) for tap in taps_of(ref, flip)]
        weights = jnp.concatenate(parts, axis=1)
        for h in range(height):
            bands = lax.dot_general(
                weights, marks(h), (((0,), (0,)), ((), ())), preferred_element_type=F32
            )
            put(h, bands.astype(BF16))

    def into(out, rows, lanes):
        def put(h, bands):
            for tap in range(9):
                out[h * rows : (h + 1) * rows, tap * lanes : (tap + 1) * lanes] = bands[
                    tap * rows : (tap + 1) * rows
                ]

        return put

    def put_half(h, bands):
        rows_one[h] = bands
        for tap in range(9):
            t1t[h * 16 : (h + 1) * 16, tap * 256 : (tap + 1) * 256] = rows_one[
                h, pl.ds(tap * 32 + half, 16), :
            ]

    def put_both(h, bands):
        for tap in range(9):
            for side, out in ((0, t1_own), (128, t1_oth)):
                out[h * 32 : (h + 1) * 32, tap * 128 : (tap + 1) * 128] = bands[
                    tap * 32 : (tap + 1) * 32, side : side + 128
                ]

    straight(w1, False, marks_by_core(), 8, put_both)
    crossed(w1, True, marks_of(32, 256, -1), 8, put_half)
    crossed(w2, False, marks_of(32, 128, 1), 4, into(t2, 64, 128))
    straight(w2, True, marks_of(64, 256, -1), 4, into(t2t, 32, 256))


def shifted(value, step):
    value = value.astype(BF16)
    lanes = value.shape[-1]
    lane = lax.broadcasted_iota(jnp.int32, (1, lanes), 1)
    inner = jnp.where(lane < step, 0.0, 1.0).astype(BF16)
    outer = jnp.where(lane >= lanes - step, 0.0, 1.0).astype(BF16)
    low = pltpu.roll(value, step, 1) * inner
    high = pltpu.roll(value, lanes - step, 1) * outer
    return low, value, high


def plane_tiles(x):
    def slot(delta):
        return lax.rem(x + delta + 4, 4)

    planes = [(slot(0), 0)]
    planes += [(slot(delta), 8 * p) for delta in (-3, -2, -1) for p in range(2)]
    planes += [(slot(0), 12), (slot(0), 20)]
    planes += [(slot(delta), 20 + 8 * p) for delta in (1, 2, 3) for p in range(2)]
    return planes + [(slot(0), 32)]


def convolve_half(tiles, bands, fields, use):
    planes = plane_tiles(lax.rem(position()[1], 4))

    def load_plane(j):
        at, start = planes[j]
        plane = tiles[at, start : start + 8].reshape(128, 128)
        for c, part in enumerate(shifted(plane, 1)):
            if j <= 8:
                fields[j, c, :, :128] = part
            if j >= 7:
                fields[j - 7, c, :, 128:] = part

    for j in (0, 1, 7, 8):
        load_plane(j)
    for k in range(7):
        for j in (k + 2, k + 9):
            if j not in (7, 8) and j < 16:
                load_plane(j)
        field = fields[k : k + 3].reshape(1152, 256)
        use(k, jnp.dot(bands[...], field, preferred_element_type=F32))


def own_kernel(own, t1_own, fields, sums):
    def use(k, part):
        sums[k] = part

    convolve_half(own, t1_own, fields, use)


def main_kernel(
    own, oth, own_fields, own_sums, t1_oth, t1t, t2, t2t, gf, wg,
    XP, PS, SL, QP, GP, HP, CT, FS, FP, G1, G2,
):
    member, place = position()
    x = lax.rem(place, 4)
    half = pl.multiple_of(member * 16, 16)

    def slot(delta):
        return lax.rem(x + delta + 4, 4)

    def use(k, part):
        pre = part + own_sums[k]
        act = (pre * jax.nn.sigmoid(pre)).astype(BF16).astype(F32).reshape(4, 2, 32, 256)
        rows = (act[:, 0] + act[:, 1]).reshape(128, 256)
        PS[k] = rows[:, :128]
        PS[k + 7] = rows[:, 128:]
        if k >= 5:
            SL[k - 5] = slope(pre[:, :128])
        if k <= 1:
            SL[k + 2] = slope(pre[:, 128:])

    convolve_half(oth, t1_oth, XP, use)

    lane = lax.broadcasted_iota(jnp.int32, (128, 128), 1)
    even = lane % 2 == 0
    for c in range(3):
        QP[4, c, :, 128:] = jnp.zeros((128, 128), BF16)
    for j in range(7):
        total = PS[2 * j] + PS[2 * j + 1]
        total = total + jnp.where(even, pltpu.roll(total, 127, 1), pltpu.roll(total, 1, 1))
        at = place + (j - 3)
        factor = jnp.where((at >= 0) & (at < SLABS), 0.125, 0.0)
        pooled = (total * factor).astype(BF16)
        for c, part in enumerate(shifted(pooled, 2)):
            if j <= 4:
                QP[j, c, :, :128] = part
            if j >= 3:
                QP[j - 3, c, :, 128:] = part

    cots = [(slot(-2), 16), (slot(-1), 16), (slot(0), 28), (slot(1), 36), (slot(2), 36)]
    own_o = pl.multiple_of(member * 32, 32)
    oth_o = pl.multiple_of(32 - member * 32, 32)
    for e, (at, start) in enumerate(cots):
        for high in range(2):
            here = start + 2 * high
            CT[e, high, pl.ds(own_o, 32), :] = own[at, here : here + 2].reshape(32, 128)
            CT[e, high, pl.ds(oth_o, 32), :] = oth[at, here : here + 2].reshape(32, 128)
    row = lax.broadcasted_iota(jnp.int32, (128, 256), 0)
    col = lax.broadcasted_iota(jnp.int32, (128, 256), 1)
    spread = jnp.where(row == (col // 128) * 64 + (col % 128) // 2, 1.0, 0.0).astype(BF16)
    cot = jnp.dot(CT[...].reshape(640, 128), spread, preferred_element_type=F32)

    for e in range(3):
        pre_two = jnp.dot(t2[...], QP[e : e + 3].reshape(1152, 256), preferred_element_type=F32)
        slopes = slope(pre_two)
        for plane in (e, e + 3):
            if plane > 4:
                continue
            side = slopes[:, :128] if plane == e else slopes[:, 128:]
            base = plane * 128
            cots_of = jnp.concatenate(
                [
                    cot[base : base + 64, :128],
                    cot[base : base + 64, 128:],
                    cot[base + 64 : base + 128, :128],
                    cot[base + 64 : base + 128, 128:],
                ],
                axis=0,
            )
            grad = (cots_of * side).astype(BF16).astype(F32)
            for c, part in enumerate(shifted(grad, 2)):
                for m in range(3):
                    n = plane - m
                    if 0 <= n <= 2:
                        GP[m, c, :, n * 128 : (n + 1) * 128] = part
            if plane == 2:
                lanes = lax.broadcasted_iota(jnp.int32, (256, 128), 1)
                kept = jnp.where(lanes % 2 == 0, grad, 0.0).astype(BF16)
                for b in range(3):
                    for at in range(4):
                        h = at + 1 - b
                        here = jnp.zeros((64, 128), BF16)
                        if 0 <= h < 4:
                            here = kept[h * 64 : (h + 1) * 64]
                        G2[b * 64 : (b + 1) * 64, at * 128 : (at + 1) * 128] = here

    back = jnp.dot(t2t[...], GP[...].reshape(2304, 384), preferred_element_type=F32)
    for q, f in enumerate((0, 1, 1, 2)):
        at = place + (f - 1)
        factor = jnp.where((at >= 0) & (at < SLABS), 0.125, 0.0)
        part = (back[:, f * 128 : (f + 1) * 128] * factor).reshape(4, 1, 32, 128)
        wide = jnp.concatenate([part, part], axis=1).reshape(256, 128)
        grad = (wide * SL[q]).astype(BF16)
        for c, piece in enumerate(shifted(grad, 1)):
            if q <= 2:
                HP[q, c, :, :128] = piece
            if q >= 1:
                HP[q - 1, c, :, 128:] = piece
            if c == 1 and q in (1, 2):
                for b in range(3):
                    for at in range(8):
                        h = at + 1 - b
                        here = jnp.zeros((32, 128), BF16)
                        if 0 <= h < 8:
                            here = piece[h * 32 : (h + 1) * 32]
                        to = (q - 1) * 128 + (64, 96, 0)[b]
                        G1[to : to + 32, at * 128 : (at + 1) * 128] = here
    for q in range(2):
        G1[q * 128 + 32 : q * 128 + 64] = jnp.zeros((32, 1024), BF16)

    out = jnp.dot(t1t[...], HP[...].reshape(2304, 256), preferred_element_type=F32)
    for p in range(2):
        side = out[:, p * 128 : (p + 1) * 128].reshape(8, 16, 128)
        gf[:, p] = jnp.transpose(side, (1, 0, 2)).astype(BF16)

    for c in range(3):
        for j in range(4):
            m, side = (j + 6, 0) if j <= 2 else (2, 128)
            to = (j * 3 + c) * 16
            for h in range(8):
                FS[to : to + 16, h * 128 : (h + 1) * 128] = own_fields[
                    m, c, h * 16 : h * 16 + 16, side : side + 128
                ]
        for a in range(3):
            to = (a * 3 + c) * 16
            for h in range(4):
                FP[to : to + 16, h * 128 : (h + 1) * 128] = QP[
                    2 + a, c, pl.ds(h * 32 + half, 16), :128
                ]
    along = (((1,), (1,)), ((), ()))
    one = lax.dot_general(FS[...], G1[...], along, preferred_element_type=F32)
    two = lax.dot_general(FP[...], G2[...], along, preferred_element_type=F32)
    one = one[0:144, :128] + one[48:192, 128:]
    wg[0:144] = jnp.concatenate([two[:, 128:], one[:, 64:]], axis=1).astype(BF16)
    wg[144:288] = two[:, :128].astype(BF16)
    thirds = [one[at : at + 48, :32] for at in (0, 48, 96)]
    rest = jnp.concatenate(thirds + [jnp.zeros((48, 32), F32)], axis=1)
    wg[288:336] = rest.astype(BF16)
    wg[336:] = jnp.zeros((48, 128), BF16)


def own_block(feats, cot, w1, w2):
    vmem = pl.BlockSpec(memory_space=pltpu.VMEM)
    hbm = pl.BlockSpec(memory_space=pltpu.MemorySpace.HBM)
    return pl.pallas_call(
        gather_kernel,
        in_specs=[hbm] * 4,
        out_specs=[vmem] * 3,
        out_shape=[
            jax.ShapeDtypeStruct((20, 16, 128), BF16),
            jax.ShapeDtypeStruct(w1.shape, BF16),
            jax.ShapeDtypeStruct(w2.shape, BF16),
        ],
        scratch_shapes=[
            pltpu.VMEM(feats.shape, BF16),
            pltpu.VMEM(cot.shape, BF16),
            pltpu.SemaphoreType.DMA((4,)),
        ],
        compiler_params=pltpu.CompilerParams(vmem_limit_bytes=4 * 2**20),
        name="gather",
    )(*[pltpu.with_memory_space_constraint(array, pltpu.HBM) for array in (feats, cot, w1, w2)])


def band_weights(w1, w2):
    vmem = pl.BlockSpec(memory_space=pltpu.VMEM)
    shapes = [(256, 1152), (256, 1152), (128, 2304), (256, 1152), (128, 2304)]
    return pl.pallas_call(
        band_kernel,
        in_specs=[vmem] * 2,
        out_specs=[vmem] * 5,
        scratch_shapes=[pltpu.VMEM((8, 288, 256), BF16)],
        out_shape=[jax.ShapeDtypeStruct(shape, BF16) for shape in shapes],
        cost_estimate=pl.CostEstimate(flops=10**9, bytes_accessed=4 * 10**6, transcendentals=0),
        compiler_params=pltpu.CompilerParams(vmem_limit_bytes=16 * 2**20),
        name="bands",
    )(w1, w2)


def slot_kernel(even, block, odd, slots, rows):
    for at, part in enumerate((even, block, odd, block, even)):
        rows[at * 20 : (at + 1) * 20] = part[...]
    place = position()[1]
    x = lax.rem(place, ROW)
    first = jnp.where(lax.rem(place // ROW, 2) == 1, 0, 40)
    for t in range(4):
        at = first + jnp.where(x > t, 0, jnp.where(x == t, 8, 20))
        slots[t] = rows[pl.ds(at, 40)]


def row_slots(even, block, odd):
    vmem = pl.BlockSpec(memory_space=pltpu.VMEM)
    return pl.pallas_call(
        slot_kernel,
        in_specs=[vmem] * 3,
        out_specs=vmem,
        out_shape=jax.ShapeDtypeStruct((4, 40, 16, 128), BF16),
        scratch_shapes=[pltpu.VMEM((100, 16, 128), BF16)],
        compiler_params=pltpu.CompilerParams(vmem_limit_bytes=4 * 2**20),
        name="slots",
    )(even, block, odd)


def own_half(own, t1_own):
    vmem = pl.BlockSpec(memory_space=pltpu.VMEM)
    return pl.pallas_call(
        own_kernel,
        in_specs=[vmem, vmem],
        out_specs=[vmem, vmem],
        out_shape=[
            jax.ShapeDtypeStruct((9, 3, 128, 256), BF16),
            jax.ShapeDtypeStruct((7, 256, 256), F32),
        ],
        cost_estimate=pl.CostEstimate(flops=10**9, bytes_accessed=5 * 10**6, transcendentals=0),
        compiler_params=pltpu.CompilerParams(vmem_limit_bytes=12 * 2**20),
        name="half",
    )(own, t1_own)


def levels(fields, bands):
    vmem = pl.BlockSpec(memory_space=pltpu.VMEM)
    scratch = [
        ((9, 3, 128, 256), BF16),
        ((14, 128, 128), F32),
        ((4, 256, 128), F32),
        ((5, 3, 128, 256), BF16),
        ((3, 3, 256, 384), BF16),
        ((3, 3, 256, 256), BF16),
        ((5, 2, 64, 128), BF16),
        ((192, 1024), BF16),
        ((144, 512), BF16),
        ((256, 1024), BF16),
        ((192, 512), BF16),
    ]
    return pl.pallas_call(
        main_kernel,
        in_specs=[vmem] * 8,
        out_specs=[vmem, vmem],
        out_shape=[
            jax.ShapeDtypeStruct((16, 2, 8, 128), BF16),
            jax.ShapeDtypeStruct((384, 128), BF16),
        ],
        scratch_shapes=[pltpu.VMEM(shape, dtype) for shape, dtype in scratch],
        cost_estimate=pl.CostEstimate(
            flops=10**10, bytes_accessed=8 * 10**6, transcendentals=10**6
        ),
        compiler_params=pltpu.CompilerParams(vmem_limit_bytes=28 * 2**20),
        name="levels",
    )(*fields, *bands)


def exchange(pieces, groups):
    return lax.all_to_all(pieces, DEPTH, 0, 0, axis_index_groups=groups, tiled=True)


def total_over_depth(part):
    pieces = exchange(part.reshape(16, 24, 128), NEAR)
    for groups in (FAR, NEAR):
        total = jnp.sum(pieces.astype(F32), axis=0).astype(BF16)
        pieces = exchange(jnp.broadcast_to(total, (16, 24, 128)), groups)
    return pieces


def split_kernel(total, gf, one_out, two_out, gf_out, one, two, sems):
    pairs = ((gf, gf_out), (one, one_out), (two, two_out))
    away = [
        pltpu.make_async_copy(source, target, sems.at[index])
        for index, (source, target) in enumerate(pairs)
    ]
    away[0].start()
    rows = total[...].reshape(384, 128).astype(F32)
    for a in range(3):
        for c in range(3):
            at = (a * 3 + c) * 16
            first = rows[at : at + 16]
            rest = rows[288 + at % 48 : 304 + at % 48]
            third = at // 48 * 32
            ones = (first[:, 64:96], first[:, 96:], rest[:, third : third + 32])
            for b in range(3):
                to = ((a * 3 + b) * 3 + c) * 16
                one[to : to + 16] = ones[b]
    away[1].start()
    for a in range(3):
        for c in range(3):
            at = (a * 3 + c) * 16
            first, second = rows[at : at + 16], rows[144 + at : 160 + at]
            twos = (second[:, :64], second[:, 64:], first[:, :64])
            for b in range(3):
                to = ((a * 3 + b) * 3 + c) * 16
                two[to : to + 16] = twos[b]
    away[2].start()
    for copy in away:
        copy.wait()


def split_total(total, gf):
    vmem = pl.BlockSpec(memory_space=pltpu.VMEM)
    shapes = [(432, 32), (432, 64)]
    return pl.pallas_call(
        split_kernel,
        in_specs=[vmem, vmem],
        out_specs=[pl.BlockSpec(memory_space=pl.ANY)] * 3,
        out_shape=[jax.ShapeDtypeStruct(shape, F32) for shape in shapes]
        + [jax.ShapeDtypeStruct(gf.shape, BF16)],
        scratch_shapes=[pltpu.VMEM(shape, F32) for shape in shapes]
        + [pltpu.SemaphoreType.DMA((3,))],
        compiler_params=pltpu.CompilerParams(vmem_limit_bytes=4 * 2**20),
        name="split",
    )(total, gf)


def shards(feats, weight_one, weight_two, cotangent):
    block, w1, w2 = own_block(
        feats,
        cotangent,
        jnp.transpose(weight_one, (2, 0, 1)),
        jnp.transpose(weight_two, (2, 1, 0)),
    )
    even = row_swap(block, 0)
    odd = row_swap(block, 1)

    bands = band_weights(w1, w2)

    own = lax.all_to_all(row_slots(even, block, odd), "x", 0, 0, tiled=True)
    oth = lax.ppermute(own, "chan", [(0, 1), (1, 0)])
    own_fields, own_sums = own_half(own, bands[0])
    grad_feats, part = levels((own, oth, own_fields, own_sums), bands[1:])
    one, two, grad_feats = split_total(total_over_depth(part), grad_feats)
    grad_weight_one = jnp.transpose(one.reshape(27, 16, 32), (2, 1, 0))
    grad_weight_two = jnp.transpose(two.reshape(27, 16, 64), (2, 1, 0))
    return (grad_feats, grad_weight_one, grad_weight_two)


def solution(mesh):
    finer = Mesh(
        mesh.devices.reshape(8, 8, 4, mesh.shape["chan"]), DEPTH + ("chan",)
    )
    in_specs = (P("chan", DEPTH, None, None), P(), P(), P("chan", DEPTH, None, None))
    out_specs = (P("chan", DEPTH, None, None), P(None, "chan", None), P(None, "chan", None))

    return jax.shard_map(
        shards, mesh=finer, in_specs=in_specs, out_specs=out_specs, check_vma=False
    )
```
